256 devices in a mesh: gx: 8 (over y, core), gy: 4 (over x), gz: 8 (over z).
Axes of the slice: x: 4, y: 4, z: 8, core: 2. Of those that a mesh axis runs over, the one named last changes fastest.
Arguments:
- positions: float32 [3, 32, 16, 1024], P(None, 'gx', 'gy', 'gz'), may hold values from 0 to 1
- charges: float32 [32, 16, 1024], P('gx', 'gy', 'gz'), may hold values from -1.2 to 1.2
- counts: int32 [32, 16, 32], P('gx', 'gy', 'gz'), may hold values from 16 to 32
- moment_shift: bfloat16 [8, 81, 81], replicated, may hold values from -0.25 to 0.25
- far_operators: bfloat16 [81, 25600], replicated, may hold values from -0.046875 to 0.046875
- local_shift: bfloat16 [8, 81, 81], replicated, may hold values from -0.625 to 0.625
- lattice_operator: bfloat16 [81, 81], replicated, may hold values from -0.625 to 0.625
Outputs:
- potential: float32 [32, 16, 1024], P('gx', 'gy', 'gz')
- electric_field: float32 [3, 32, 16, 1024], P(None, 'gx', 'gy', 'gz')
The draws below stay inside these ranges and needn't reach their ends.
Inputs may be any that keep to these rules, and one draw needn't show every extreme that they name: `counts`: number of live charges in each leaf; slots at or past it are pads.
All inputs are finite; a program needn't handle non-finite values.
Results may differ from the reference program's by a relative error of at most 0.00035.
Values sent between devices are 32-bit elements; how exact they have to be, the bound alone decides.
A program may use at most 256 MiB of HBM per device.

```python
import jax
import jax.numpy as jnp
import numpy as np
from jax import lax

ORDER = 8
TERMS = 81
SLOTS = 32
OPERATOR_COLUMNS = 25600
GRID_X = 32
GRID_Y = 16
GRID_Z = 32


def touch_ends(entries, own_key, least, top_value):
    shape = entries.shape
    spot = [jax.random.randint(jax.random.fold_in(own_key, axis), (), 0, shape[axis]) for axis in range(len(shape))]
    entries = entries.at[tuple(spot)].set(least)
    longest = shape.index(max(shape))
    spot[longest] = (spot[longest] + 1) % shape[longest]
    return entries.at[tuple(spot)].set(top_value)


def block_levels(own_key, dims, shards, least, top_value):
    gain = 1.0
    for axis_at, blocks in shards:
        steps = jax.random.uniform(jax.random.fold_in(jax.random.fold_in(own_key, 6), axis_at), (blocks,), jnp.float32, least / len(shards), top_value / len(shards))
        gain = gain * jnp.repeat(jnp.exp(steps), dims[axis_at] // blocks).reshape((-1,) + (1,) * (len(dims) - 1 - axis_at))
    return gain


def bell_draw(rng, shape, deviation, most, split=(), kind=jnp.bfloat16):
    drawn = jax.random.normal(rng, shape, jnp.float32) * deviation
    if len(split) > 0:
        drawn = block_levels(rng, shape, split, -0.22, 0.18) * drawn
    return jnp.clip(drawn, min=-most, max=most).astype(kind)


def setup_inputs(seed: int = 0) -> dict:
    seeds = jax.random.split(jax.random.key(seed), 8)
    return {
        "positions": jnp.clip(1.0 * jax.random.uniform(seeds[0], (3, GRID_X, GRID_Y, GRID_Z * SLOTS), jnp.float32) ** block_levels(seeds[0], (3, GRID_X, GRID_Y, GRID_Z * SLOTS), ((1, 8), (2, 4), (3, 8)), -0.2, 0.2), 0.0, 1.0),
        "charges": bell_draw(seeds[1], (GRID_X, GRID_Y, GRID_Z * SLOTS), 0.2, 1.2, ((0, 8), (1, 4), (2, 8)), jnp.float32),
        "counts": touch_ends(jax.random.randint(seeds[2], (GRID_X, GRID_Y, GRID_Z), SLOTS // 2, SLOTS + 1), jax.random.fold_in(seeds[2], 1), SLOTS // 2, SLOTS).astype(jnp.int32),
        "moment_shift": bell_draw(seeds[3], (8, TERMS, TERMS), (8 * TERMS) ** -0.5, 0.25),
        "far_operators": bell_draw(seeds[4], (TERMS, OPERATOR_COLUMNS), (189 * TERMS) ** -0.5, 0.046875),
        "local_shift": bell_draw(seeds[5], (8, TERMS, TERMS), TERMS ** -0.5, 0.625),
        "lattice_operator": bell_draw(seeds[6], (TERMS, TERMS), TERMS ** -0.5, 0.625),
    }


SOFTENING = 0.0625

def offset_table():
    listed = []
    for shift_x in range(-3, 4):
        for shift_y in range(-3, 4):
            for shift_z in range(-3, 4):
                if max(abs(shift_x), abs(shift_y), abs(shift_z)) >= 2:
                    listed.append((shift_x, shift_y, shift_z))
    return np.array(listed, dtype=np.int32)

def exponent_table(degree):
    listed = []
    for accumulated in range(degree + 1):
        for height in (0, 1):
            for power_x in range(accumulated - height + 1):
                listed.append((power_x, accumulated - height - power_x, height))
    return np.array(listed, dtype=np.int32)

def power_stack(values, degree):
    listed = [jnp.ones_like(values)]
    for exponent in range(degree):
        listed.append(listed[-1] * values)
    return jnp.stack(listed)

def slope_stack(powers, degree):
    listed = [jnp.zeros_like(powers[0])]
    for exponent in range(1, degree + 1):
        listed.append(float(exponent) * powers[exponent - 1])
    return jnp.stack(listed)

def monomials(relative, degree, with_slopes):
    centred = relative - 0.5
    exponents = exponent_table(degree)
    powers_x = power_stack(centred[0], degree)
    powers_y = power_stack(centred[1], degree)
    powers_z = power_stack(centred[2], degree)
    part_x = powers_x[exponents[:, 0]]
    part_y = powers_y[exponents[:, 1]]
    part_z = powers_z[exponents[:, 2]]
    values = part_x * part_y * part_z
    if not with_slopes:
        return (values, None)
    slope_x = slope_stack(powers_x, degree)[exponents[:, 0]]
    slope_y = slope_stack(powers_y, degree)[exponents[:, 1]]
    slope_z = slope_stack(powers_z, degree)[exponents[:, 2]]
    slopes = (slope_x * part_y * part_z, part_x * slope_y * part_z, part_x * part_y * slope_z)
    return (values, slopes)

def to_moments(stacked):
    values = monomials(stacked[:3], ORDER, False)[0]
    return lax.optimization_barrier(jnp.sum(values * stacked[3][None], axis=-1))

def moments_up(child, operators):
    term_count, size_x, size_y, size_z = child.shape
    grouped = child.reshape(term_count, size_x // 2, 2, size_y // 2, 2, size_z // 2, 2)
    accumulated = jnp.zeros((term_count, size_x // 2 * (size_y // 2) * (size_z // 2)), jnp.float32)
    for octant in range(8):
        child_piece = grouped[:, :, octant >> 2 & 1, :, octant >> 1 & 1, :, octant & 1].reshape(term_count, -1)
        accumulated = accumulated + jnp.dot(operators[octant], child_piece, precision=lax.Precision.HIGHEST)
    return accumulated.reshape(term_count, size_x // 2, size_y // 2, size_z // 2)

def locals_down(parent, operators):
    term_count, size_x, size_y, size_z = parent.shape
    flat_parent = parent.reshape(term_count, -1)
    pieces = [jnp.dot(operators[octant], flat_parent, precision=lax.Precision.HIGHEST).reshape(term_count, size_x, size_y, size_z) for octant in range(8)]
    stacked = jnp.stack(pieces, axis=1).reshape(term_count, 2, 2, 2, size_x, size_y, size_z)
    return stacked.transpose(0, 4, 1, 5, 2, 6, 3).reshape(term_count, 2 * size_x, 2 * size_y, 2 * size_z)

def far_terms(source, grid_shape, coords, parity, operators):
    shifts = offset_table()
    offset_count = shifts.shape[0]
    term_count = source.shape[0]
    shift_x = jnp.asarray(shifts[:, 0:1])
    shift_y = jnp.asarray(shifts[:, 1:2])
    shift_z = jnp.asarray(shifts[:, 2:3])
    size_x, size_y, size_z = grid_shape
    coord_x, coord_y, coord_z = coords
    flat_index = ((coord_x[None, :] + shift_x) % size_x * size_y + (coord_y[None, :] + shift_y) % size_y) * size_z + (coord_z[None, :] + shift_z) % size_z
    picked = jnp.take(source, flat_index, axis=1)
    if parity is not None:
        odd_x, odd_y, odd_z = parity
        admitted = (shift_x >= -2 - odd_x[None, :]) & (shift_x <= 3 - odd_x[None, :])
        admitted = admitted & (shift_y >= -2 - odd_y[None, :]) & (shift_y <= 3 - odd_y[None, :])
        admitted = admitted & (shift_z >= -2 - odd_z[None, :]) & (shift_z <= 3 - odd_z[None, :])
        picked = picked * admitted.astype(jnp.float32)[None]
    ordered = jnp.transpose(picked, (1, 0, 2)).reshape(offset_count * term_count, -1)
    return jnp.dot(operators[:, :offset_count * term_count], ordered, precision=lax.Precision.HIGHEST)

def level_terms(moments, restrict, operators):
    term_count, size_x, size_y, size_z = moments.shape
    target_count = size_x * size_y * size_z
    block_size = min(target_count, 512)
    blocks = jnp.arange(target_count, dtype=jnp.int32).reshape(target_count // block_size, block_size)
    source = moments.reshape(term_count, target_count)

    def one_block(block_rows):
        coord_x = block_rows // (size_y * size_z)
        coord_y = block_rows // size_z % size_y
        coord_z = block_rows % size_z
        parity = (coord_x % 2, coord_y % 2, coord_z % 2) if restrict else None
        return far_terms(source, (size_x, size_y, size_z), (coord_x, coord_y, coord_z), parity, operators)
    result = lax.map(one_block, blocks)
    return result.transpose(1, 0, 2).reshape(term_count, size_x, size_y, size_z)

def evaluate(extended, slab_local, live_mask):
    term_count, size_x, size_y, size_z = slab_local.shape
    slot_count = extended.shape[4]
    target = extended[:, 1:size_x + 1, 1:size_y + 1, 1:size_z + 1, :]
    self_mask = (1.0 - jnp.eye(slot_count, dtype=jnp.float32))[:, None, None, None, :]
    near_potential = jnp.zeros((size_x, size_y, size_z, slot_count), jnp.float32)
    near_x = jnp.zeros_like(near_potential)
    near_y = jnp.zeros_like(near_potential)
    near_z = jnp.zeros_like(near_potential)
    for shift_x in (-1, 0, 1):
        for shift_y in (-1, 0, 1):
            for shift_z in (-1, 0, 1):
                source = extended[:, 1 + shift_x:1 + shift_x + size_x, 1 + shift_y:1 + shift_y + size_y, 1 + shift_z:1 + shift_z + size_z, :]
                source = jnp.moveaxis(source, 4, 1)[..., None]
                delta_x = target[0][None] - source[0] - float(shift_x)
                delta_y = target[1][None] - source[1] - float(shift_y)
                delta_z = target[2][None] - source[2] - float(shift_z)
                distance = delta_x * delta_x + delta_y * delta_y + delta_z * delta_z + SOFTENING
                inverse = lax.rsqrt(distance)
                weight = source[3] * inverse
                if shift_x == 0 and shift_y == 0 and (shift_z == 0):
                    weight = weight * self_mask
                near_potential = near_potential + lax.optimization_barrier(jnp.sum(weight, axis=0))
                cubic_weight = weight * inverse * inverse
                near_x = near_x + lax.optimization_barrier(jnp.sum(cubic_weight * delta_x, axis=0))
                near_y = near_y + lax.optimization_barrier(jnp.sum(cubic_weight * delta_y, axis=0))
                near_z = near_z + lax.optimization_barrier(jnp.sum(cubic_weight * delta_z, axis=0))
    values, slopes = monomials(target[:3], ORDER, True)
    expanded = slab_local[..., None]
    potential = (near_potential + lax.optimization_barrier(jnp.sum(expanded * values, axis=0))) * live_mask
    field_out = jnp.stack([near_x - lax.optimization_barrier(jnp.sum(expanded * slopes[0], axis=0)), near_y - lax.optimization_barrier(jnp.sum(expanded * slopes[1], axis=0)), near_z - lax.optimization_barrier(jnp.sum(expanded * slopes[2], axis=0))]) * live_mask[None]
    return (potential, field_out)

def reference(positions, charges, counts, moment_shift, far_operators, local_shift, lattice_operator):
    slots_index = jnp.arange(SLOTS, dtype=jnp.int32)
    live_mask = (slots_index[None, None, None, :] < counts[..., None]).astype(jnp.float32)
    weights = charges.reshape(GRID_X, GRID_Y, GRID_Z, SLOTS) * live_mask
    stacked = jnp.concatenate([positions.reshape(3, GRID_X, GRID_Y, GRID_Z, SLOTS), weights[None]], axis=0)
    upward = moment_shift.astype(jnp.float32)
    across = far_operators.astype(jnp.float32)
    downward = local_shift.astype(jnp.float32)
    lattice = lattice_operator.astype(jnp.float32)
    moments_leaf = jnp.moveaxis(lax.map(to_moments, jnp.moveaxis(stacked, 1, 0)), 0, 1)
    moments_mid = moments_up(moments_leaf, upward)
    moments_upper = moments_up(moments_mid, upward)
    moments_top = moments_up(moments_upper, upward)
    term_count = moments_top.shape[0]
    root_moments = lax.optimization_barrier(jnp.sum(moments_top.reshape(term_count, -1), axis=1))
    lattice_term = jnp.dot(lattice, root_moments[:, None], precision=lax.Precision.HIGHEST).reshape(term_count, 1, 1, 1)
    local_top = 0.125 * (level_terms(moments_top, False, across) + lattice_term)
    local_upper = 0.25 * level_terms(moments_upper, True, across) + locals_down(local_top, downward)
    local_mid = 0.5 * level_terms(moments_mid, True, across) + locals_down(local_upper, downward)
    local_leaf = level_terms(moments_leaf, True, across) + locals_down(local_mid, downward)
    padded = jnp.pad(stacked, ((0, 0), (1, 1), (1, 1), (1, 1), (0, 0)), mode='wrap')

    def one_slab(slab_row):
        extended = lax.dynamic_slice_in_dim(padded, slab_row, 3, axis=1)
        slab_local = lax.dynamic_slice_in_dim(local_leaf, slab_row, 1, axis=1)
        slab_live = lax.dynamic_slice_in_dim(live_mask, slab_row, 1, axis=0)
        return evaluate(extended, slab_local, slab_live)
    potential, field_out = lax.map(one_slab, jnp.arange(GRID_X, dtype=jnp.int32))
    potential = potential.reshape(GRID_X, GRID_Y, GRID_Z * SLOTS)
    field_out = jnp.moveaxis(field_out, 0, 1).reshape(3, GRID_X, GRID_Y, GRID_Z * SLOTS)
    return (potential, field_out)
```

```python
import functools

import jax
import jax.numpy as jnp
import numpy as np
from jax import lax
from jax.experimental import pallas as pl
from jax.experimental.pallas import tpu as pltpu
from jax.sharding import PartitionSpec as P

ORDER = 8
SLOTS = 32
SOFTENING = 0.0625
TERMS = 81
KPAD = 96
LANES = 128
OFFSETS = 316
CHUNK = 8
MESH = pl.DeviceIdType.MESH
F32 = jnp.float32
BF16 = jnp.bfloat16


def offset_table():
    listed = []
    for shift_x in range(-3, 4):
        for shift_y in range(-3, 4):
            for shift_z in range(-3, 4):
                if max(abs(shift_x), abs(shift_y), abs(shift_z)) >= 2:
                    listed.append((shift_x, shift_y, shift_z))
    return listed


def exponent_list():
    listed = []
    for accumulated in range(ORDER + 1):
        for height in (0, 1):
            for power_x in range(accumulated - height + 1):
                listed.append((power_x, accumulated - height - power_x, height))
    return listed


def exponent_planes():
    planes = np.zeros((4, KPAD, LANES), np.int32)
    for row, (a, b, c) in enumerate(exponent_list()):
        planes[0, row], planes[1, row], planes[2, row], planes[3, row] = a, b, c, 1
    return planes


def slope_matrix():
    listed = exponent_list()
    place = {e: i for i, e in enumerate(listed)}
    matrix = np.zeros((TERMS, 3 * LANES), np.float32)
    for row, (a, b, c) in enumerate(listed):
        if a > 0:
            matrix[row, place[(a - 1, b, c)]] = a
        if b > 0:
            matrix[row, LANES + place[(a, b - 1, c)]] = b
        if c > 0:
            matrix[row, 2 * LANES + place[(a, b, c - 1)]] = c
    return matrix


def lanes_nt(lhs, rhs):
    return lax.dot_general(lhs, rhs, (((1,), (1,)), ((), ())), preferred_element_type=F32)


def halves(value):
    upper = value.astype(BF16)
    return upper, (value - upper.astype(F32)).astype(BF16)


def split_nt(value, rhs):
    rows = value.shape[0]
    if rows % 8:
        value = jnp.concatenate([value, jnp.zeros((8 - rows, value.shape[1]), F32)], axis=0)
    upper, lower = halves(value)
    both = lanes_nt(upper, rhs) + lanes_nt(lower, rhs)
    return both[:rows]


def widen(value):
    return jnp.concatenate([value, jnp.zeros((value.shape[0], LANES - value.shape[1]), F32)], axis=1)


def power_of(base, exponents):
    square = base * base
    fourth = square * square
    eighth = fourth * fourth
    result = jnp.where((exponents & 1) != 0, base, 1.0)
    result = result * jnp.where((exponents & 2) != 0, square, 1.0)
    result = result * jnp.where((exponents & 4) != 0, fourth, 1.0)
    return jnp.where(exponents == 8, eighth, result)


def monomial_tiles(rows_of, exps_ref, high_ref, low_ref):
    for tile in range(16):
        px, py, ox, oy = tile >> 3, tile >> 2 & 1, tile >> 1 & 1, tile & 1
        row_x, row_y, row_z = rows_of(2 * px + ox, 2 * py + oy)
        full = lambda row: jnp.broadcast_to(row - 0.5, (KPAD, LANES))
        value = power_of(full(row_x), exps_ref[0]) * power_of(full(row_y), exps_ref[1])
        value = value * jnp.where(exps_ref[2] != 0, full(row_z), 1.0)
        value = jnp.where(exps_ref[3] != 0, value, 0.0)
        upper, lower = halves(value)
        high_ref[:, tile * LANES : (tile + 1) * LANES] = upper
        low_ref[:, tile * LANES : (tile + 1) * LANES] = lower


def moments_kernel(
    pos_ref, chg_ref, cnt_ref, exps_ref, up_ref, data_ref, live_ref, leaf_ref, mid_ref, top_ref, high_ref, low_ref
):
    counts = jnp.concatenate([cnt_ref[x] for x in range(4)], axis=0).astype(F32).astype(BF16)
    spread = (
        lax.broadcasted_iota(jnp.int32, (4, LANES), 1) // SLOTS == lax.broadcasted_iota(jnp.int32, (4, LANES), 0)
    ).astype(F32).astype(BF16)
    limit = jnp.dot(counts, spread, preferred_element_type=F32)
    slot_of = (lax.broadcasted_iota(jnp.int32, (16, LANES), 1) % SLOTS).astype(F32)
    live = (slot_of < limit).astype(F32)
    for x in range(4):
        live_ref[x] = live[4 * x : 4 * x + 4]
        for y in range(4):
            for c in range(3):
                data_ref[x, y, c : c + 1, :] = pos_ref[c, x, y : y + 1, :]
            data_ref[x, y, 3:4, :] = chg_ref[x, y : y + 1, :] * live[4 * x + y : 4 * x + y + 1]

    def rows_of(x, y):
        return tuple(pos_ref[c, x, y : y + 1, :] for c in range(3))

    monomial_tiles(rows_of, exps_ref, high_ref, low_ref)
    row = lax.broadcasted_iota(jnp.int32, (16, LANES), 0)
    lane = lax.broadcasted_iota(jnp.int32, (16, LANES), 1)
    for group in range(4):
        px, py = group >> 1, group & 1
        pieces = []
        for tile in range(4):
            ox, oy = tile >> 1, tile & 1
            hit = (row // 8 == lane // 64) & (row % 8 == ox * 4 + oy * 2 + lane // 32 % 2)
            weight = jnp.broadcast_to(data_ref[2 * px + ox, 2 * py + oy, 3:4, :], (16, LANES))
            pieces.append(jnp.where(hit, weight, 0.0))
        upper, lower = halves(jnp.concatenate(pieces, axis=1))
        span = slice(group * 512, group * 512 + 512)
        both = lanes_nt(jnp.concatenate([upper, lower], axis=0), high_ref[:, span])
        total = both[:16] + both[16:] + lanes_nt(upper, low_ref[:, span])
        leaf_ref[group * 16 : group * 16 + 16, :] = widen(total)
    mid = jnp.zeros((8, TERMS), F32)
    for octant in range(8):
        mid = mid + split_nt(leaf_ref[pl.ds(octant, 8, stride=8), :][:, :TERMS], up_ref[octant])
    mid_ref[...] = widen(mid)
    which = lax.broadcasted_iota(jnp.int32, (8, TERMS), 0)
    top = jnp.zeros((8, TERMS), F32)
    for octant in range(8):
        top = top + jnp.where(which == octant, split_nt(mid, up_ref[octant]), 0.0)
    top_ref[...] = widen(jnp.sum(top, axis=0, keepdims=True))


DIRECTIONS = [
    (dx, dy, dz) for dx in (-1, 0, 1) for dy in (-1, 0, 1) for dz in (-1, 0, 1) if (dx, dy, dz) != (0, 0, 0)
]


def span_of(step, own, first):
    if step == 0:
        return pl.ds(0, own), pl.ds(first, own)
    if step > 0:
        return pl.ds(own - 1, 1), pl.ds(first - 1, 1)
    return pl.ds(0, 1), pl.ds(first + own, 1)


def exchange_kernel(
    nx, ny, nz, data_ref, leaf_ref, mid_ref, top_ref, ext_ref, wide_ref, mids_ref, tops_ref, send, recv, gsend, grecv, own
):
    ix, iy, iz = lax.axis_index("gx"), lax.axis_index("gy"), lax.axis_index("gz")

    def at(dx, dy, dz):
        return {
            "gx": lax.rem(ix + (dx + nx), nx),
            "gy": lax.rem(iy + (dy + ny), ny),
            "gz": lax.rem(iz + (dz + nz), nz),
        }

    partners = list(DIRECTIONS)
    partners += [(0, 0, k) for k in range(2, nz - 1)]
    partners += [(0, k, 0) for k in range(2, ny - 1)]
    partners += [(k, 0, 0) for k in range(2, nx - 1)]
    barrier = pltpu.get_barrier_semaphore()
    for step in partners:
        pl.semaphore_signal(barrier, inc=1, device_id=at(*step), device_id_type=MESH)
    pl.semaphore_wait(barrier, len(partners))

    def remote(src, dst, ssem, rsem, step):
        copy = pltpu.make_async_remote_copy(
            src_ref=src, dst_ref=dst, send_sem=ssem, recv_sem=rsem, device_id=at(*step), device_id_type=MESH
        )
        copy.start()
        return copy

    first = [
        remote(top_ref, tops_ref.at[ix, iy, iz], gsend.at[k], grecv.at[k], (0, 0, k)) for k in range(1, nz)
    ]
    local = [
        pltpu.make_async_copy(top_ref, tops_ref.at[ix, iy, iz], own.at[0]),
        pltpu.make_async_copy(mid_ref, mids_ref.at[13], own.at[1]),
        pltpu.make_async_copy(leaf_ref, wide_ref.at[pl.ds(1, 2), pl.ds(1, 2), pl.ds(1, 2)], own.at[2]),
        pltpu.make_async_copy(data_ref, ext_ref.at[pl.ds(1, 4), pl.ds(1, 4), 1], own.at[3]),
    ]
    for copy in local:
        copy.start()
    copies = []
    for index, step in enumerate(DIRECTIONS):
        dx, dy, dz = step
        from_x, to_x = span_of(dx, 4, 1)
        from_y, to_y = span_of(dy, 4, 1)
        copies.append(
            remote(
                data_ref.at[from_x, from_y],
                ext_ref.at[to_x, to_y, 1 - dz],
                send.at[0, index],
                recv.at[0, index],
                step,
            )
        )
    for index, step in enumerate(DIRECTIONS):
        dx, dy, dz = step
        from_x, to_x = span_of(dx, 2, 1)
        from_y, to_y = span_of(dy, 2, 1)
        from_z, to_z = span_of(dz, 2, 1)
        copies.append(
            remote(
                leaf_ref.at[from_x, from_y, from_z],
                wide_ref.at[to_x, to_y, to_z],
                send.at[1, index],
                recv.at[1, index],
                step,
            )
        )
        slot = ((1 - dx) * 3 + (1 - dy)) * 3 + (1 - dz)
        copies.append(remote(mid_ref, mids_ref.at[slot], send.at[2, index], recv.at[2, index], step))
    for copy in local:
        copy.wait()
    for copy in first:
        copy.wait()
    second = [
        remote(tops_ref.at[ix, iy], tops_ref.at[ix, iy], gsend.at[8 + k], grecv.at[8 + k], (0, k, 0))
        for k in range(1, ny)
    ]
    for copy in second:
        copy.wait()
    third = [
        remote(tops_ref.at[ix], tops_ref.at[ix], gsend.at[16 + k], grecv.at[16 + k], (k, 0, 0)) for k in range(1, nx)
    ]
    for copy in third:
        copy.wait()
    for copy in copies:
        copy.wait()


def near_kernel(ext_ref, out_ref, table_ref):
    lane = lax.broadcasted_iota(jnp.int32, (4, LANES), 1)
    lane8 = lax.broadcasted_iota(jnp.int32, (8, LANES), 1)
    row8 = lax.broadcasted_iota(jnp.int32, (8, LANES), 0)
    picks = [(lane8 // SLOTS + turn) % 4 * SLOTS + row8 for turn in (3, 0, 1)]

    def fill(cell, carry):
        x, y = cell // 6, cell % 6
        before, here, after = ext_ref[x, y, 0], ext_ref[x, y, 1], ext_ref[x, y, 2]
        sources = (jnp.where(lane >= 96, before, here), here, jnp.where(lane < 32, after, here))
        for ez in range(3):
            for c in range(4):
                wide = jnp.broadcast_to(sources[ez][c : c + 1], (8, LANES))
                for group in range(4):
                    table_ref[cell, ez, c, group * 8 : group * 8 + 8, :] = jnp.take_along_axis(
                        wide, picks[ez] + group * 8, axis=1
                    )
        return carry

    lax.fori_loop(0, 36, fill, 0)

    def target(cell, carry):
        x, y = cell // 4, cell % 4
        mine = ext_ref[x + 1, y + 1, 1]
        wide = [jnp.broadcast_to(mine[c : c + 1], (8, LANES)) for c in range(4)]

        def around(step, sums):
            ex, ey = step // 3, step % 3
            here_x = wide[0] - (ex - 1).astype(F32)
            here_y = wide[1] - (ey - 1).astype(F32)
            other = (x + ex) * 6 + y + ey
            potential, along_x, along_y, along_z = sums
            for ez in range(3):
                here_z = wide[2] - float(ez - 1)
                for group in range(4):
                    span = pl.ds(group * 8, 8)
                    delta_x = here_x - table_ref[other, ez, 0, span, :]
                    delta_y = here_y - table_ref[other, ez, 1, span, :]
                    delta_z = here_z - table_ref[other, ez, 2, span, :]
                    distance = delta_x * delta_x + delta_y * delta_y + (delta_z * delta_z + SOFTENING)
                    inverse = lax.rsqrt(distance)
                    weight = table_ref[other, ez, 3, span, :] * inverse
                    cubic = weight * (inverse * inverse)
                    potential = potential + weight
                    along_x = along_x + cubic * delta_x
                    along_y = along_y + cubic * delta_y
                    along_z = along_z + cubic * delta_z
            return potential, along_x, along_y, along_z

        zero = jnp.zeros((8, LANES), F32)
        sums = lax.fori_loop(0, 9, around, (zero, zero, zero, zero))
        itself = mine[3:4] * lax.rsqrt(jnp.full((1, LANES), SOFTENING, F32))
        rows = [jnp.sum(part, axis=0, keepdims=True) for part in sums]
        rows[0] = rows[0] - itself
        for c in range(4):
            out_ref[x, y, c : c + 1, :] = rows[c]
        return carry

    lax.fori_loop(0, 16, target, 0)


def far_kernel(
    far_ref,
    wide_ref,
    mids_ref,
    tops_ref,
    near_ref,
    data_ref,
    live_ref,
    exps_ref,
    slope_ref,
    up_ref,
    down_ref,
    lattice_ref,
    pot_ref,
    field_ref,
    rows_ref,
    tiles_ref,
    upper_ref,
    ring_ref,
    acc_ref,
    local_ref,
    high_ref,
    low_ref,
):
    ix, iy, iz = lax.axis_index("gx"), lax.axis_index("gy"), lax.axis_index("gz")
    top_x, top_y, top_z = ix // 2, iy // 2, iz // 2
    octant_own = (ix % 2) * 4 + (iy % 2) * 2 + iz % 2

    def gather(n, carry):
        step_x, step_y, step_z = n // 9, n // 3 % 3, n % 3
        for parent in range(8):
            px, py, pz = parent >> 2, parent >> 1 & 1, parent & 1
            rows_ref[pl.ds(n * 128 + parent, 8, stride=16), :] = wide_ref[px + step_x, py + step_y, pz + step_z]
        rows_ref[pl.ds(n * 128 + 8, 8, stride=16), :] = mids_ref[n]
        far_x = lax.rem(top_x + step_x + 3, 4) * 2
        far_y = lax.rem(top_y + step_y + 1, 2) * 2
        far_z = lax.rem(top_z + step_z + 3, 4) * 2
        for octant in range(8):
            ox, oy, oz = octant >> 2, octant >> 1 & 1, octant & 1
            base = n * 128 + octant * 16
            rows_ref[pl.ds(base + 9, 1), :] = tops_ref[far_x + ox, far_y + oy, far_z + oz]
            rows_ref[pl.ds(base + 10, 6), :] = jnp.zeros((6, LANES), F32)
        return carry

    lax.fori_loop(0, 27, gather, 0)

    def convert(n, carry):
        for octant in range(8):
            start = pl.multiple_of(n * 128 + octant * 16, 16)
            tiles_ref[n * 8 + octant] = rows_ref[pl.ds(start, 16), :].astype(BF16)
        return carry

    lax.fori_loop(0, 27, convert, 0)

    for octant in range(8):
        ox, oy, oz = octant >> 2, octant >> 1 & 1, octant & 1
        for box in range(32):
            bx, by, bz = box >> 3, box >> 2 & 1, box & 3
            upper_ref[octant, box : box + 1, :] = tops_ref[2 * bx + ox, 2 * by + oy, 2 * bz + oz]
    coarse = jnp.zeros((32, TERMS), F32)
    for octant in range(8):
        coarse = coarse + split_nt(upper_ref[octant][:, :TERMS], up_ref[octant])
    root = jnp.sum(coarse, axis=0, keepdims=True)
    lattice_term = split_nt(root, lattice_ref[...])
    row = lax.broadcasted_iota(jnp.int32, (32, 32), 0)
    column = lax.broadcasted_iota(jnp.int32, (32, 32), 1)
    wanted = (
        (row // 8 + top_x) % 4 * 8 + (row // 4 % 2 + top_y) % 2 * 4 + (row % 4 + top_z) % 4
    )
    turned = jnp.dot(
        (wanted == column).astype(F32).astype(BF16), widen(coarse).astype(BF16), preferred_element_type=F32
    )
    for box in range(32):
        ring_ref[box] = jnp.broadcast_to(turned[box : box + 1], (16, LANES)).astype(BF16)

    shifts = offset_table()
    empty = jnp.zeros((16, LANES), BF16)
    total = jnp.zeros((144, TERMS), F32)
    for start in range(0, OFFSETS, CHUNK):
        columns, operators = [], []
        for index in range(start, min(start + CHUNK, OFFSETS)):
            shift = shifts[index]
            parts = []
            for parity in range(8):
                odd = (parity >> 2, parity >> 1 & 1, parity & 1)
                place = [shift[axis] + odd[axis] for axis in range(3)]
                if all(-2 <= c <= 3 for c in place):
                    around = [(c + 2) // 2 for c in place]
                    inner = [(c + 2) % 2 for c in place]
                    cell = ((around[0] * 3 + around[1]) * 3 + around[2]) * 8
                    parts.append(tiles_ref[cell + inner[0] * 4 + inner[1] * 2 + inner[2]])
                else:
                    parts.append(empty)
            parts.append(ring_ref[shift[0] % 4 * 8 + shift[1] % 2 * 4 + shift[2] % 4])
            columns.append(jnp.concatenate(parts, axis=0))
            begin = index * TERMS
            if begin + LANES <= far_ref.shape[1]:
                operators.append(far_ref[:, begin : begin + LANES])
            else:
                tail = far_ref[:, begin : begin + TERMS]
                operators.append(jnp.concatenate([tail, jnp.zeros((TERMS, LANES - TERMS), BF16)], axis=1))
        total = total + lanes_nt(jnp.concatenate(columns, axis=1), jnp.concatenate(operators, axis=1))
    acc_ref[...] = widen(total)

    local_top = 0.125 * (acc_ref[128:129, :][:, :TERMS] + lattice_term)
    local_upper = 0.25 * acc_ref[pl.ds(octant_own * 16 + 9, 1), :][:, :TERMS] + split_nt(
        local_top, down_ref[octant_own]
    )
    upper_wide = jnp.broadcast_to(local_upper, (8, TERMS))
    which = lax.broadcasted_iota(jnp.int32, (8, TERMS), 0)
    local_mid = 0.5 * acc_ref[pl.ds(8, 8, stride=16), :][:, :TERMS]
    for octant in range(8):
        local_mid = local_mid + jnp.where(which == octant, split_nt(upper_wide, down_ref[octant]), 0.0)
    for octant in range(8):
        local = acc_ref[octant * 16 : octant * 16 + 8, :][:, :TERMS] + split_nt(local_mid, down_ref[octant])
        local_ref[octant * 8 : octant * 8 + 8, :] = widen(local)
    local_leaf = local_ref[...]
    upper, lower = halves(local_leaf[:, :TERMS])
    slopes = jnp.dot(upper, slope_ref[...], preferred_element_type=F32) + jnp.dot(
        lower, slope_ref[...], preferred_element_type=F32
    )
    parts = [local_leaf] + [slopes[:, c * LANES : (c + 1) * LANES] for c in range(3)]
    split_parts = [halves(part[:, :KPAD]) for part in parts]

    def rows_of(x, y):
        return tuple(data_ref[x, y, c : c + 1, :] for c in range(3))

    monomial_tiles(rows_of, exps_ref, high_ref, low_ref)
    row = lax.broadcasted_iota(jnp.int32, (16, LANES), 0)
    lane = lax.broadcasted_iota(jnp.int32, (16, LANES), 1)
    for parity in range(4):
        span = slice(parity * 16, parity * 16 + 16)
        coef_high = jnp.concatenate([part[0][span] for part in split_parts], axis=0)
        coef_low = jnp.concatenate([part[1][span] for part in split_parts], axis=0)
        coef = jnp.concatenate([coef_high, coef_low], axis=0)
        for group in range(4):
            x, y = (group >> 1) * 2 + (parity >> 1), (group & 1) * 2 + (parity & 1)
            tile = group * 4 + parity
            lanes = slice(tile * LANES, tile * LANES + LANES)
            both = jnp.dot(coef, high_ref[:, lanes], preferred_element_type=F32)
            value = both[:64] + both[64:] + jnp.dot(coef_high, low_ref[:, lanes], preferred_element_type=F32)
            hit = (row // 8 == lane // 32 % 2) & (row % 8 == group * 2 + lane // 64)
            sums = [
                jnp.sum(jnp.where(hit, value[16 * c : 16 * c + 16], 0.0), axis=0, keepdims=True) for c in range(4)
            ]
            live = live_ref[x, y : y + 1, :]
            pot_ref[x, y : y + 1, :] = (near_ref[x, y, 0:1, :] + sums[0]) * live
            for c in range(3):
                field_ref[c, x, y : y + 1, :] = (near_ref[x, y, c + 1 : c + 2, :] - sums[c + 1]) * live


VMEM = pl.BlockSpec(memory_space=pltpu.VMEM)


def shape(*dims):
    return jax.ShapeDtypeStruct(dims, F32)


def moments_call(positions, charges, counts, exps, moment_shift):
    return pl.pallas_call(
        moments_kernel,
        out_shape=(shape(4, 4, 4, LANES), shape(4, 4, LANES), shape(64, LANES), shape(8, LANES), shape(1, LANES)),
        in_specs=[VMEM] * 5,
        out_specs=(VMEM,) * 5,
        scratch_shapes=[pltpu.VMEM((KPAD, 2048), BF16)] * 2,
        name="moments",
    )(positions, charges, counts, exps, moment_shift)


def exchange_call(sizes, data, leaf, mid, top):
    dma = pltpu.SemaphoreType.DMA
    return pl.pallas_call(
        functools.partial(exchange_kernel, *sizes),
        out_shape=(
            shape(6, 6, 3, 4, LANES),
            shape(4, 4, 4, 8, LANES),
            shape(27, 8, LANES),
            shape(*sizes, 1, LANES),
        ),
        in_specs=[VMEM] * 4,
        out_specs=(VMEM,) * 4,
        scratch_shapes=[dma((3, 26)), dma((3, 26)), dma((24,)), dma((24,)), dma((4,))],
        compiler_params=pltpu.CompilerParams(collective_id=0, has_side_effects=True),
        name="exchange",
    )(data, leaf, mid, top)


def near_call(ext):
    return pl.pallas_call(
        near_kernel,
        out_shape=shape(4, 4, 4, LANES),
        in_specs=[VMEM],
        out_specs=VMEM,
        scratch_shapes=[pltpu.VMEM((36, 3, 4, SLOTS, LANES), F32)],
        name="near",
    )(ext)


def far_call(*operands):
    return pl.pallas_call(
        far_kernel,
        out_shape=(shape(4, 4, LANES), shape(3, 4, 4, LANES)),
        in_specs=[VMEM] * 12,
        out_specs=(VMEM,) * 2,
        scratch_shapes=[
            pltpu.VMEM((27 * 128, LANES), F32),
            pltpu.VMEM((216, 16, LANES), BF16),
            pltpu.VMEM((8, 32, LANES), F32),
            pltpu.VMEM((32, 16, LANES), BF16),
            pltpu.VMEM((144, LANES), F32),
            pltpu.VMEM((64, LANES), F32),
            pltpu.VMEM((KPAD, 2048), BF16),
            pltpu.VMEM((KPAD, 2048), BF16),
        ],
        name="far",
    )(*operands)


def solution(mesh):
    sizes = tuple(mesh.shape[axis] for axis in ("gx", "gy", "gz"))

    def per_device(
        positions, charges, counts, moment_shift, far_operators, local_shift, lattice_operator
    ):
        exps = jnp.asarray(exponent_planes())
        slope = jnp.asarray(slope_matrix()).astype(BF16)
        data, live, leaf, mid, top = moments_call(positions, charges, counts, exps, moment_shift)
        ext, wide, mids, tops = exchange_call(sizes, data, leaf.reshape(2, 2, 2, 8, LANES), mid, top)
        near = near_call(ext)
        return far_call(
            far_operators,
            wide,
            mids,
            tops,
            near,
            data,
            live,
            exps,
            slope,
            moment_shift,
            local_shift,
            lattice_operator,
        )

    placed = (
        P(None, "gx", "gy", "gz"),
        P("gx", "gy", "gz"),
        P("gx", "gy", "gz"),
        P(),
        P(),
        P(),
        P(),
    )
    return jax.shard_map(
        per_device,
        mesh=mesh,
        in_specs=placed,
        out_specs=(P("gx", "gy", "gz"), P(None, "gx", "gy", "gz")),
        check_vma=False,
    )
```

```python
import functools

import jax
import jax.numpy as jnp
import numpy as np
from jax import lax
from jax.experimental import pallas as pl
from jax.experimental.pallas import tpu as pltpu
from jax.sharding import PartitionSpec as P

ORDER = 8
SLOTS = 32
SOFTENING = 0.0625
TERMS = 81
KPAD = 96
LANES = 128
OFFSETS = 316
CHUNK = 8
MESH = pl.DeviceIdType.MESH
F32 = jnp.float32
BF16 = jnp.bfloat16


def offset_table():
    listed = []
    for shift_x in range(-3, 4):
        for shift_y in range(-3, 4):
            for shift_z in range(-3, 4):
                if max(abs(shift_x), abs(shift_y), abs(shift_z)) >= 2:
                    listed.append((shift_x, shift_y, shift_z))
    return listed


def exponent_list():
    listed = []
    for accumulated in range(ORDER + 1):
        for height in (0, 1):
            for power_x in range(accumulated - height + 1):
                listed.append((power_x, accumulated - height - power_x, height))
    return listed


def exponent_planes():
    planes = np.zeros((4, KPAD, LANES), np.int32)
    for row, (a, b, c) in enumerate(exponent_list()):
        planes[0, row], planes[1, row], planes[2, row], planes[3, row] = a, b, c, 1
    return planes


def slope_matrix():
    listed = exponent_list()
    place = {e: i for i, e in enumerate(listed)}
    matrix = np.zeros((TERMS, 3 * LANES), np.float32)
    for row, (a, b, c) in enumerate(listed):
        if a > 0:
            matrix[row, place[(a - 1, b, c)]] = a
        if b > 0:
            matrix[row, LANES + place[(a, b - 1, c)]] = b
        if c > 0:
            matrix[row, 2 * LANES + place[(a, b, c - 1)]] = c
    return matrix


def lanes_nt(lhs, rhs):
    return lax.dot_general(lhs, rhs, (((1,), (1,)), ((), ())), preferred_element_type=F32)


def halves(value):
    upper = value.astype(BF16)
    return upper, (value - upper.astype(F32)).astype(BF16)


def split_nt(value, rhs):
    rows = value.shape[0]
    if rows % 8:
        value = jnp.concatenate([value, jnp.zeros((8 - rows, value.shape[1]), F32)], axis=0)
    upper, lower = halves(value)
    both = lanes_nt(upper, rhs) + lanes_nt(lower, rhs)
    return both[:rows]


def widen(value):
    return jnp.concatenate([value, jnp.zeros((value.shape[0], LANES - value.shape[1]), F32)], axis=1)


def power_of(base, exponents):
    square = base * base
    fourth = square * square
    eighth = fourth * fourth
    result = jnp.where((exponents & 1) != 0, base, 1.0)
    result = result * jnp.where((exponents & 2) != 0, square, 1.0)
    result = result * jnp.where((exponents & 4) != 0, fourth, 1.0)
    return jnp.where(exponents == 8, eighth, result)


def monomial_tiles(rows_of, exps_ref, high_ref, low_ref):
    for tile in range(16):
        px, py, ox, oy = tile >> 3, tile >> 2 & 1, tile >> 1 & 1, tile & 1
        row_x, row_y, row_z = rows_of(2 * px + ox, 2 * py + oy)
        full = lambda row: jnp.broadcast_to(row - 0.5, (KPAD, LANES))
        value = power_of(full(row_x), exps_ref[0]) * power_of(full(row_y), exps_ref[1])
        value = value * jnp.where(exps_ref[2] != 0, full(row_z), 1.0)
        value = jnp.where(exps_ref[3] != 0, value, 0.0)
        upper, lower = halves(value)
        high_ref[:, tile * LANES : (tile + 1) * LANES] = upper
        low_ref[:, tile * LANES : (tile + 1) * LANES] = lower


def octant_operators(native_ref, rows_ref):
    rows_ref[:, :TERMS] = native_ref[...].astype(F32).reshape(TERMS * 8, TERMS)


def octant_operator(rows_ref, octant):
    return rows_ref[pl.ds(octant, TERMS, stride=8), :][:, :TERMS].astype(BF16)


def prepare(pos_ref, chg_ref, cnt_ref, data_ref, live_ref):
    counts = jnp.concatenate([cnt_ref[x] for x in range(4)], axis=0).astype(F32).astype(BF16)
    spread = (
        lax.broadcasted_iota(jnp.int32, (4, LANES), 1) // SLOTS == lax.broadcasted_iota(jnp.int32, (4, LANES), 0)
    ).astype(F32).astype(BF16)
    limit = jnp.dot(counts, spread, preferred_element_type=F32)
    slot_of = (lax.broadcasted_iota(jnp.int32, (16, LANES), 1) % SLOTS).astype(F32)
    live = (slot_of < limit).astype(F32)
    for x in range(4):
        live_ref[x] = live[4 * x : 4 * x + 4]
        for y in range(4):
            for c in range(3):
                data_ref[x, y, c : c + 1, :] = pos_ref[c, x, y : y + 1, :]
            data_ref[x, y, 3:4, :] = chg_ref[x, y : y + 1, :] * live[4 * x + y : 4 * x + y + 1]


def rows_from(data_ref):
    return lambda x, y: tuple(data_ref[x, y, c : c + 1, :] for c in range(3))


def moments(data_ref, operator_rows, leaf_ref, mid_ref, top_ref, high_ref, low_ref):
    row = lax.broadcasted_iota(jnp.int32, (16, LANES), 0)
    lane = lax.broadcasted_iota(jnp.int32, (16, LANES), 1)
    for group in range(4):
        px, py = group >> 1, group & 1
        pieces = []
        for tile in range(4):
            ox, oy = tile >> 1, tile & 1
            hit = (row // 8 == lane // 64) & (row % 8 == ox * 4 + oy * 2 + lane // 32 % 2)
            weight = jnp.broadcast_to(data_ref[2 * px + ox, 2 * py + oy, 3:4, :], (16, LANES))
            pieces.append(jnp.where(hit, weight, 0.0))
        upper, lower = halves(jnp.concatenate(pieces, axis=1))
        span = slice(group * 512, group * 512 + 512)
        both = lanes_nt(jnp.concatenate([upper, lower], axis=0), high_ref[:, span])
        total = widen(both[:16] + both[16:] + lanes_nt(upper, low_ref[:, span]))
        leaf_ref[px, py, 0] = total[:8]
        leaf_ref[px, py, 1] = total[8:]
    mid = jnp.zeros((8, TERMS), F32)
    top = jnp.zeros((8, TERMS), F32)
    which = lax.broadcasted_iota(jnp.int32, (8, TERMS), 0)
    tiles = [leaf_ref[p >> 2, p >> 1 & 1, p & 1] for p in range(8)]
    operators = [octant_operator(operator_rows, octant) for octant in range(8)]
    for octant in range(8):
        rows = jnp.concatenate([tile[octant : octant + 1] for tile in tiles], axis=0)
        mid = mid + split_nt(rows[:, :TERMS], operators[octant])
    mid_ref[...] = widen(mid)
    for octant in range(8):
        top = top + jnp.where(which == octant, split_nt(mid, operators[octant]), 0.0)
    top_ref[...] = widen(jnp.sum(top, axis=0, keepdims=True))


DIRECTIONS = [
    (dx, dy, dz) for dx in (-1, 0, 1) for dy in (-1, 0, 1) for dz in (-1, 0, 1) if (dx, dy, dz) != (0, 0, 0)
]


def span_of(step, own, first):
    if step == 0:
        return pl.ds(0, own), pl.ds(first, own)
    if step > 0:
        return pl.ds(own - 1, 1), pl.ds(first - 1, 1)
    return pl.ds(0, 1), pl.ds(first + own, 1)


def fill_rows(ext_ref, turned_ref):
    lane = lax.broadcasted_iota(jnp.int32, (4, LANES), 1)

    def along_x(x, carry):
        def along_y(y, inner):
            before, here, after = ext_ref[x, y, 0], ext_ref[x, y, 1], ext_ref[x, y, 2]
            turned_ref[x, y, 0] = pltpu.roll(jnp.where(lane >= 96, before, here), 32, 1)
            turned_ref[x, y, 1] = here
            turned_ref[x, y, 2] = pltpu.roll(jnp.where(lane < 32, after, here), 96, 1)
            return inner

        return lax.fori_loop(0, 6, along_y, carry)

    lax.fori_loop(0, 6, along_x, 0)


def fill_table(turned_ref, table_ref):
    lane = lax.broadcasted_iota(jnp.int32, (8, LANES), 1)
    base = lane // SLOTS * SLOTS + lax.broadcasted_iota(jnp.int32, (8, LANES), 0)
    for group in range(4):
        pick = base + group * 8

        def along_x(x, carry):
            def along_y(y, inner):
                for ez in range(3):
                    rows = turned_ref[x, y, ez]
                    for c in range(4):
                        table_ref[x, y, ez, c, group * 8 : group * 8 + 8, :] = jnp.take_along_axis(
                            jnp.broadcast_to(rows[c : c + 1], (8, LANES)), pick, axis=1
                        )
                return inner

            return lax.fori_loop(0, 6, along_y, carry)

        lax.fori_loop(0, 6, along_x, 0)


def near_rows(first, last, data_ref, table_ref, out_ref):
    def along_x(x, carry):
        def along_y(y, inner):
            mine = data_ref[x, y]
            wide = [jnp.broadcast_to(mine[c : c + 1], (8, LANES)) for c in range(3)]
            here_y = [wide[1] - float(ey - 1) for ey in range(3)]
            here_z = [wide[2] - float(ez - 1) for ez in range(3)]

            def around(ex, sums):
                here_x = wide[0] - (ex - 1).astype(F32)
                potential, field_x, field_y, field_z = sums
                for ey in range(3):
                    for ez in range(3):
                        for group in range(4):
                            span = pl.ds(group * 8, 8)
                            delta_x = here_x - table_ref[x + ex, y + ey, ez, 0, span, :]
                            delta_y = here_y[ey] - table_ref[x + ex, y + ey, ez, 1, span, :]
                            delta_z = here_z[ez] - table_ref[x + ex, y + ey, ez, 2, span, :]
                            distance = delta_x * delta_x + delta_y * delta_y + (delta_z * delta_z + SOFTENING)
                            inverse = lax.rsqrt(distance)
                            weight = table_ref[x + ex, y + ey, ez, 3, span, :] * inverse
                            cubic = weight * (inverse * inverse)
                            potential = potential + weight
                            field_x = field_x + cubic * delta_x
                            field_y = field_y + cubic * delta_y
                            field_z = field_z + cubic * delta_z
                return potential, field_x, field_y, field_z

            zero = jnp.zeros((8, LANES), F32)
            sums = lax.fori_loop(0, 3, around, (zero, zero, zero, zero))
            itself = mine[3:4] * lax.rsqrt(jnp.full((1, LANES), SOFTENING, F32))
            rows = [jnp.sum(part, axis=0, keepdims=True) for part in sums]
            rows[0] = rows[0] - itself
            for c in range(4):
                out_ref[x, y, c : c + 1, :] = rows[c]
            return inner

        return lax.fori_loop(0, 4, along_y, carry)

    lax.fori_loop(first, last, along_x, 0)


def pairs_kernel(
    nx,
    ny,
    nz,
    pos_ref,
    chg_ref,
    cnt_ref,
    exps_ref,
    up_ref,
    near_ref,
    data_ref,
    live_ref,
    wide_ref,
    mids_ref,
    tops_ref,
    ext_ref,
    leaf_ref,
    mid_ref,
    top_ref,
    operator_rows,
    high_ref,
    low_ref,
    turned_ref,
    table_ref,
    send,
    recv,
    gsend,
    grecv,
    own,
):
    ix, iy, iz = lax.axis_index("gx"), lax.axis_index("gy"), lax.axis_index("gz")

    def at(dx, dy, dz):
        return {
            "gx": lax.rem(ix + (dx + nx), nx),
            "gy": lax.rem(iy + (dy + ny), ny),
            "gz": lax.rem(iz + (dz + nz), nz),
        }

    plane = [(0, b, c) for b in range(ny) for c in range(nz) if b or c]
    line = [(a, 0, 0) for a in range(1, nx)]
    wrapped = lambda step: (step[0] % nx, step[1] % ny, step[2] % nz)
    partners = sorted({wrapped(step) for step in DIRECTIONS} | set(plane) | set(line))
    barrier = pltpu.get_barrier_semaphore()
    for step in partners:
        pl.semaphore_signal(barrier, inc=1, device_id=at(*step), device_id_type=MESH)

    prepare(pos_ref, chg_ref, cnt_ref, data_ref, live_ref)
    octant_operators(up_ref, operator_rows)
    monomial_tiles(rows_from(data_ref), exps_ref, high_ref, low_ref)
    moments(data_ref, operator_rows, leaf_ref, mid_ref, top_ref, high_ref, low_ref)

    pl.semaphore_wait(barrier, len(partners))

    def remote(src, dst, ssem, rsem, step):
        copy = pltpu.make_async_remote_copy(
            src_ref=src, dst_ref=dst, send_sem=ssem, recv_sem=rsem, device_id=at(*step), device_id_type=MESH
        )
        copy.start()
        return copy

    local = [
        pltpu.make_async_copy(data_ref, ext_ref.at[pl.ds(1, 4), pl.ds(1, 4), 1], own.at[0]),
        pltpu.make_async_copy(leaf_ref, wide_ref.at[pl.ds(1, 2), pl.ds(1, 2), pl.ds(1, 2)], own.at[1]),
        pltpu.make_async_copy(mid_ref, mids_ref.at[13], own.at[2]),
        pltpu.make_async_copy(top_ref, tops_ref.at[ix, iy, iz], own.at[3]),
    ]
    for copy in local:
        copy.start()
    halo = []
    for index, step in enumerate(DIRECTIONS):
        dx, dy, dz = step
        from_x, to_x = span_of(dx, 4, 1)
        from_y, to_y = span_of(dy, 4, 1)
        src, dst = data_ref.at[from_x, from_y], ext_ref.at[to_x, to_y, 1 - dz]
        halo.append(remote(src, dst, send.at[0, index], recv.at[0, index], step))
    first = [
        remote(top_ref, tops_ref.at[ix, iy, iz], gsend.at[k], grecv.at[k], step) for k, step in enumerate(plane)
    ]
    boxes = []
    for index, step in enumerate(DIRECTIONS):
        spans = [span_of(d, 2, 1) for d in step]
        src = leaf_ref.at[spans[0][0], spans[1][0], spans[2][0]]
        dst = wide_ref.at[spans[0][1], spans[1][1], spans[2][1]]
        boxes.append(remote(src, dst, send.at[1, index], recv.at[1, index], step))
        slot = ((1 - step[0]) * 3 + (1 - step[1])) * 3 + (1 - step[2])
        boxes.append(remote(mid_ref, mids_ref.at[slot], send.at[2, index], recv.at[2, index], step))
    for copy in local:
        copy.wait()
    for copy in halo:
        copy.wait()
    fill_rows(ext_ref, turned_ref)
    fill_table(turned_ref, table_ref)
    for copy in first:
        copy.wait()
    second = [
        remote(tops_ref.at[ix], tops_ref.at[ix], gsend.at[32 + k], grecv.at[32 + k], step)
        for k, step in enumerate(line)
    ]
    near_rows(0, 4, data_ref, table_ref, near_ref)
    for copy in second:
        copy.wait()
    for copy in boxes:
        copy.wait()


def far_kernel(
    far_ref,
    wide_ref,
    mids_ref,
    tops_ref,
    near_ref,
    data_ref,
    live_ref,
    exps_ref,
    slope_ref,
    up_ref,
    down_ref,
    lattice_ref,
    pot_ref,
    field_ref,
    rows_ref,
    tiles_ref,
    upper_ref,
    ring_ref,
    acc_ref,
    local_ref,
    high_ref,
    low_ref,
    up_rows,
    down_rows,
    whole_ref,
    arrive,
):
    fetch = pltpu.make_async_copy(far_ref, whole_ref, arrive.at[0])
    fetch.start()
    octant_operators(up_ref, up_rows)
    octant_operators(down_ref, down_rows)
    ix, iy, iz = lax.axis_index("gx"), lax.axis_index("gy"), lax.axis_index("gz")
    top_x, top_y, top_z = ix // 2, iy // 2, iz // 2
    octant_own = (ix % 2) * 4 + (iy % 2) * 2 + iz % 2

    def gather(n, carry):
        step_x, step_y, step_z = n // 9, n // 3 % 3, n % 3
        for parent in range(8):
            px, py, pz = parent >> 2, parent >> 1 & 1, parent & 1
            rows_ref[pl.ds(n * 128 + parent, 8, stride=16), :] = wide_ref[px + step_x, py + step_y, pz + step_z]
        rows_ref[pl.ds(n * 128 + 8, 8, stride=16), :] = mids_ref[n]
        far_x = lax.rem(top_x + step_x + 3, 4) * 2
        far_y = lax.rem(top_y + step_y + 1, 2) * 2
        far_z = lax.rem(top_z + step_z + 3, 4) * 2
        for octant in range(8):
            ox, oy, oz = octant >> 2, octant >> 1 & 1, octant & 1
            base = n * 128 + octant * 16
            rows_ref[pl.ds(base + 9, 1), :] = tops_ref[far_x + ox, far_y + oy, far_z + oz]
            rows_ref[pl.ds(base + 10, 6), :] = jnp.zeros((6, LANES), F32)
        return carry

    lax.fori_loop(0, 27, gather, 0)

    def convert(n, carry):
        for octant in range(8):
            start = pl.multiple_of(n * 128 + octant * 16, 16)
            tiles_ref[n * 8 + octant] = rows_ref[pl.ds(start, 16), :].astype(BF16)
        return carry

    lax.fori_loop(0, 27, convert, 0)

    for octant in range(8):
        ox, oy, oz = octant >> 2, octant >> 1 & 1, octant & 1
        for box in range(32):
            bx, by, bz = box >> 3, box >> 2 & 1, box & 3
            upper_ref[octant, box : box + 1, :] = tops_ref[2 * bx + ox, 2 * by + oy, 2 * bz + oz]
    coarse = jnp.zeros((32, TERMS), F32)
    for octant in range(8):
        coarse = coarse + split_nt(upper_ref[octant][:, :TERMS], octant_operator(up_rows, octant))
    root = jnp.sum(coarse, axis=0, keepdims=True)
    lattice_term = split_nt(root, lattice_ref[...])
    row = lax.broadcasted_iota(jnp.int32, (32, 32), 0)
    column = lax.broadcasted_iota(jnp.int32, (32, 32), 1)
    wanted = (
        (row // 8 + top_x) % 4 * 8 + (row // 4 % 2 + top_y) % 2 * 4 + (row % 4 + top_z) % 4
    )
    turned = jnp.dot(
        (wanted == column).astype(F32).astype(BF16), widen(coarse).astype(BF16), preferred_element_type=F32
    )
    for box in range(32):
        ring_ref[box] = jnp.broadcast_to(turned[box : box + 1], (16, LANES)).astype(BF16)

    fetch.wait()
    shifts = offset_table()
    empty = jnp.zeros((16, LANES), BF16)
    total = jnp.zeros((144, TERMS), F32)
    for start in range(0, OFFSETS, CHUNK):
        columns, operators = [], []
        for index in range(start, min(start + CHUNK, OFFSETS)):
            shift = shifts[index]
            parts = []
            for parity in range(8):
                odd = (parity >> 2, parity >> 1 & 1, parity & 1)
                place = [shift[axis] + odd[axis] for axis in range(3)]
                if all(-2 <= c <= 3 for c in place):
                    around = [(c + 2) // 2 for c in place]
                    inner = [(c + 2) % 2 for c in place]
                    cell = ((around[0] * 3 + around[1]) * 3 + around[2]) * 8
                    parts.append(tiles_ref[cell + inner[0] * 4 + inner[1] * 2 + inner[2]])
                else:
                    parts.append(empty)
            parts.append(ring_ref[shift[0] % 4 * 8 + shift[1] % 2 * 4 + shift[2] % 4])
            columns.append(jnp.concatenate(parts, axis=0))
            begin = index * TERMS
            if begin + LANES <= whole_ref.shape[1]:
                operators.append(whole_ref[:, begin : begin + LANES])
            else:
                tail = whole_ref[:, begin : begin + TERMS]
                operators.append(jnp.concatenate([tail, jnp.zeros((TERMS, LANES - TERMS), BF16)], axis=1))
        total = total + lanes_nt(jnp.concatenate(columns, axis=1), jnp.concatenate(operators, axis=1))
    acc_ref[...] = widen(total)

    local_top = 0.125 * (acc_ref[128:129, :][:, :TERMS] + lattice_term)
    own_down = jnp.where(
        lax.broadcasted_iota(jnp.int32, (TERMS * 8, LANES), 0) % 8 == octant_own, down_rows[...], 0.0
    )
    own_down = jnp.sum(own_down.reshape(TERMS, 8, LANES), axis=1)[:, :TERMS].astype(BF16)
    downs = [octant_operator(down_rows, octant) for octant in range(8)]
    local_upper = 0.25 * acc_ref[pl.ds(octant_own * 16 + 9, 1), :][:, :TERMS] + split_nt(
        local_top, own_down
    )
    upper_wide = jnp.broadcast_to(local_upper, (8, TERMS))
    which = lax.broadcasted_iota(jnp.int32, (8, TERMS), 0)
    local_mid = 0.5 * acc_ref[pl.ds(8, 8, stride=16), :][:, :TERMS]
    for octant in range(8):
        local_mid = local_mid + jnp.where(which == octant, split_nt(upper_wide, downs[octant]), 0.0)
    for octant in range(8):
        local = acc_ref[octant * 16 : octant * 16 + 8, :][:, :TERMS] + split_nt(local_mid, downs[octant])
        local_ref[octant * 8 : octant * 8 + 8, :] = widen(local)
    local_leaf = local_ref[...]
    upper, lower = halves(local_leaf[:, :TERMS])
    slopes = jnp.dot(upper, slope_ref[...], preferred_element_type=F32) + jnp.dot(
        lower, slope_ref[...], preferred_element_type=F32
    )
    parts = [local_leaf] + [slopes[:, c * LANES : (c + 1) * LANES] for c in range(3)]
    split_parts = [halves(part[:, :KPAD]) for part in parts]

    monomial_tiles(rows_from(data_ref), exps_ref, high_ref, low_ref)
    row = lax.broadcasted_iota(jnp.int32, (16, LANES), 0)
    lane = lax.broadcasted_iota(jnp.int32, (16, LANES), 1)
    for parity in range(4):
        span = slice(parity * 16, parity * 16 + 16)
        coef_high = jnp.concatenate([part[0][span] for part in split_parts], axis=0)
        coef_low = jnp.concatenate([part[1][span] for part in split_parts], axis=0)
        coef = jnp.concatenate([coef_high, coef_low], axis=0)
        for group in range(4):
            x, y = (group >> 1) * 2 + (parity >> 1), (group & 1) * 2 + (parity & 1)
            tile = group * 4 + parity
            lanes = slice(tile * LANES, tile * LANES + LANES)
            both = jnp.dot(coef, high_ref[:, lanes], preferred_element_type=F32)
            value = both[:64] + both[64:] + jnp.dot(coef_high, low_ref[:, lanes], preferred_element_type=F32)
            hit = (row // 8 == lane // 32 % 2) & (row % 8 == group * 2 + lane // 64)
            sums = [
                jnp.sum(jnp.where(hit, value[16 * c : 16 * c + 16], 0.0), axis=0, keepdims=True) for c in range(4)
            ]
            live = live_ref[x, y : y + 1, :]
            pot_ref[x, y : y + 1, :] = (near_ref[x, y, 0:1, :] + sums[0]) * live
            for c in range(3):
                field_ref[c, x, y : y + 1, :] = (near_ref[x, y, c + 1 : c + 2, :] - sums[c + 1]) * live


VMEM = pl.BlockSpec(memory_space=pltpu.VMEM)


def shape(*dims):
    return jax.ShapeDtypeStruct(dims, F32)


def pairs_call(sizes, positions, charges, counts, exps, moment_shift):
    dma = pltpu.SemaphoreType.DMA
    return pl.pallas_call(
        functools.partial(pairs_kernel, *sizes),
        out_shape=(
            shape(4, 4, 4, LANES),
            shape(4, 4, 4, LANES),
            shape(4, 4, LANES),
            shape(4, 4, 4, 8, LANES),
            shape(27, 8, LANES),
            shape(*sizes, 1, LANES),
        ),
        in_specs=[VMEM] * 5,
        out_specs=(VMEM,) * 6,
        scratch_shapes=[
            pltpu.VMEM((6, 6, 3, 4, LANES), F32),
            pltpu.VMEM((2, 2, 2, 8, LANES), F32),
            pltpu.VMEM((8, LANES), F32),
            pltpu.VMEM((1, LANES), F32),
            pltpu.VMEM((TERMS * 8, LANES), F32),
            pltpu.VMEM((KPAD, 2048), BF16),
            pltpu.VMEM((KPAD, 2048), BF16),
            pltpu.VMEM((6, 6, 3, 4, LANES), F32),
            pltpu.VMEM((6, 6, 3, 4, SLOTS, LANES), F32),
            dma((3, 26)),
            dma((3, 26)),
            dma((40,)),
            dma((40,)),
            dma((4,)),
        ],
        compiler_params=pltpu.CompilerParams(collective_id=0, has_side_effects=True),
        name="pairs",
    )(positions, charges, counts, exps, moment_shift)


def far_call(*operands):
    return pl.pallas_call(
        far_kernel,
        out_shape=(shape(4, 4, LANES), shape(3, 4, 4, LANES)),
        in_specs=[pl.BlockSpec(memory_space=pl.ANY)] + [VMEM] * 11,
        out_specs=(VMEM,) * 2,
        scratch_shapes=[
            pltpu.VMEM((27 * 128, LANES), F32),
            pltpu.VMEM((216, 16, LANES), BF16),
            pltpu.VMEM((8, 32, LANES), F32),
            pltpu.VMEM((32, 16, LANES), BF16),
            pltpu.VMEM((144, LANES), F32),
            pltpu.VMEM((64, LANES), F32),
            pltpu.VMEM((KPAD, 2048), BF16),
            pltpu.VMEM((KPAD, 2048), BF16),
            pltpu.VMEM((TERMS * 8, LANES), F32),
            pltpu.VMEM((TERMS * 8, LANES), F32),
            pltpu.VMEM((TERMS, 25600), BF16),
            pltpu.SemaphoreType.DMA((1,)),
        ],
        name="far",
    )(*operands)


def solution(mesh):
    sizes = tuple(mesh.shape[axis] for axis in ("gx", "gy", "gz"))

    def per_device(
        positions, charges, counts, moment_shift, far_operators, local_shift, lattice_operator
    ):
        exps = jnp.asarray(exponent_planes())
        slope = jnp.asarray(slope_matrix()).astype(BF16)
        native_up = jnp.transpose(moment_shift, (1, 0, 2))
        native_down = jnp.transpose(local_shift, (1, 0, 2))
        near, data, live, wide, mids, tops = pairs_call(sizes, positions, charges, counts, exps, native_up)
        return far_call(
            far_operators,
            wide,
            mids,
            tops,
            near,
            data,
            live,
            exps,
            slope,
            native_up,
            native_down,
            lattice_operator,
        )

    placed = (
        P(None, "gx", "gy", "gz"),
        P("gx", "gy", "gz"),
        P("gx", "gy", "gz"),
        P(),
        P(),
        P(),
        P(),
    )
    return jax.shard_map(
        per_device,
        mesh=mesh,
        in_specs=placed,
        out_specs=(P("gx", "gy", "gz"), P(None, "gx", "gy", "gz")),
        check_vma=False,
    )
```

```python
import functools

import jax
import jax.numpy as jnp
import numpy as np
from jax import lax
from jax.experimental import pallas as pl
from jax.experimental.pallas import tpu as pltpu
from jax.sharding import PartitionSpec as P

ORDER = 8
SLOTS = 32
SOFTENING = 0.0625
TERMS = 81
KPAD = 96
LANES = 128
OFFSETS = 316
CHUNK = 4
MESH = pl.DeviceIdType.MESH
F32 = jnp.float32
BF16 = jnp.bfloat16


def offset_table():
    listed = []
    for shift_x in range(-3, 4):
        for shift_y in range(-3, 4):
            for shift_z in range(-3, 4):
                if max(abs(shift_x), abs(shift_y), abs(shift_z)) >= 2:
                    listed.append((shift_x, shift_y, shift_z))
    return listed


def admitted(shift):
    listed = []
    for parity in range(8):
        place = [shift[axis] + (parity >> (2 - axis) & 1) for axis in range(3)]
        if all(-2 <= c <= 3 for c in place):
            listed.append((parity, tuple(place)))
    return listed


def tile_of(place):
    around = [(c + 2) // 2 for c in place]
    inner = [(c + 2) % 2 for c in place]
    return ((around[0] * 3 + around[1]) * 3 + around[2]) * 8 + inner[0] * 4 + inner[1] * 2 + inner[2]


def offset_groups():
    groups = {}
    for index, shift in enumerate(offset_table()):
        groups.setdefault(tuple(p for p, _ in admitted(shift)), []).append(index)
    return sorted(groups.items(), key=lambda item: -len(item[0]))


TOP_ROWS = {0: 10, 7: 11, 3: 12, 4: 13, 1: 14, 6: 15}
EXTRA_TILES = {2: 216, 5: 217}


def top_parity(shift):
    if min(shift) > -3:
        return 0
    if max(shift) < 3:
        return 7
    fits = [parity for parity, _ in admitted(shift) if parity in TOP_ROWS]
    return fits[0] if fits else None


def exponent_list():
    listed = []
    for accumulated in range(ORDER + 1):
        for height in (0, 1):
            for power_x in range(accumulated - height + 1):
                listed.append((power_x, accumulated - height - power_x, height))
    return listed


def exponent_planes():
    planes = np.zeros((4, KPAD, LANES), np.int32)
    for row, (a, b, c) in enumerate(exponent_list()):
        planes[0, row], planes[1, row], planes[2, row], planes[3, row] = a, b, c, 1
    return planes


def slope_matrix():
    listed = exponent_list()
    place = {e: i for i, e in enumerate(listed)}
    matrix = np.zeros((TERMS, 3 * LANES), np.float32)
    for row, (a, b, c) in enumerate(listed):
        if a > 0:
            matrix[row, place[(a - 1, b, c)]] = a
        if b > 0:
            matrix[row, LANES + place[(a, b - 1, c)]] = b
        if c > 0:
            matrix[row, 2 * LANES + place[(a, b, c - 1)]] = c
    return matrix


def lanes_nt(lhs, rhs):
    return lax.dot_general(lhs, rhs, (((1,), (1,)), ((), ())), preferred_element_type=F32)


def halves(value):
    upper = value.astype(BF16)
    return upper, (value - upper.astype(F32)).astype(BF16)


def split_nt(value, rhs):
    rows = value.shape[0]
    if rows % 8:
        value = jnp.concatenate([value, jnp.zeros((8 - rows, value.shape[1]), F32)], axis=0)
    upper, lower = halves(value)
    both = lanes_nt(upper, rhs) + lanes_nt(lower, rhs)
    return both[:rows]


def widen(value):
    return jnp.concatenate([value, jnp.zeros((value.shape[0], LANES - value.shape[1]), F32)], axis=1)


def power_of(base, exponents):
    square = base * base
    fourth = square * square
    eighth = fourth * fourth
    result = jnp.where((exponents & 1) != 0, base, 1.0)
    result = result * jnp.where((exponents & 2) != 0, square, 1.0)
    result = result * jnp.where((exponents & 4) != 0, fourth, 1.0)
    return jnp.where(exponents == 8, eighth, result)


def monomial_tiles(rows_of, exps_ref, high_ref, low_ref):
    for tile in range(16):
        px, py, ox, oy = tile >> 3, tile >> 2 & 1, tile >> 1 & 1, tile & 1
        row_x, row_y, row_z = rows_of(2 * px + ox, 2 * py + oy)
        full = lambda row: jnp.broadcast_to(row - 0.5, (KPAD, LANES))
        value = power_of(full(row_x), exps_ref[0]) * power_of(full(row_y), exps_ref[1])
        value = value * jnp.where(exps_ref[2] != 0, full(row_z), 1.0)
        value = jnp.where(exps_ref[3] != 0, value, 0.0)
        upper, lower = halves(value)
        high_ref[:, tile * LANES : (tile + 1) * LANES] = upper
        low_ref[:, tile * LANES : (tile + 1) * LANES] = lower


def octant_operators(native_ref, rows_ref):
    rows_ref[:, :TERMS] = native_ref[...].astype(F32).reshape(TERMS * 8, TERMS)


def octant_operator(rows_ref, octant):
    return rows_ref[pl.ds(octant, TERMS, stride=8), :][:, :TERMS].astype(BF16)


def prepare(pos_ref, chg_ref, cnt_ref, data_ref, live_ref):
    counts = jnp.concatenate([cnt_ref[x] for x in range(4)], axis=0).astype(F32).astype(BF16)
    spread = (
        lax.broadcasted_iota(jnp.int32, (4, LANES), 1) // SLOTS == lax.broadcasted_iota(jnp.int32, (4, LANES), 0)
    ).astype(F32).astype(BF16)
    limit = jnp.dot(counts, spread, preferred_element_type=F32)
    slot_of = (lax.broadcasted_iota(jnp.int32, (16, LANES), 1) % SLOTS).astype(F32)
    live = (slot_of < limit).astype(F32)
    for x in range(4):
        live_ref[x] = live[4 * x : 4 * x + 4]
        for y in range(4):
            for c in range(3):
                data_ref[x, y, c : c + 1, :] = pos_ref[c, x, y : y + 1, :]
            data_ref[x, y, 3:4, :] = chg_ref[x, y : y + 1, :] * live[4 * x + y : 4 * x + y + 1]


def rows_from(data_ref):
    return lambda x, y: tuple(data_ref[x, y, c : c + 1, :] for c in range(3))


def moments(data_ref, operator_rows, leaf_ref, mid_ref, top_ref, high_ref, low_ref):
    row = lax.broadcasted_iota(jnp.int32, (16, LANES), 0)
    lane = lax.broadcasted_iota(jnp.int32, (16, LANES), 1)
    for group in range(4):
        px, py = group >> 1, group & 1
        pieces = []
        for tile in range(4):
            ox, oy = tile >> 1, tile & 1
            hit = (row // 8 == lane // 64) & (row % 8 == ox * 4 + oy * 2 + lane // 32 % 2)
            weight = jnp.broadcast_to(data_ref[2 * px + ox, 2 * py + oy, 3:4, :], (16, LANES))
            pieces.append(jnp.where(hit, weight, 0.0))
        upper, lower = halves(jnp.concatenate(pieces, axis=1))
        span = slice(group * 512, group * 512 + 512)
        both = lanes_nt(jnp.concatenate([upper, lower], axis=0), high_ref[:, span])
        total = widen(both[:16] + both[16:] + lanes_nt(upper, low_ref[:, span]))
        leaf_ref[px, py, 0] = total[:8]
        leaf_ref[px, py, 1] = total[8:]
    mid = jnp.zeros((8, TERMS), F32)
    top = jnp.zeros((8, TERMS), F32)
    which = lax.broadcasted_iota(jnp.int32, (8, TERMS), 0)
    tiles = [leaf_ref[p >> 2, p >> 1 & 1, p & 1] for p in range(8)]
    operators = [octant_operator(operator_rows, octant) for octant in range(8)]
    for octant in range(8):
        rows = jnp.concatenate([tile[octant : octant + 1] for tile in tiles], axis=0)
        mid = mid + split_nt(rows[:, :TERMS], operators[octant])
    mid_ref[...] = widen(mid)
    for octant in range(8):
        top = top + jnp.where(which == octant, split_nt(mid, operators[octant]), 0.0)
    top_ref[...] = widen(jnp.sum(top, axis=0, keepdims=True))


DIRECTIONS = [
    (dx, dy, dz) for dx in (-1, 0, 1) for dy in (-1, 0, 1) for dz in (-1, 0, 1) if (dx, dy, dz) != (0, 0, 0)
]


def span_of(step, own, first):
    if step == 0:
        return pl.ds(0, own), pl.ds(first, own)
    if step > 0:
        return pl.ds(own - 1, 1), pl.ds(first - 1, 1)
    return pl.ds(0, 1), pl.ds(first + own, 1)


def fill_cells(cells, ext_ref, turned_ref, table_ref):
    lane4 = lax.broadcasted_iota(jnp.int32, (4, LANES), 1)
    for x, y in cells:
        before, here, after = ext_ref[x, y, 0], ext_ref[x, y, 1], ext_ref[x, y, 2]
        turned_ref[x, y, 0] = pltpu.roll(jnp.where(lane4 >= 96, before, here), 32, 1)
        turned_ref[x, y, 1] = here
        turned_ref[x, y, 2] = pltpu.roll(jnp.where(lane4 < 32, after, here), 96, 1)
    lane = lax.broadcasted_iota(jnp.int32, (8, LANES), 1)
    base = lane // SLOTS * SLOTS + lax.broadcasted_iota(jnp.int32, (8, LANES), 0)

    def one_group(group, carry):
        pick = base + group * 8
        start = pl.multiple_of(group * 8, 8)
        for x, y in cells:
            for ez in range(3):
                for c in range(4):
                    row = jnp.broadcast_to(turned_ref[x, y, ez, c : c + 1, :], (8, LANES))
                    table_ref[x, y, ez, c, pl.ds(start, 8), :] = jnp.take_along_axis(row, pick, axis=1)
        return carry

    lax.fori_loop(0, 4, one_group, 0)


def load_wide(data_ref, x, y):
    mine = data_ref[x, y]
    return [jnp.broadcast_to(mine[c : c + 1], (8, LANES)) for c in range(3)]


def pair_sums(sums, here_x, here_y, here_z, x, y, table_ref):
    potential, field_x, field_y, field_z = sums
    for ez in range(3):
        for group in range(4):
            span = pl.ds(group * 8, 8)
            delta_x = here_x - table_ref[x, y, ez, 0, span, :]
            delta_y = here_y - table_ref[x, y, ez, 1, span, :]
            delta_z = here_z[ez] - table_ref[x, y, ez, 2, span, :]
            distance = delta_x * delta_x + delta_y * delta_y + (delta_z * delta_z + SOFTENING)
            inverse = lax.rsqrt(distance)
            weight = table_ref[x, y, ez, 3, span, :] * inverse
            cubic = weight * (inverse * inverse)
            potential = potential + weight
            field_x = field_x + cubic * delta_x
            field_y = field_y + cubic * delta_y
            field_z = field_z + cubic * delta_z
    return potential, field_x, field_y, field_z


def near_inside(rows, data_ref, table_ref, sums_ref):
    for y in rows:
        steps = [ey for ey in (-1, 0, 1) if 0 <= y + ey < 4]

        def along_x(x, carry):
            wide = load_wide(data_ref, x, y)
            here_z = [wide[2] - float(ez - 1) for ez in range(3)]

            def around(ex, sums):
                here_x = wide[0] - (ex - 1).astype(F32)
                for ey in steps:
                    sums = pair_sums(sums, here_x, wide[1] - float(ey), here_z, x + ex, y + ey + 1, table_ref)
                return sums

            zero = jnp.zeros((8, LANES), F32)
            low = 1 - jnp.minimum(x, 1)
            high = 2 + jnp.minimum(3 - x, 1)
            sums = lax.fori_loop(low, high, around, (zero, zero, zero, zero))
            for c in range(4):
                sums_ref[x, y, c] = sums[c]
            return carry

        lax.fori_loop(0, 4, along_x, 0)


def near_outside(data_ref, table_ref, sums_ref):
    for x, ex in ((0, -1), (3, 1)):

        def along_y(y, carry):
            wide = load_wide(data_ref, x, y)
            here_z = [wide[2] - float(ez - 1) for ez in range(3)]
            sums = tuple(sums_ref[x, y, c] for c in range(4))
            for ey in (-1, 0, 1):
                sums = pair_sums(
                    sums, wide[0] - float(ex), wide[1] - float(ey), here_z, x + ex + 1, y + ey + 1, table_ref
                )
            for c in range(4):
                sums_ref[x, y, c] = sums[c]
            return carry

        lax.fori_loop(0, 4, along_y, 0)
    for y, ey in ((0, -1), (3, 1)):
        for x in range(4):
            wide = load_wide(data_ref, x, y)
            here_z = [wide[2] - float(ez - 1) for ez in range(3)]
            sums = tuple(sums_ref[x, y, c] for c in range(4))
            for ex in (-1, 0, 1):
                if 0 <= x + ex < 4:
                    sums = pair_sums(
                        sums, wide[0] - float(ex), wide[1] - float(ey), here_z, x + ex + 1, y + ey + 1, table_ref
                    )
            for c in range(4):
                sums_ref[x, y, c] = sums[c]


def align_operators(whole_ref, aligned_ref):
    slot = 0
    for _, members in offset_groups():
        for index in members:
            begin = index * TERMS
            if begin + LANES <= whole_ref.shape[1]:
                piece = whole_ref[:, begin : begin + LANES]
            else:
                tail = whole_ref[:, begin : begin + TERMS]
                piece = jnp.concatenate([tail, jnp.zeros((TERMS, LANES - TERMS), BF16)], axis=1)
            aligned_ref[:TERMS, slot * LANES : (slot + 1) * LANES] = piece
            slot += 1


def gather_boxes(wide_ref, mids_ref, rows_ref):
    def step(n, carry):
        step_x, step_y, step_z = n // 9, n // 3 % 3, n % 3
        for octant in range(8):
            rows_ref[pl.ds(pl.multiple_of(n * 128 + octant * 16 + 8, 8), 8), :] = jnp.zeros((8, LANES), F32)
        for parent in range(8):
            px, py, pz = parent >> 2, parent >> 1 & 1, parent & 1
            rows_ref[pl.ds(n * 128 + parent, 8, stride=16), :] = wide_ref[px + step_x, py + step_y, pz + step_z]
        rows_ref[pl.ds(n * 128 + 8, 8, stride=16), :] = mids_ref[n]
        return carry

    lax.fori_loop(0, 27, step, 0)


def gather_upper(tops, tops_ref, rows_ref):
    def step(n, carry):
        step_x, step_y, step_z = n // 9, n // 3 % 3, n % 3
        far_x = lax.rem(tops[0] + step_x + 3, 4) * 2
        far_y = lax.rem(tops[1] + step_y + 1, 2) * 2
        far_z = lax.rem(tops[2] + step_z + 3, 4) * 2
        for octant in range(8):
            ox, oy, oz = octant >> 2, octant >> 1 & 1, octant & 1
            rows_ref[pl.ds(n * 128 + octant * 16 + 9, 1), :] = tops_ref[far_x + ox, far_y + oy, far_z + oz]
        return carry

    lax.fori_loop(0, 27, step, 0)


def convert_tiles(rows_ref, tiles_ref):
    def step(n, carry):
        for octant in range(8):
            start = pl.multiple_of(n * 128 + octant * 16, 16)
            tiles_ref[n * 8 + octant] = rows_ref[pl.ds(start, 16), :].astype(BF16)
        return carry

    lax.fori_loop(0, 27, step, 0)
    for tile in EXTRA_TILES.values():
        tiles_ref[tile] = rows_ref[tile * 16 : tile * 16 + 16, :].astype(BF16)


def gather_top(tops, tops_ref, upper_ref, operators, lattice_ref, turned_ref, rows_ref):
    for octant in range(8):
        ox, oy, oz = octant >> 2, octant >> 1 & 1, octant & 1
        for box in range(32):
            bx, by, bz = box >> 3, box >> 2 & 1, box & 3
            upper_ref[octant, box : box + 1, :] = tops_ref[2 * bx + ox, 2 * by + oy, 2 * bz + oz]
    coarse = jnp.zeros((32, TERMS), F32)
    for octant in range(8):
        coarse = coarse + split_nt(upper_ref[octant][:, :TERMS], operators[octant])
    lattice_term = split_nt(jnp.sum(coarse, axis=0, keepdims=True), lattice_ref[...])
    row = lax.broadcasted_iota(jnp.int32, (32, 32), 0)
    column = lax.broadcasted_iota(jnp.int32, (32, 32), 1)
    wanted = (
        (row // 8 + tops[0]) % 4 * 8 + (row // 4 % 2 + tops[1]) % 2 * 4 + (row % 4 + tops[2]) % 4
    )
    turned_ref[...] = jnp.dot(
        (wanted == column).astype(F32).astype(BF16), widen(coarse).astype(BF16), preferred_element_type=F32
    )
    for shift in offset_table():
        parity = top_parity(shift)
        source = shift[0] % 4 * 8 + shift[1] % 2 * 4 + shift[2] % 4
        if parity is not None:
            place = [shift[axis] + (parity >> (2 - axis) & 1) for axis in range(3)]
            target = tile_of(place) * 16 + TOP_ROWS[parity]
            rows_ref[target : target + 1, :] = turned_ref[source : source + 1, :]
        else:
            ((parity, place),) = admitted(shift)
            begin, target = tile_of(place) * 16, EXTRA_TILES[parity] * 16
            which = lax.broadcasted_iota(jnp.int32, (8, LANES), 0)
            lower = jnp.where(which < 2, rows_ref[begin + 8 : begin + 16, :], 0.0)
            top = jnp.broadcast_to(turned_ref[source : source + 1, :], (8, LANES))
            rows_ref[target : target + 8, :] = rows_ref[begin : begin + 8, :]
            rows_ref[target + 8 : target + 16, :] = jnp.where(which == 2, top, lower)
    return lattice_term


def far_products(tiles_ref, aligned_ref, acc_ref):
    total = [jnp.zeros((16, TERMS), F32) for _ in range(8)]
    extra = jnp.zeros((1, TERMS), F32)
    shifts = offset_table()
    slot = 0
    for parities, members in offset_groups():
        for start in range(0, len(members), CHUNK):
            part = members[start : start + CHUNK]
            special = len(parities) == 1 and parities[0] in EXTRA_TILES
            columns = []
            for index in part:
                tiles = [EXTRA_TILES[parities[0]]] if special else [tile_of(place) for _, place in admitted(shifts[index])]
                columns.append(jnp.concatenate([tiles_ref[tile] for tile in tiles], axis=0))
            data = columns[0] if len(columns) == 1 else jnp.concatenate(columns, axis=1)
            product = lanes_nt(data, aligned_ref[:TERMS, slot * LANES : (slot + len(part)) * LANES])
            slot += len(part)
            for place, parity in enumerate(parities):
                total[parity] = total[parity] + product[place * 16 : place * 16 + 16]
            if special:
                extra = extra + product[10:11]
    for parity in range(8):
        acc_ref[parity * 16 : parity * 16 + 16, :] = widen(total[parity])
    return extra


def locals_down(octant_own, acc_ref, lattice_term, down_rows, local_ref):
    own_down = jnp.where(
        lax.broadcasted_iota(jnp.int32, (TERMS * 8, LANES), 0) % 8 == octant_own, down_rows[...], 0.0
    )
    own_down = jnp.sum(own_down.reshape(TERMS, 8, LANES), axis=1)[:, :TERMS].astype(BF16)
    downs = [octant_operator(down_rows, octant) for octant in range(8)]
    far_top = lattice_term
    for parity, place in TOP_ROWS.items():
        row = parity * 16 + place
        far_top = far_top + acc_ref[row : row + 1, :][:, :TERMS]
    local_upper = 0.25 * acc_ref[pl.ds(octant_own * 16 + 9, 1), :][:, :TERMS] + split_nt(0.125 * far_top, own_down)
    upper_wide = jnp.broadcast_to(local_upper, (8, TERMS))
    which = lax.broadcasted_iota(jnp.int32, (8, TERMS), 0)
    local_mid = 0.5 * acc_ref[pl.ds(8, 8, stride=16), :][:, :TERMS]
    for octant in range(8):
        local_mid = local_mid + jnp.where(which == octant, split_nt(upper_wide, downs[octant]), 0.0)
    for octant in range(8):
        local = acc_ref[octant * 16 : octant * 16 + 8, :][:, :TERMS] + split_nt(local_mid, downs[octant])
        local_ref[octant * 8 : octant * 8 + 8, :] = widen(local)


def evaluate(local_ref, slope_ref, high_ref, low_ref, sums_ref, data_ref, live_ref, pot_ref, field_ref):
    local_leaf = local_ref[...]
    upper, lower = halves(local_leaf[:, :TERMS])
    slopes = jnp.dot(upper, slope_ref[...], preferred_element_type=F32) + jnp.dot(
        lower, slope_ref[...], preferred_element_type=F32
    )
    parts = [local_leaf] + [slopes[:, c * LANES : (c + 1) * LANES] for c in range(3)]
    split_parts = [halves(part[:, :KPAD]) for part in parts]
    row = lax.broadcasted_iota(jnp.int32, (16, LANES), 0)
    lane = lax.broadcasted_iota(jnp.int32, (16, LANES), 1)
    self_weight = lax.rsqrt(jnp.full((1, LANES), SOFTENING, F32))
    for parity in range(4):
        span = slice(parity * 16, parity * 16 + 16)
        coef_high = jnp.concatenate([part[0][span] for part in split_parts], axis=0)
        coef_low = jnp.concatenate([part[1][span] for part in split_parts], axis=0)
        coef = jnp.concatenate([coef_high, coef_low], axis=0)
        for group in range(4):
            x, y = (group >> 1) * 2 + (parity >> 1), (group & 1) * 2 + (parity & 1)
            tile = group * 4 + parity
            lanes = slice(tile * LANES, tile * LANES + LANES)
            both = jnp.dot(coef, high_ref[:, lanes], preferred_element_type=F32)
            value = both[:64] + both[64:] + jnp.dot(coef_high, low_ref[:, lanes], preferred_element_type=F32)
            hit = (row // 8 == lane // 32 % 2) & (row % 8 == group * 2 + lane // 64)
            sums = [
                jnp.sum(jnp.where(hit, value[16 * c : 16 * c + 16], 0.0), axis=0, keepdims=True) for c in range(4)
            ]
            near = [jnp.sum(sums_ref[x, y, c], axis=0, keepdims=True) for c in range(4)]
            live = live_ref[x, y : y + 1, :]
            near[0] = near[0] - data_ref[x, y, 3:4, :] * self_weight
            pot_ref[x, y : y + 1, :] = (near[0] + sums[0]) * live
            for c in range(3):
                field_ref[c, x, y : y + 1, :] = (near[c + 1] - sums[c + 1]) * live


def whole_kernel(
    nx,
    ny,
    nz,
    pos_ref,
    chg_ref,
    cnt_ref,
    exps_ref,
    slope_ref,
    up_ref,
    down_ref,
    lattice_ref,
    far_ref,
    pot_ref,
    field_ref,
    data_ref,
    live_ref,
    ext_ref,
    wide_ref,
    mids_ref,
    tops_ref,
    leaf_ref,
    mid_ref,
    top_ref,
    up_rows,
    down_rows,
    high_ref,
    low_ref,
    turned_ref,
    table_ref,
    sums_ref,
    whole_ref,
    aligned_ref,
    rows_ref,
    tiles_ref,
    upper_ref,
    coarse_ref,
    acc_ref,
    local_ref,
    send,
    recv,
    gsend,
    grecv,
    own,
):
    ix, iy, iz = lax.axis_index("gx"), lax.axis_index("gy"), lax.axis_index("gz")

    def at(dx, dy, dz):
        return {
            "gx": lax.rem(ix + (dx + nx), nx),
            "gy": lax.rem(iy + (dy + ny), ny),
            "gz": lax.rem(iz + (dz + nz), nz),
        }

    plane = [(0, b, c) for b in range(ny) for c in range(nz) if b or c]
    line = [(a, 0, 0) for a in range(1, nx)]
    wrapped = lambda step: (step[0] % nx, step[1] % ny, step[2] % nz)
    partners = sorted({wrapped(step) for step in DIRECTIONS} | set(plane) | set(line))
    barrier = pltpu.get_barrier_semaphore()
    for step in partners:
        pl.semaphore_signal(barrier, inc=1, device_id=at(*step), device_id_type=MESH)
    fetch = pltpu.make_async_copy(far_ref, whole_ref, own.at[4])
    fetch.start()

    prepare(pos_ref, chg_ref, cnt_ref, data_ref, live_ref)
    octant_operators(up_ref, up_rows)
    monomial_tiles(rows_from(data_ref), exps_ref, high_ref, low_ref)
    moments(data_ref, up_rows, leaf_ref, mid_ref, top_ref, high_ref, low_ref)

    pl.semaphore_wait(barrier, len(partners))

    def remote(src, dst, ssem, rsem, step):
        copy = pltpu.make_async_remote_copy(
            src_ref=src, dst_ref=dst, send_sem=ssem, recv_sem=rsem, device_id=at(*step), device_id_type=MESH
        )
        copy.start()
        return copy

    local = [
        pltpu.make_async_copy(data_ref, ext_ref.at[pl.ds(1, 4), pl.ds(1, 4), 1], own.at[0]),
        pltpu.make_async_copy(leaf_ref, wide_ref.at[pl.ds(1, 2), pl.ds(1, 2), pl.ds(1, 2)], own.at[1]),
        pltpu.make_async_copy(mid_ref, mids_ref.at[13], own.at[2]),
        pltpu.make_async_copy(top_ref, tops_ref.at[ix, iy, iz], own.at[3]),
    ]
    for copy in local:
        copy.start()
    halo = {}
    order = sorted(range(len(DIRECTIONS)), key=lambda i: sum(abs(d) for d in DIRECTIONS[i][:2]))
    for index in order:
        dx, dy, dz = DIRECTIONS[index]
        from_x, to_x = span_of(dx, 4, 1)
        from_y, to_y = span_of(dy, 4, 1)
        src, dst = data_ref.at[from_x, from_y], ext_ref.at[to_x, to_y, 1 - dz]
        halo[index] = remote(src, dst, send.at[0, index], recv.at[0, index], DIRECTIONS[index])
    first = [
        remote(top_ref, tops_ref.at[ix, iy, iz], gsend.at[k], grecv.at[k], step) for k, step in enumerate(plane)
    ]
    boxes = []
    for index, step in enumerate(DIRECTIONS):
        spans = [span_of(d, 2, 1) for d in step]
        src = leaf_ref.at[spans[0][0], spans[1][0], spans[2][0]]
        dst = wide_ref.at[spans[0][1], spans[1][1], spans[2][1]]
        boxes.append(remote(src, dst, send.at[1, index], recv.at[1, index], step))
        slot = ((1 - step[0]) * 3 + (1 - step[1])) * 3 + (1 - step[2])
        boxes.append(remote(mid_ref, mids_ref.at[slot], send.at[2, index], recv.at[2, index], step))

    octant_operators(down_ref, down_rows)
    fetch.wait()
    align_operators(whole_ref, aligned_ref)
    for copy in local:
        copy.wait()
    for index in order[:2]:
        halo[index].wait()
    inside = [(x, y) for x in range(1, 5) for y in range(1, 5)]
    fill_cells(inside, ext_ref, turned_ref, table_ref)
    near_inside((0, 1), data_ref, table_ref, sums_ref)
    for copy in first:
        copy.wait()
    second = [
        remote(tops_ref.at[ix], tops_ref.at[ix], gsend.at[32 + k], grecv.at[32 + k], step)
        for k, step in enumerate(line)
    ]
    near_inside((2, 3), data_ref, table_ref, sums_ref)
    for index in order[2:]:
        halo[index].wait()
    fill_cells(
        [(x, y) for x in range(6) for y in range(6) if (x, y) not in inside], ext_ref, turned_ref, table_ref
    )
    near_outside(data_ref, table_ref, sums_ref)
    for copy in boxes:
        copy.wait()
    gather_boxes(wide_ref, mids_ref, rows_ref)
    for copy in second:
        copy.wait()
    tops = (ix // 2, iy // 2, iz // 2)
    octant_own = (ix % 2) * 4 + (iy % 2) * 2 + iz % 2
    gather_upper(tops, tops_ref, rows_ref)
    operators = [octant_operator(up_rows, octant) for octant in range(8)]
    lattice_term = gather_top(tops, tops_ref, upper_ref, operators, lattice_ref, coarse_ref, rows_ref)
    convert_tiles(rows_ref, tiles_ref)
    extra = far_products(tiles_ref, aligned_ref, acc_ref)
    locals_down(octant_own, acc_ref, lattice_term + extra, down_rows, local_ref)
    evaluate(local_ref, slope_ref, high_ref, low_ref, sums_ref, data_ref, live_ref, pot_ref, field_ref)


VMEM = pl.BlockSpec(memory_space=pltpu.VMEM)


def shape(*dims):
    return jax.ShapeDtypeStruct(dims, F32)


def whole_call(sizes, *operands):
    dma = pltpu.SemaphoreType.DMA
    return pl.pallas_call(
        functools.partial(whole_kernel, *sizes),
        out_shape=(shape(4, 4, LANES), shape(3, 4, 4, LANES)),
        in_specs=[VMEM] * 8 + [pl.BlockSpec(memory_space=pl.ANY)],
        out_specs=(VMEM,) * 2,
        scratch_shapes=[
            pltpu.VMEM((4, 4, 4, LANES), F32),
            pltpu.VMEM((4, 4, LANES), F32),
            pltpu.VMEM((6, 6, 3, 4, LANES), F32),
            pltpu.VMEM((4, 4, 4, 8, LANES), F32),
            pltpu.VMEM((27, 8, LANES), F32),
            pltpu.VMEM((*sizes, 1, LANES), F32),
            pltpu.VMEM((2, 2, 2, 8, LANES), F32),
            pltpu.VMEM((8, LANES), F32),
            pltpu.VMEM((1, LANES), F32),
            pltpu.VMEM((TERMS * 8, LANES), F32),
            pltpu.VMEM((TERMS * 8, LANES), F32),
            pltpu.VMEM((KPAD, 2048), BF16),
            pltpu.VMEM((KPAD, 2048), BF16),
            pltpu.VMEM((6, 6, 3, 4, LANES), F32),
            pltpu.VMEM((6, 6, 3, 4, SLOTS, LANES), F32),
            pltpu.VMEM((4, 4, 4, 8, LANES), F32),
            pltpu.VMEM((TERMS, 25600), BF16),
            pltpu.VMEM((KPAD, OFFSETS * LANES), BF16),
            pltpu.VMEM((218 * 16, LANES), F32),
            pltpu.VMEM((218, 16, LANES), BF16),
            pltpu.VMEM((8, 32, LANES), F32),
            pltpu.VMEM((32, LANES), F32),
            pltpu.VMEM((LANES, LANES), F32),
            pltpu.VMEM((64, LANES), F32),
            dma((3, 26)),
            dma((3, 26)),
            dma((40,)),
            dma((40,)),
            dma((5,)),
        ],
        compiler_params=pltpu.CompilerParams(collective_id=0, has_side_effects=True),
        name="whole",
    )(*operands)


def solution(mesh):
    sizes = tuple(mesh.shape[axis] for axis in ("gx", "gy", "gz"))

    def per_device(
        positions, charges, counts, moment_shift, far_operators, local_shift, lattice_operator
    ):
        exps = jnp.asarray(exponent_planes())
        slope = jnp.asarray(slope_matrix()).astype(BF16)
        native_up = jnp.transpose(moment_shift, (1, 0, 2))
        native_down = jnp.transpose(local_shift, (1, 0, 2))
        return whole_call(
            sizes,
            positions,
            charges,
            counts,
            exps,
            slope,
            native_up,
            native_down,
            lattice_operator,
            far_operators,
        )

    placed = (
        P(None, "gx", "gy", "gz"),
        P("gx", "gy", "gz"),
        P("gx", "gy", "gz"),
        P(),
        P(),
        P(),
        P(),
    )
    return jax.shard_map(
        per_device,
        mesh=mesh,
        in_specs=placed,
        out_specs=(P("gx", "gy", "gz"), P(None, "gx", "gy", "gz")),
        check_vma=False,
    )
```

```python
import functools

import jax
import jax.numpy as jnp
import numpy as np
from jax import lax
from jax.experimental import pallas as pl
from jax.experimental.pallas import tpu as pltpu
from jax.sharding import PartitionSpec as P

ORDER = 8
SLOTS = 32
SOFTENING = 0.0625
TERMS = 81
KPAD = 96
LANES = 128
OFFSETS = 316
CHUNK = 4
PIECES = 4
MESH = pl.DeviceIdType.MESH
F32 = jnp.float32
BF16 = jnp.bfloat16


def offset_table():
    listed = []
    for shift_x in range(-3, 4):
        for shift_y in range(-3, 4):
            for shift_z in range(-3, 4):
                if max(abs(shift_x), abs(shift_y), abs(shift_z)) >= 2:
                    listed.append((shift_x, shift_y, shift_z))
    return listed


def admitted(shift):
    listed = []
    for parity in range(8):
        place = [shift[axis] + (parity >> (2 - axis) & 1) for axis in range(3)]
        if all(-2 <= c <= 3 for c in place):
            listed.append((parity, tuple(place)))
    return listed


def tile_of(place):
    around = [(c + 2) // 2 for c in place]
    inner = [(c + 2) % 2 for c in place]
    return ((around[0] * 3 + around[1]) * 3 + around[2]) * 8 + inner[0] * 4 + inner[1] * 2 + inner[2]


def offset_groups():
    groups = {}
    for index, shift in enumerate(offset_table()):
        groups.setdefault(tuple(p for p, _ in admitted(shift)), []).append(index)
    return sorted(groups.items(), key=lambda item: -len(item[0]))


TOP_ROWS = {0: 10, 7: 11, 3: 12, 4: 13, 1: 14, 6: 15}
EXTRA_TILES = {2: 216, 5: 217}


def top_parity(shift):
    if min(shift) > -3:
        return 0
    if max(shift) < 3:
        return 7
    fits = [parity for parity, _ in admitted(shift) if parity in TOP_ROWS]
    return fits[0] if fits else None


def exponent_list():
    listed = []
    for accumulated in range(ORDER + 1):
        for height in (0, 1):
            for power_x in range(accumulated - height + 1):
                listed.append((power_x, accumulated - height - power_x, height))
    return listed


def slope_matrix():
    listed = exponent_list()
    place = {e: i for i, e in enumerate(listed)}
    matrix = np.zeros((TERMS, 3 * LANES), np.float32)
    for row, (a, b, c) in enumerate(listed):
        if a > 0:
            matrix[row, place[(a - 1, b, c)]] = a
        if b > 0:
            matrix[row, LANES + place[(a, b - 1, c)]] = b
        if c > 0:
            matrix[row, 2 * LANES + place[(a, b, c - 1)]] = c
    return matrix


def lanes_nt(lhs, rhs):
    return lax.dot_general(lhs, rhs, (((1,), (1,)), ((), ())), preferred_element_type=F32)


def halves(value):
    upper = value.astype(BF16)
    return upper, (value - upper.astype(F32)).astype(BF16)


def split_nt(value, rhs):
    rows = value.shape[0]
    if rows % 8:
        value = jnp.concatenate([value, jnp.zeros((8 - rows, value.shape[1]), F32)], axis=0)
    size = value.shape[0]
    both = lanes_nt(jnp.concatenate(halves(value), axis=0), rhs)
    return (both[:size] + both[size:])[:rows]


def widen(value):
    return jnp.concatenate([value, jnp.zeros((value.shape[0], LANES - value.shape[1]), F32)], axis=1)


def power_of(base, exponents):
    square = base * base
    fourth = square * square
    eighth = fourth * fourth
    result = jnp.where((exponents & 1) != 0, base, 1.0)
    result = result * jnp.where((exponents & 2) != 0, square, 1.0)
    result = result * jnp.where((exponents & 4) != 0, fourth, 1.0)
    return jnp.where(exponents == 8, eighth, result)


def exponents():
    row = lax.broadcasted_iota(jnp.int32, (KPAD, LANES), 0)
    degree = jnp.zeros((KPAD, LANES), jnp.int32)
    for n in range(1, ORDER + 1):
        degree = degree + (row >= n * n).astype(jnp.int32)
    place = row - degree * degree
    height = (place > degree).astype(jnp.int32)
    power_x = place - height * (degree + 1)
    return power_x, degree - height - power_x, height, row < TERMS


def monomial_tiles(rows_of, high_ref, low_ref):
    power_x, power_y, power_z, valid = exponents()
    for tile in range(16):
        px, py, ox, oy = tile >> 3, tile >> 2 & 1, tile >> 1 & 1, tile & 1
        row_x, row_y, row_z = rows_of(2 * px + ox, 2 * py + oy)
        full = lambda row: jnp.broadcast_to(row - 0.5, (KPAD, LANES))
        value = power_of(full(row_x), power_x) * power_of(full(row_y), power_y)
        value = value * jnp.where(power_z != 0, full(row_z), 1.0)
        value = jnp.where(valid, value, 0.0)
        upper, lower = halves(value)
        high_ref[:, tile * LANES : (tile + 1) * LANES] = upper
        low_ref[:, tile * LANES : (tile + 1) * LANES] = lower


def octant_operators(native_ref, rows_ref):
    rows_ref[:, :TERMS] = native_ref[...].astype(F32).reshape(TERMS * 8, TERMS)


def octant_operator(rows_ref, octant):
    return rows_ref[pl.ds(octant, TERMS, stride=8), :][:, :TERMS].astype(BF16)


def prepare(pos_ref, chg_ref, cnt_ref, data_ref, live_ref):
    counts = jnp.concatenate([cnt_ref[x] for x in range(4)], axis=0).astype(F32).astype(BF16)
    spread = (
        lax.broadcasted_iota(jnp.int32, (4, LANES), 1) // SLOTS == lax.broadcasted_iota(jnp.int32, (4, LANES), 0)
    ).astype(F32).astype(BF16)
    limit = jnp.dot(counts, spread, preferred_element_type=F32)
    slot_of = (lax.broadcasted_iota(jnp.int32, (16, LANES), 1) % SLOTS).astype(F32)
    live = (slot_of < limit).astype(F32)
    for x in range(4):
        live_ref[x] = live[4 * x : 4 * x + 4]
        for y in range(4):
            for c in range(3):
                data_ref[x, y, c : c + 1, :] = pos_ref[c, x, y : y + 1, :]
            data_ref[x, y, 3:4, :] = chg_ref[x, y : y + 1, :] * live[4 * x + y : 4 * x + y + 1]


def rows_from(data_ref):
    return lambda x, y: tuple(data_ref[x, y, c : c + 1, :] for c in range(3))


def moments(data_ref, operator_rows, leaf_ref, mid_ref, top_ref, high_ref, low_ref):
    row = lax.broadcasted_iota(jnp.int32, (16, LANES), 0)
    lane = lax.broadcasted_iota(jnp.int32, (16, LANES), 1)
    for group in range(4):
        px, py = group >> 1, group & 1
        pieces = []
        for tile in range(4):
            ox, oy = tile >> 1, tile & 1
            hit = (row // 8 == lane // 64) & (row % 8 == ox * 4 + oy * 2 + lane // 32 % 2)
            weight = jnp.broadcast_to(data_ref[2 * px + ox, 2 * py + oy, 3:4, :], (16, LANES))
            pieces.append(jnp.where(hit, weight, 0.0))
        upper, lower = halves(jnp.concatenate(pieces, axis=1))
        span = slice(group * 512, group * 512 + 512)
        both = lanes_nt(jnp.concatenate([upper, lower], axis=0), high_ref[:, span])
        total = widen(both[:16] + both[16:] + lanes_nt(upper, low_ref[:, span]))
        leaf_ref[px, py, 0] = total[:8]
        leaf_ref[px, py, 1] = total[8:]
    mid = jnp.zeros((8, TERMS), F32)
    top = jnp.zeros((8, TERMS), F32)
    which = lax.broadcasted_iota(jnp.int32, (8, TERMS), 0)
    tiles = [leaf_ref[p >> 2, p >> 1 & 1, p & 1] for p in range(8)]
    operators = [octant_operator(operator_rows, octant) for octant in range(8)]
    for octant in range(8):
        rows = jnp.concatenate([tile[octant : octant + 1] for tile in tiles], axis=0)
        mid = mid + split_nt(rows[:, :TERMS], operators[octant])
    mid_ref[...] = widen(mid)
    for octant in range(8):
        top = top + jnp.where(which == octant, split_nt(mid, operators[octant]), 0.0)
    top_ref[...] = widen(jnp.sum(top, axis=0, keepdims=True))


DIRECTIONS = [
    (dx, dy, dz) for dx in (-1, 0, 1) for dy in (-1, 0, 1) for dz in (-1, 0, 1) if (dx, dy, dz) != (0, 0, 0)
]


def span_of(step, own, first):
    if step == 0:
        return pl.ds(0, own), pl.ds(first, own)
    if step > 0:
        return pl.ds(own - 1, 1), pl.ds(first - 1, 1)
    return pl.ds(0, 1), pl.ds(first + own, 1)


def fill_cells(cells, ext_ref, turned_ref, table_ref):
    lane4 = lax.broadcasted_iota(jnp.int32, (4, LANES), 1)
    for x, y in cells:
        before, here, after = ext_ref[x, y, 0], ext_ref[x, y, 1], ext_ref[x, y, 2]
        turned_ref[x, y, 0] = pltpu.roll(jnp.where(lane4 >= 96, before, here), 32, 1)
        turned_ref[x, y, 1] = here
        turned_ref[x, y, 2] = pltpu.roll(jnp.where(lane4 < 32, after, here), 96, 1)
    lane = lax.broadcasted_iota(jnp.int32, (8, LANES), 1)
    base = lane // SLOTS * SLOTS + lax.broadcasted_iota(jnp.int32, (8, LANES), 0)

    def one_group(group, carry):
        pick = base + group * 8
        start = pl.multiple_of(group * 8, 8)
        for x, y in cells:
            for ez in range(3):
                for c in range(4):
                    row = jnp.broadcast_to(turned_ref[x, y, ez, c : c + 1, :], (8, LANES))
                    table_ref[x, y, ez, c, pl.ds(start, 8), :] = jnp.take_along_axis(row, pick, axis=1)
        return carry

    lax.fori_loop(0, 4, one_group, 0)


def load_wide(data_ref, x, y):
    mine = data_ref[x, y]
    return [jnp.broadcast_to(mine[c : c + 1], (8, LANES)) for c in range(3)]


def pair_sums(sums, here_x, here_y, here_z, x, y, table_ref):
    potential, field_x, field_y, field_z = sums
    for ez in range(3):
        for group in range(4):
            span = pl.ds(group * 8, 8)
            delta_x = here_x - table_ref[x, y, ez, 0, span, :]
            delta_y = here_y - table_ref[x, y, ez, 1, span, :]
            delta_z = here_z[ez] - table_ref[x, y, ez, 2, span, :]
            distance = delta_x * delta_x + delta_y * delta_y + (delta_z * delta_z + SOFTENING)
            inverse = lax.rsqrt(distance)
            weight = table_ref[x, y, ez, 3, span, :] * inverse
            cubic = weight * (inverse * inverse)
            potential = potential + weight
            field_x = field_x + cubic * delta_x
            field_y = field_y + cubic * delta_y
            field_z = field_z + cubic * delta_z
    return potential, field_x, field_y, field_z


def near_inside(rows, data_ref, table_ref, sums_ref):
    for y in rows:
        steps = [ey for ey in (-1, 0, 1) if 0 <= y + ey < 4]

        def along_x(x, carry):
            wide = load_wide(data_ref, x, y)
            here_z = [wide[2] - float(ez - 1) for ez in range(3)]

            def around(ex, sums):
                here_x = wide[0] - (ex - 1).astype(F32)
                for ey in steps:
                    sums = pair_sums(sums, here_x, wide[1] - float(ey), here_z, x + ex, y + ey + 1, table_ref)
                return sums

            zero = jnp.zeros((8, LANES), F32)
            low = 1 - jnp.minimum(x, 1)
            high = 2 + jnp.minimum(3 - x, 1)
            sums = lax.fori_loop(low, high, around, (zero, zero, zero, zero))
            for c in range(4):
                sums_ref[x, y, c] = sums[c]
            return carry

        lax.fori_loop(0, 4, along_x, 0)


def near_outside(data_ref, table_ref, sums_ref):
    for x, ex in ((0, -1), (3, 1)):

        def along_y(y, carry):
            wide = load_wide(data_ref, x, y)
            here_z = [wide[2] - float(ez - 1) for ez in range(3)]
            sums = tuple(sums_ref[x, y, c] for c in range(4))
            for ey in (-1, 0, 1):
                sums = pair_sums(
                    sums, wide[0] - float(ex), wide[1] - float(ey), here_z, x + ex + 1, y + ey + 1, table_ref
                )
            for c in range(4):
                sums_ref[x, y, c] = sums[c]
            return carry

        lax.fori_loop(0, 4, along_y, 0)
    for y, ey in ((0, -1), (3, 1)):
        for x in range(4):
            wide = load_wide(data_ref, x, y)
            here_z = [wide[2] - float(ez - 1) for ez in range(3)]
            sums = tuple(sums_ref[x, y, c] for c in range(4))
            for ex in (-1, 0, 1):
                if 0 <= x + ex < 4:
                    sums = pair_sums(
                        sums, wide[0] - float(ex), wide[1] - float(ey), here_z, x + ex + 1, y + ey + 1, table_ref
                    )
            for c in range(4):
                sums_ref[x, y, c] = sums[c]


def align_operators(first, last, whole_ref, aligned_ref):
    slots = {}
    for _, members in offset_groups():
        for index in members:
            slots[index] = len(slots)
    for index in range(first, last):
        begin = index * TERMS
        if begin + LANES <= whole_ref.shape[1]:
            piece = whole_ref[:, begin : begin + LANES]
        else:
            tail = whole_ref[:, begin : begin + TERMS]
            piece = jnp.concatenate([tail, jnp.zeros((TERMS, LANES - TERMS), BF16)], axis=1)
        slot = slots[index]
        aligned_ref[:TERMS, slot * LANES : (slot + 1) * LANES] = piece


def clear_rows(rows_ref):
    def step(n, carry):
        for octant in range(8):
            rows_ref[pl.ds(pl.multiple_of(n * 128 + octant * 16 + 8, 8), 8), :] = jnp.zeros((8, LANES), F32)
        return carry

    lax.fori_loop(0, 27, step, 0)


def gather_boxes(wide_ref, mids_ref, rows_ref):
    for n in range(27):
        step_x, step_y, step_z = n // 9, n // 3 % 3, n % 3
        for parent in range(8):
            px, py, pz = parent >> 2, parent >> 1 & 1, parent & 1
            rows_ref[pl.ds(n * 128 + parent, 8, stride=16), :] = wide_ref[px + step_x, py + step_y, pz + step_z]
        rows_ref[pl.ds(n * 128 + 8, 8, stride=16), :] = mids_ref[n]


def gather_upper(tops, tops_ref, rows_ref):
    far_x = [lax.rem(tops[0] + step + 3, 4) * 2 for step in range(3)]
    far_y = [lax.rem(tops[1] + step + 1, 2) * 2 for step in range(3)]
    far_z = [lax.rem(tops[2] + step + 3, 4) * 2 for step in range(3)]
    for n in range(27):
        step_x, step_y, step_z = n // 9, n // 3 % 3, n % 3
        for octant in range(8):
            ox, oy, oz = octant >> 2, octant >> 1 & 1, octant & 1
            place = n * 128 + octant * 16 + 9
            rows_ref[place : place + 1, :] = tops_ref[far_x[step_x] + ox, far_y[step_y] + oy, far_z[step_z] + oz]


def convert_tiles(rows_ref, tiles_ref):
    for tile in range(218):
        tiles_ref[tile] = rows_ref[tile * 16 : tile * 16 + 16, :].astype(BF16)


def gather_top(tops, tops_ref, upper_ref, operators, lattice_ref, turned_ref, rows_ref):
    for octant in range(8):
        ox, oy, oz = octant >> 2, octant >> 1 & 1, octant & 1
        for box in range(32):
            bx, by, bz = box >> 3, box >> 2 & 1, box & 3
            upper_ref[octant, box : box + 1, :] = tops_ref[2 * bx + ox, 2 * by + oy, 2 * bz + oz]
    coarse = jnp.zeros((32, TERMS), F32)
    for octant in range(8):
        coarse = coarse + split_nt(upper_ref[octant][:, :TERMS], operators[octant])
    lattice_term = split_nt(jnp.sum(coarse, axis=0, keepdims=True), lattice_ref[...])
    row = lax.broadcasted_iota(jnp.int32, (32, 32), 0)
    column = lax.broadcasted_iota(jnp.int32, (32, 32), 1)
    wanted = (
        (row // 8 + tops[0]) % 4 * 8 + (row // 4 % 2 + tops[1]) % 2 * 4 + (row % 4 + tops[2]) % 4
    )
    turned_ref[...] = jnp.dot(
        (wanted == column).astype(F32).astype(BF16), widen(coarse).astype(BF16), preferred_element_type=F32
    )
    for shift in offset_table():
        parity = top_parity(shift)
        source = shift[0] % 4 * 8 + shift[1] % 2 * 4 + shift[2] % 4
        if parity is not None:
            place = [shift[axis] + (parity >> (2 - axis) & 1) for axis in range(3)]
            target = tile_of(place) * 16 + TOP_ROWS[parity]
            rows_ref[target : target + 1, :] = turned_ref[source : source + 1, :]
        else:
            ((parity, place),) = admitted(shift)
            begin, target = tile_of(place) * 16, EXTRA_TILES[parity] * 16
            which = lax.broadcasted_iota(jnp.int32, (8, LANES), 0)
            lower = jnp.where(which < 2, rows_ref[begin + 8 : begin + 16, :], 0.0)
            top = jnp.broadcast_to(turned_ref[source : source + 1, :], (8, LANES))
            rows_ref[target : target + 8, :] = rows_ref[begin : begin + 8, :]
            rows_ref[target + 8 : target + 16, :] = jnp.where(which == 2, top, lower)
    return lattice_term


def far_products(tiles_ref, aligned_ref, acc_ref):
    total = [jnp.zeros((16, TERMS), F32) for _ in range(8)]
    extra = jnp.zeros((1, TERMS), F32)
    shifts = offset_table()
    slot = 0
    for parities, members in offset_groups():
        for start in range(0, len(members), CHUNK):
            part = members[start : start + CHUNK]
            special = len(parities) == 1 and parities[0] in EXTRA_TILES
            columns = []
            for index in part:
                tiles = [EXTRA_TILES[parities[0]]] if special else [tile_of(place) for _, place in admitted(shifts[index])]
                columns.append(jnp.concatenate([tiles_ref[tile] for tile in tiles], axis=0))
            data = columns[0] if len(columns) == 1 else jnp.concatenate(columns, axis=1)
            product = lanes_nt(data, aligned_ref[:TERMS, slot * LANES : (slot + len(part)) * LANES])
            slot += len(part)
            for place, parity in enumerate(parities):
                total[parity] = total[parity] + product[place * 16 : place * 16 + 16]
            if special:
                extra = extra + product[10:11]
    for parity in range(8):
        acc_ref[parity * 16 : parity * 16 + 16, :] = widen(total[parity])
    return extra


def down_operators(octant_own, down_rows, downs_ref):
    own = jnp.where(
        lax.broadcasted_iota(jnp.int32, (TERMS * 8, LANES), 0) % 8 == octant_own, down_rows[...], 0.0
    )
    downs_ref[8, :TERMS, :] = jnp.sum(own.reshape(TERMS, 8, LANES), axis=1).astype(BF16)
    for octant in range(8):
        downs_ref[octant, :TERMS, :TERMS] = octant_operator(down_rows, octant)


def locals_down(octant_own, acc_ref, lattice_term, downs_ref, local_ref):
    far_top = lattice_term
    for parity, place in TOP_ROWS.items():
        row = parity * 16 + place
        far_top = far_top + acc_ref[row : row + 1, :][:, :TERMS]
    operator = lambda octant: downs_ref[octant, :TERMS, :TERMS]
    local_upper = 0.25 * acc_ref[pl.ds(octant_own * 16 + 9, 1), :][:, :TERMS] + split_nt(
        0.125 * far_top, operator(8)
    )
    upper_wide = jnp.broadcast_to(local_upper, (8, TERMS))
    which = lax.broadcasted_iota(jnp.int32, (8, TERMS), 0)
    local_mid = 0.5 * acc_ref[pl.ds(8, 8, stride=16), :][:, :TERMS]
    for octant in range(8):
        local_mid = local_mid + jnp.where(which == octant, split_nt(upper_wide, operator(octant)), 0.0)
    for octant in range(8):
        local = acc_ref[octant * 16 : octant * 16 + 8, :][:, :TERMS] + split_nt(local_mid, operator(octant))
        local_ref[octant * 8 : octant * 8 + 8, :] = widen(local)


def evaluate(local_ref, slope_ref, high_ref, low_ref, sums_ref, data_ref, live_ref, pot_ref, field_ref):
    local_leaf = local_ref[...]
    upper, lower = halves(local_leaf[:, :TERMS])
    slopes = jnp.dot(upper, slope_ref[...], preferred_element_type=F32) + jnp.dot(
        lower, slope_ref[...], preferred_element_type=F32
    )
    parts = [local_leaf] + [slopes[:, c * LANES : (c + 1) * LANES] for c in range(3)]
    split_parts = [halves(part[:, :KPAD]) for part in parts]
    row = lax.broadcasted_iota(jnp.int32, (16, LANES), 0)
    lane = lax.broadcasted_iota(jnp.int32, (16, LANES), 1)
    self_weight = lax.rsqrt(jnp.full((1, LANES), SOFTENING, F32))
    for parity in range(4):
        span = slice(parity * 16, parity * 16 + 16)
        coef_high = jnp.concatenate([part[0][span] for part in split_parts], axis=0)
        coef_low = jnp.concatenate([part[1][span] for part in split_parts], axis=0)
        coef = jnp.concatenate([coef_high, coef_low], axis=0)
        for group in range(4):
            x, y = (group >> 1) * 2 + (parity >> 1), (group & 1) * 2 + (parity & 1)
            tile = group * 4 + parity
            lanes = slice(tile * LANES, tile * LANES + LANES)
            both = jnp.dot(coef, high_ref[:, lanes], preferred_element_type=F32)
            value = both[:64] + both[64:] + jnp.dot(coef_high, low_ref[:, lanes], preferred_element_type=F32)
            hit = (row // 8 == lane // 32 % 2) & (row % 8 == group * 2 + lane // 64)
            sums = [
                jnp.sum(jnp.where(hit, value[16 * c : 16 * c + 16], 0.0), axis=0, keepdims=True) for c in range(4)
            ]
            near = [jnp.sum(sums_ref[x, y, c], axis=0, keepdims=True) for c in range(4)]
            live = live_ref[x, y : y + 1, :]
            near[0] = near[0] - data_ref[x, y, 3:4, :] * self_weight
            pot_ref[x, y : y + 1, :] = (near[0] + sums[0]) * live
            for c in range(3):
                field_ref[c, x, y : y + 1, :] = (near[c + 1] - sums[c + 1]) * live


def whole_kernel(
    nx,
    ny,
    nz,
    pos_hbm,
    chg_hbm,
    cnt_hbm,
    up_hbm,
    down_hbm,
    slope_hbm,
    lattice_hbm,
    far_hbm,
    pot_ref,
    field_ref,
    pos_ref,
    chg_ref,
    cnt_ref,
    up_ref,
    down_ref,
    slope_ref,
    lattice_ref,
    data_ref,
    live_ref,
    ext_ref,
    wide_ref,
    mids_ref,
    tops_ref,
    leaf_ref,
    mid_ref,
    top_ref,
    up_rows,
    down_rows,
    downs_ref,
    high_ref,
    low_ref,
    turned_ref,
    table_ref,
    sums_ref,
    whole_ref,
    aligned_ref,
    rows_ref,
    tiles_ref,
    upper_ref,
    coarse_ref,
    acc_ref,
    local_ref,
    send,
    recv,
    gsend,
    grecv,
    own,
    load,
):
    ix, iy, iz = lax.axis_index("gx"), lax.axis_index("gy"), lax.axis_index("gz")

    def at(dx, dy, dz):
        return {
            "gx": lax.rem(ix + (dx + nx), nx),
            "gy": lax.rem(iy + (dy + ny), ny),
            "gz": lax.rem(iz + (dz + nz), nz),
        }

    plane = [(0, b, c) for b in range(ny) for c in range(nz) if b or c]
    line = [(a, 0, 0) for a in range(1, nx)]
    wrapped = lambda step: (step[0] % nx, step[1] % ny, step[2] % nz)
    partners = sorted({wrapped(step) for step in DIRECTIONS} | set(plane) | set(line))
    barrier = pltpu.get_barrier_semaphore()
    for step in partners:
        pl.semaphore_signal(barrier, inc=1, device_id=at(*step), device_id_type=MESH)
    operands = ((pos_hbm, pos_ref), (chg_hbm, chg_ref), (cnt_hbm, cnt_ref), (up_hbm, up_ref))
    operands += ((down_hbm, down_ref), (slope_hbm, slope_ref), (lattice_hbm, lattice_ref))
    loads = [pltpu.make_async_copy(src, dst, load.at[k]) for k, (src, dst) in enumerate(operands)]
    pieces = []
    for k in range(PIECES):
        span = pl.ds(k * (25600 // PIECES), 25600 // PIECES)
        pieces.append(pltpu.make_async_copy(far_hbm.at[:, span], whole_ref.at[:, span], load.at[7 + k]))
    for copy in loads + pieces:
        copy.start()
    octant_own = (ix % 2) * 4 + (iy % 2) * 2 + iz % 2
    for copy in loads[:4]:
        copy.wait()

    prepare(pos_ref, chg_ref, cnt_ref, data_ref, live_ref)
    octant_operators(up_ref, up_rows)
    monomial_tiles(rows_from(data_ref), high_ref, low_ref)
    moments(data_ref, up_rows, leaf_ref, mid_ref, top_ref, high_ref, low_ref)

    pl.semaphore_wait(barrier, len(partners))

    def remote(src, dst, ssem, rsem, step):
        copy = pltpu.make_async_remote_copy(
            src_ref=src, dst_ref=dst, send_sem=ssem, recv_sem=rsem, device_id=at(*step), device_id_type=MESH
        )
        copy.start()
        return copy

    local = [
        pltpu.make_async_copy(data_ref, ext_ref.at[pl.ds(1, 4), pl.ds(1, 4), 1], own.at[0]),
        pltpu.make_async_copy(leaf_ref, wide_ref.at[pl.ds(1, 2), pl.ds(1, 2), pl.ds(1, 2)], own.at[1]),
        pltpu.make_async_copy(mid_ref, mids_ref.at[13], own.at[2]),
        pltpu.make_async_copy(top_ref, tops_ref.at[ix, iy, iz], own.at[3]),
    ]
    for copy in local:
        copy.start()
    halo = {}
    order = sorted(range(len(DIRECTIONS)), key=lambda i: sum(abs(d) for d in DIRECTIONS[i][:2]))
    for index in order:
        dx, dy, dz = DIRECTIONS[index]
        from_x, to_x = span_of(dx, 4, 1)
        from_y, to_y = span_of(dy, 4, 1)
        src, dst = data_ref.at[from_x, from_y], ext_ref.at[to_x, to_y, 1 - dz]
        halo[index] = remote(src, dst, send.at[0, index], recv.at[0, index], DIRECTIONS[index])
    first = [
        remote(top_ref, tops_ref.at[ix, iy, iz], gsend.at[k], grecv.at[k], step) for k, step in enumerate(plane)
    ]
    boxes = []
    for index, step in enumerate(DIRECTIONS):
        spans = [span_of(d, 2, 1) for d in step]
        src = leaf_ref.at[spans[0][0], spans[1][0], spans[2][0]]
        dst = wide_ref.at[spans[0][1], spans[1][1], spans[2][1]]
        boxes.append(remote(src, dst, send.at[1, index], recv.at[1, index], step))
        slot = ((1 - step[0]) * 3 + (1 - step[1])) * 3 + (1 - step[2])
        boxes.append(remote(mid_ref, mids_ref.at[slot], send.at[2, index], recv.at[2, index], step))

    for copy in loads[4:]:
        copy.wait()
    octant_operators(down_ref, down_rows)
    down_operators(octant_own, down_rows, downs_ref)
    clear_rows(rows_ref)
    done = 0
    for k in range(PIECES):
        pieces[k].wait()
        ready = OFFSETS if k == PIECES - 1 else ((k + 1) * (25600 // PIECES) - LANES) // TERMS
        align_operators(done, ready, whole_ref, aligned_ref)
        done = ready
    for copy in local:
        copy.wait()
    for index in order[:2]:
        halo[index].wait()
    inside = [(x, y) for x in range(1, 5) for y in range(1, 5)]
    fill_cells(inside, ext_ref, turned_ref, table_ref)
    near_inside((0, 1), data_ref, table_ref, sums_ref)
    for copy in first:
        copy.wait()
    second = [
        remote(tops_ref.at[ix], tops_ref.at[ix], gsend.at[32 + k], grecv.at[32 + k], step)
        for k, step in enumerate(line)
    ]
    near_inside((2, 3), data_ref, table_ref, sums_ref)
    for index in order[2:]:
        halo[index].wait()
    fill_cells(
        [(x, y) for x in range(6) for y in range(6) if (x, y) not in inside], ext_ref, turned_ref, table_ref
    )
    near_outside(data_ref, table_ref, sums_ref)
    for copy in boxes:
        copy.wait()
    gather_boxes(wide_ref, mids_ref, rows_ref)
    for copy in second:
        copy.wait()
    tops = (ix // 2, iy // 2, iz // 2)
    gather_upper(tops, tops_ref, rows_ref)
    operators = [octant_operator(up_rows, octant) for octant in range(8)]
    lattice_term = gather_top(tops, tops_ref, upper_ref, operators, lattice_ref, coarse_ref, rows_ref)
    convert_tiles(rows_ref, tiles_ref)
    extra = far_products(tiles_ref, aligned_ref, acc_ref)
    locals_down(octant_own, acc_ref, lattice_term + extra, downs_ref, local_ref)
    evaluate(local_ref, slope_ref, high_ref, low_ref, sums_ref, data_ref, live_ref, pot_ref, field_ref)


VMEM = pl.BlockSpec(memory_space=pltpu.VMEM)


def shape(*dims):
    return jax.ShapeDtypeStruct(dims, F32)


def whole_call(sizes, *operands):
    dma = pltpu.SemaphoreType.DMA
    return pl.pallas_call(
        functools.partial(whole_kernel, *sizes),
        out_shape=(shape(4, 4, LANES), shape(3, 4, 4, LANES)),
        in_specs=[pl.BlockSpec(memory_space=pltpu.HBM)] * 8,
        out_specs=(VMEM,) * 2,
        scratch_shapes=[
            pltpu.VMEM((3, 4, 4, LANES), F32),
            pltpu.VMEM((4, 4, LANES), F32),
            pltpu.VMEM((4, 4, 4), jnp.int32),
            pltpu.VMEM((TERMS, 8, TERMS), BF16),
            pltpu.VMEM((TERMS, 8, TERMS), BF16),
            pltpu.VMEM((TERMS, 3 * LANES), BF16),
            pltpu.VMEM((TERMS, TERMS), BF16),
            pltpu.VMEM((4, 4, 4, LANES), F32),
            pltpu.VMEM((4, 4, LANES), F32),
            pltpu.VMEM((6, 6, 3, 4, LANES), F32),
            pltpu.VMEM((4, 4, 4, 8, LANES), F32),
            pltpu.VMEM((27, 8, LANES), F32),
            pltpu.VMEM((*sizes, 1, LANES), F32),
            pltpu.VMEM((2, 2, 2, 8, LANES), F32),
            pltpu.VMEM((8, LANES), F32),
            pltpu.VMEM((1, LANES), F32),
            pltpu.VMEM((TERMS * 8, LANES), F32),
            pltpu.VMEM((TERMS * 8, LANES), F32),
            pltpu.VMEM((9, KPAD, LANES), BF16),
            pltpu.VMEM((KPAD, 2048), BF16),
            pltpu.VMEM((KPAD, 2048), BF16),
            pltpu.VMEM((6, 6, 3, 4, LANES), F32),
            pltpu.VMEM((6, 6, 3, 4, SLOTS, LANES), F32),
            pltpu.VMEM((4, 4, 4, 8, LANES), F32),
            pltpu.VMEM((TERMS, 25600), BF16),
            pltpu.VMEM((KPAD, OFFSETS * LANES), BF16),
            pltpu.VMEM((218 * 16, LANES), F32),
            pltpu.VMEM((218, 16, LANES), BF16),
            pltpu.VMEM((8, 32, LANES), F32),
            pltpu.VMEM((32, LANES), F32),
            pltpu.VMEM((LANES, LANES), F32),
            pltpu.VMEM((64, LANES), F32),
            dma((3, 26)),
            dma((3, 26)),
            dma((40,)),
            dma((40,)),
            dma((4,)),
            dma((7 + PIECES,)),
        ],
        compiler_params=pltpu.CompilerParams(
            collective_id=0, has_side_effects=True, vmem_limit_bytes=56000000
        ),
        name="whole",
    )(*operands)


def solution(mesh):
    sizes = tuple(mesh.shape[axis] for axis in ("gx", "gy", "gz"))

    def per_device(
        positions, charges, counts, moment_shift, far_operators, local_shift, lattice_operator
    ):
        slope = jnp.asarray(slope_matrix()).astype(BF16)
        native_up = jnp.transpose(moment_shift, (1, 0, 2))
        native_down = jnp.transpose(local_shift, (1, 0, 2))
        return whole_call(
            sizes,
            positions,
            charges,
            counts,
            native_up,
            native_down,
            slope,
            lattice_operator,
            far_operators,
        )

    placed = (
        P(None, "gx", "gy", "gz"),
        P("gx", "gy", "gz"),
        P("gx", "gy", "gz"),
        P(),
        P(),
        P(),
        P(),
    )
    return jax.shard_map(
        per_device,
        mesh=mesh,
        in_specs=placed,
        out_specs=(P("gx", "gy", "gz"), P(None, "gx", "gy", "gz")),
        check_vma=False,
    )
```

```python
import functools

import jax
import jax.numpy as jnp
import numpy as np
from jax import lax
from jax.experimental import pallas as pl
from jax.experimental.pallas import tpu as pltpu
from jax.sharding import PartitionSpec as P

ORDER = 8
SLOTS = 32
SOFTENING = 0.0625
TERMS = 81
KPAD = 96
LANES = 128
OFFSETS = 316
CHUNK = 4
PIECES = 4
MESH = pl.DeviceIdType.MESH
F32 = jnp.float32
BF16 = jnp.bfloat16


def offset_table():
    listed = []
    for shift_x in range(-3, 4):
        for shift_y in range(-3, 4):
            for shift_z in range(-3, 4):
                if max(abs(shift_x), abs(shift_y), abs(shift_z)) >= 2:
                    listed.append((shift_x, shift_y, shift_z))
    return listed


def admitted(shift):
    listed = []
    for parity in range(8):
        place = [shift[axis] + (parity >> (2 - axis) & 1) for axis in range(3)]
        if all(-2 <= c <= 3 for c in place):
            listed.append((parity, tuple(place)))
    return listed


def tile_of(place):
    around = [(c + 2) // 2 for c in place]
    inner = [(c + 2) % 2 for c in place]
    return ((around[0] * 3 + around[1]) * 3 + around[2]) * 8 + inner[0] * 4 + inner[1] * 2 + inner[2]


def offset_groups():
    groups = {}
    for index, shift in enumerate(offset_table()):
        groups.setdefault(tuple(p for p, _ in admitted(shift)), []).append(index)
    return sorted(groups.items(), key=lambda item: -len(item[0]))


TOP_ROWS = {0: 10, 7: 11, 3: 12, 4: 13, 1: 14, 6: 15}
EXTRA_TILES = {2: 216, 5: 217}


def top_parity(shift):
    if min(shift) > -3:
        return 0
    if max(shift) < 3:
        return 7
    fits = [parity for parity, _ in admitted(shift) if parity in TOP_ROWS]
    return fits[0] if fits else None


def exponent_list():
    listed = []
    for accumulated in range(ORDER + 1):
        for height in (0, 1):
            for power_x in range(accumulated - height + 1):
                listed.append((power_x, accumulated - height - power_x, height))
    return listed


def slope_matrix():
    listed = exponent_list()
    place = {e: i for i, e in enumerate(listed)}
    matrix = np.zeros((TERMS, 3 * LANES), np.float32)
    for row, (a, b, c) in enumerate(listed):
        if a > 0:
            matrix[row, place[(a - 1, b, c)]] = a
        if b > 0:
            matrix[row, LANES + place[(a, b - 1, c)]] = b
        if c > 0:
            matrix[row, 2 * LANES + place[(a, b, c - 1)]] = c
    return matrix


def lanes_nt(lhs, rhs):
    return lax.dot_general(lhs, rhs, (((1,), (1,)), ((), ())), preferred_element_type=F32)


def halves(value):
    upper = value.astype(BF16)
    return upper, (value - upper.astype(F32)).astype(BF16)


def split_nt(value, rhs):
    rows = value.shape[0]
    if rows % 8:
        value = jnp.concatenate([value, jnp.zeros((8 - rows, value.shape[1]), F32)], axis=0)
    size = value.shape[0]
    both = lanes_nt(jnp.concatenate(halves(value), axis=0), rhs)
    return (both[:size] + both[size:])[:rows]


def widen(value):
    return jnp.concatenate([value, jnp.zeros((value.shape[0], LANES - value.shape[1]), F32)], axis=1)


def power_of(base, exponents):
    square = base * base
    fourth = square * square
    eighth = fourth * fourth
    result = jnp.where((exponents & 1) != 0, base, 1.0)
    result = result * jnp.where((exponents & 2) != 0, square, 1.0)
    result = result * jnp.where((exponents & 4) != 0, fourth, 1.0)
    return jnp.where(exponents == 8, eighth, result)


def exponents():
    row = lax.broadcasted_iota(jnp.int32, (KPAD, LANES), 0)
    degree = jnp.zeros((KPAD, LANES), jnp.int32)
    for n in range(1, ORDER + 1):
        degree = degree + (row >= n * n).astype(jnp.int32)
    place = row - degree * degree
    height = (place > degree).astype(jnp.int32)
    power_x = place - height * (degree + 1)
    return power_x, degree - height - power_x, height, row < TERMS


def monomial_tiles(rows_of, high_ref, low_ref):
    power_x, power_y, power_z, valid = exponents()
    for tile in range(16):
        px, py, ox, oy = tile >> 3, tile >> 2 & 1, tile >> 1 & 1, tile & 1
        row_x, row_y, row_z = rows_of(2 * px + ox, 2 * py + oy)
        full = lambda row: jnp.broadcast_to(row - 0.5, (KPAD, LANES))
        value = power_of(full(row_x), power_x) * power_of(full(row_y), power_y)
        value = value * jnp.where(power_z != 0, full(row_z), 1.0)
        value = jnp.where(valid, value, 0.0)
        upper, lower = halves(value)
        high_ref[:, tile * LANES : (tile + 1) * LANES] = upper
        low_ref[:, tile * LANES : (tile + 1) * LANES] = lower


def octant_operators(native_ref, rows_ref):
    rows_ref[:, :TERMS] = native_ref[...].astype(F32).reshape(TERMS * 8, TERMS)


def octant_operator(rows_ref, octant):
    return rows_ref[pl.ds(octant, TERMS, stride=8), :][:, :TERMS].astype(BF16)


def prepare(pos_ref, chg_ref, cnt_ref, data_ref, live_ref):
    counts = jnp.concatenate([cnt_ref[x] for x in range(4)], axis=0).astype(F32).astype(BF16)
    spread = (
        lax.broadcasted_iota(jnp.int32, (4, LANES), 1) // SLOTS == lax.broadcasted_iota(jnp.int32, (4, LANES), 0)
    ).astype(F32).astype(BF16)
    limit = jnp.dot(counts, spread, preferred_element_type=F32)
    slot_of = (lax.broadcasted_iota(jnp.int32, (16, LANES), 1) % SLOTS).astype(F32)
    live = (slot_of < limit).astype(F32)
    for x in range(4):
        live_ref[x] = live[4 * x : 4 * x + 4]
        for y in range(4):
            for c in range(3):
                data_ref[x, y, c : c + 1, :] = pos_ref[c, x, y : y + 1, :]
            data_ref[x, y, 3:4, :] = chg_ref[x, y : y + 1, :] * live[4 * x + y : 4 * x + y + 1]


def rows_from(data_ref):
    return lambda x, y: tuple(data_ref[x, y, c : c + 1, :] for c in range(3))


def moments(data_ref, operator_rows, leaf_ref, mid_ref, top_ref, high_ref, low_ref):
    row = lax.broadcasted_iota(jnp.int32, (16, LANES), 0)
    lane = lax.broadcasted_iota(jnp.int32, (16, LANES), 1)
    for group in range(4):
        px, py = group >> 1, group & 1
        pieces = []
        for tile in range(4):
            ox, oy = tile >> 1, tile & 1
            hit = (row // 8 == lane // 64) & (row % 8 == ox * 4 + oy * 2 + lane // 32 % 2)
            weight = jnp.broadcast_to(data_ref[2 * px + ox, 2 * py + oy, 3:4, :], (16, LANES))
            pieces.append(jnp.where(hit, weight, 0.0))
        upper, lower = halves(jnp.concatenate(pieces, axis=1))
        span = slice(group * 512, group * 512 + 512)
        both = lanes_nt(jnp.concatenate([upper, lower], axis=0), high_ref[:, span])
        total = widen(both[:16] + both[16:] + lanes_nt(upper, low_ref[:, span]))
        leaf_ref[px, py, 0] = total[:8]
        leaf_ref[px, py, 1] = total[8:]
    mid = jnp.zeros((8, TERMS), F32)
    top = jnp.zeros((8, TERMS), F32)
    which = lax.broadcasted_iota(jnp.int32, (8, TERMS), 0)
    tiles = [leaf_ref[p >> 2, p >> 1 & 1, p & 1] for p in range(8)]
    operators = [octant_operator(operator_rows, octant) for octant in range(8)]
    for octant in range(8):
        rows = jnp.concatenate([tile[octant : octant + 1] for tile in tiles], axis=0)
        mid = mid + split_nt(rows[:, :TERMS], operators[octant])
    mid_ref[...] = widen(mid)
    for octant in range(8):
        top = top + jnp.where(which == octant, split_nt(mid, operators[octant]), 0.0)
    top_ref[...] = widen(jnp.sum(top, axis=0, keepdims=True))


DIRECTIONS = [
    (dx, dy, dz) for dx in (-1, 0, 1) for dy in (-1, 0, 1) for dz in (-1, 0, 1) if (dx, dy, dz) != (0, 0, 0)
]


def span_of(step, own, first):
    if step == 0:
        return pl.ds(0, own), pl.ds(first, own)
    if step > 0:
        return pl.ds(own - 1, 1), pl.ds(first - 1, 1)
    return pl.ds(0, 1), pl.ds(first + own, 1)


def fill_cells(cells, ext_ref, turned_ref, table_ref):
    lane4 = lax.broadcasted_iota(jnp.int32, (4, LANES), 1)
    for x, y in cells:
        before, here, after = ext_ref[x, y, 0], ext_ref[x, y, 1], ext_ref[x, y, 2]
        turned_ref[x, y, 0] = pltpu.roll(jnp.where(lane4 >= 96, before, here), 32, 1)
        turned_ref[x, y, 1] = here
        turned_ref[x, y, 2] = pltpu.roll(jnp.where(lane4 < 32, after, here), 96, 1)
    lane = lax.broadcasted_iota(jnp.int32, (8, LANES), 1)
    base = lane // SLOTS * SLOTS + lax.broadcasted_iota(jnp.int32, (8, LANES), 0)

    def one_group(group, carry):
        pick = base + group * 8
        start = pl.multiple_of(group * 8, 8)
        for x, y in cells:
            for ez in range(3):
                for c in range(4):
                    row = jnp.broadcast_to(turned_ref[x, y, ez, c : c + 1, :], (8, LANES))
                    table_ref[x, y, ez, c, pl.ds(start, 8), :] = jnp.take_along_axis(row, pick, axis=1)
        return carry

    lax.fori_loop(0, 4, one_group, 0)


def load_wide(data_ref, x, y):
    mine = data_ref[x, y]
    return [jnp.broadcast_to(mine[c : c + 1], (8, LANES)) for c in range(3)]


def pair_sums(sums, here_x, here_y, here_z, x, y, table_ref):
    potential, field_x, field_y, field_z = sums
    for ez in range(3):
        for group in range(4):
            span = pl.ds(group * 8, 8)
            delta_x = here_x - table_ref[x, y, ez, 0, span, :]
            delta_y = here_y - table_ref[x, y, ez, 1, span, :]
            delta_z = here_z[ez] - table_ref[x, y, ez, 2, span, :]
            distance = delta_x * delta_x + delta_y * delta_y + (delta_z * delta_z + SOFTENING)
            inverse = lax.rsqrt(distance)
            weight = table_ref[x, y, ez, 3, span, :] * inverse
            cubic = weight * (inverse * inverse)
            potential = potential + weight
            field_x = field_x + cubic * delta_x
            field_y = field_y + cubic * delta_y
            field_z = field_z + cubic * delta_z
    return potential, field_x, field_y, field_z


def near_inside(rows, data_ref, table_ref, sums_ref):
    for y in rows:
        steps = [ey for ey in (-1, 0, 1) if 0 <= y + ey < 4]

        def along_x(x, carry):
            wide = load_wide(data_ref, x, y)
            here_z = [wide[2] - float(ez - 1) for ez in range(3)]

            def around(ex, sums):
                here_x = wide[0] - (ex - 1).astype(F32)
                for ey in steps:
                    sums = pair_sums(sums, here_x, wide[1] - float(ey), here_z, x + ex, y + ey + 1, table_ref)
                return sums

            zero = jnp.zeros((8, LANES), F32)
            low = 1 - jnp.minimum(x, 1)
            high = 2 + jnp.minimum(3 - x, 1)
            sums = lax.fori_loop(low, high, around, (zero, zero, zero, zero))
            for c in range(4):
                sums_ref[x, y, c] = sums[c]
            return carry

        lax.fori_loop(0, 4, along_x, 0)


def near_outside(data_ref, table_ref, sums_ref):
    for x, ex in ((0, -1), (3, 1)):

        def along_y(y, carry):
            wide = load_wide(data_ref, x, y)
            here_z = [wide[2] - float(ez - 1) for ez in range(3)]
            sums = tuple(sums_ref[x, y, c] for c in range(4))
            for ey in (-1, 0, 1):
                sums = pair_sums(
                    sums, wide[0] - float(ex), wide[1] - float(ey), here_z, x + ex + 1, y + ey + 1, table_ref
                )
            for c in range(4):
                sums_ref[x, y, c] = sums[c]
            return carry

        lax.fori_loop(0, 4, along_y, 0)
    for y, ey in ((0, -1), (3, 1)):
        for x in range(4):
            wide = load_wide(data_ref, x, y)
            here_z = [wide[2] - float(ez - 1) for ez in range(3)]
            sums = tuple(sums_ref[x, y, c] for c in range(4))
            for ex in (-1, 0, 1):
                if 0 <= x + ex < 4:
                    sums = pair_sums(
                        sums, wide[0] - float(ex), wide[1] - float(ey), here_z, x + ex + 1, y + ey + 1, table_ref
                    )
            for c in range(4):
                sums_ref[x, y, c] = sums[c]


def align_operators(first, last, whole_ref, aligned_ref):
    slots = {}
    for _, members in offset_groups():
        for index in members:
            slots[index] = len(slots)
    for index in range(first, last):
        begin = index * TERMS
        if begin + LANES <= whole_ref.shape[1]:
            piece = whole_ref[:, begin : begin + LANES]
        else:
            tail = whole_ref[:, begin : begin + TERMS]
            piece = jnp.concatenate([tail, jnp.zeros((TERMS, LANES - TERMS), BF16)], axis=1)
        slot = slots[index]
        aligned_ref[:TERMS, slot * LANES : (slot + 1) * LANES] = piece


def clear_rows(rows_ref):
    def step(n, carry):
        for octant in range(8):
            rows_ref[pl.ds(pl.multiple_of(n * 128 + octant * 16 + 8, 8), 8), :] = jnp.zeros((8, LANES), F32)
        return carry

    lax.fori_loop(0, 27, step, 0)


def gather_boxes(wide_ref, mids_ref, rows_ref):
    for n in range(27):
        step_x, step_y, step_z = n // 9, n // 3 % 3, n % 3
        for parent in range(8):
            px, py, pz = parent >> 2, parent >> 1 & 1, parent & 1
            rows_ref[pl.ds(n * 128 + parent, 8, stride=16), :] = wide_ref[px + step_x, py + step_y, pz + step_z]
        rows_ref[pl.ds(n * 128 + 8, 8, stride=16), :] = mids_ref[n]


def gather_upper(tops, tops_ref, rows_ref):
    far_x = [lax.rem(tops[0] + step + 3, 4) * 2 for step in range(3)]
    far_y = [lax.rem(tops[1] + step + 1, 2) * 2 for step in range(3)]
    far_z = [lax.rem(tops[2] + step + 3, 4) * 2 for step in range(3)]
    for n in range(27):
        step_x, step_y, step_z = n // 9, n // 3 % 3, n % 3
        for octant in range(8):
            ox, oy, oz = octant >> 2, octant >> 1 & 1, octant & 1
            place = n * 128 + octant * 16 + 9
            rows_ref[place : place + 1, :] = tops_ref[far_x[step_x] + ox, far_y[step_y] + oy, far_z[step_z] + oz]


def convert_tiles(rows_ref, tiles_ref):
    for tile in range(218):
        tiles_ref[tile] = rows_ref[tile * 16 : tile * 16 + 16, :].astype(BF16)


def gather_top(tops, tops_ref, upper_ref, operators, lattice_ref, turned_ref, rows_ref):
    for octant in range(8):
        ox, oy, oz = octant >> 2, octant >> 1 & 1, octant & 1
        for box in range(32):
            bx, by, bz = box >> 3, box >> 2 & 1, box & 3
            upper_ref[octant, box : box + 1, :] = tops_ref[2 * bx + ox, 2 * by + oy, 2 * bz + oz]
    coarse = jnp.zeros((32, TERMS), F32)
    for octant in range(8):
        coarse = coarse + split_nt(upper_ref[octant][:, :TERMS], operators[octant])
    lattice_term = split_nt(jnp.sum(coarse, axis=0, keepdims=True), lattice_ref[...])
    row = lax.broadcasted_iota(jnp.int32, (32, 32), 0)
    column = lax.broadcasted_iota(jnp.int32, (32, 32), 1)
    wanted = (
        (row // 8 + tops[0]) % 4 * 8 + (row // 4 % 2 + tops[1]) % 2 * 4 + (row % 4 + tops[2]) % 4
    )
    turned_ref[...] = jnp.dot(
        (wanted == column).astype(F32).astype(BF16), widen(coarse).astype(BF16), preferred_element_type=F32
    )
    for shift in offset_table():
        parity = top_parity(shift)
        source = shift[0] % 4 * 8 + shift[1] % 2 * 4 + shift[2] % 4
        if parity is not None:
            place = [shift[axis] + (parity >> (2 - axis) & 1) for axis in range(3)]
            target = tile_of(place) * 16 + TOP_ROWS[parity]
            rows_ref[target : target + 1, :] = turned_ref[source : source + 1, :]
        else:
            ((parity, place),) = admitted(shift)
            begin, target = tile_of(place) * 16, EXTRA_TILES[parity] * 16
            which = lax.broadcasted_iota(jnp.int32, (8, LANES), 0)
            lower = jnp.where(which < 2, rows_ref[begin + 8 : begin + 16, :], 0.0)
            top = jnp.broadcast_to(turned_ref[source : source + 1, :], (8, LANES))
            rows_ref[target : target + 8, :] = rows_ref[begin : begin + 8, :]
            rows_ref[target + 8 : target + 16, :] = jnp.where(which == 2, top, lower)
    return lattice_term


def far_products(tiles_ref, aligned_ref, acc_ref):
    total = [jnp.zeros((16, TERMS), F32) for _ in range(8)]
    extra = jnp.zeros((1, TERMS), F32)
    shifts = offset_table()
    slot = 0
    for parities, members in offset_groups():
        for start in range(0, len(members), CHUNK):
            part = members[start : start + CHUNK]
            special = len(parities) == 1 and parities[0] in EXTRA_TILES
            columns = []
            for index in part:
                tiles = [EXTRA_TILES[parities[0]]] if special else [tile_of(place) for _, place in admitted(shifts[index])]
                columns.append(jnp.concatenate([tiles_ref[tile] for tile in tiles], axis=0))
            data = columns[0] if len(columns) == 1 else jnp.concatenate(columns, axis=1)
            product = lanes_nt(data, aligned_ref[:TERMS, slot * LANES : (slot + len(part)) * LANES])
            slot += len(part)
            for place, parity in enumerate(parities):
                total[parity] = total[parity] + product[place * 16 : place * 16 + 16]
            if special:
                extra = extra + product[10:11]
    for parity in range(8):
        acc_ref[parity * 16 : parity * 16 + 16, :] = widen(total[parity])
    return extra


def down_operators(octant_own, down_rows, downs_ref):
    own = jnp.where(
        lax.broadcasted_iota(jnp.int32, (TERMS * 8, LANES), 0) % 8 == octant_own, down_rows[...], 0.0
    )
    downs_ref[8, :TERMS, :] = jnp.sum(own.reshape(TERMS, 8, LANES), axis=1).astype(BF16)
    for octant in range(8):
        downs_ref[octant, :TERMS, :TERMS] = octant_operator(down_rows, octant)


def locals_down(octant_own, acc_ref, lattice_term, downs_ref, local_ref):
    far_top = lattice_term
    for parity, place in TOP_ROWS.items():
        row = parity * 16 + place
        far_top = far_top + acc_ref[row : row + 1, :][:, :TERMS]
    operator = lambda octant: downs_ref[octant, :TERMS, :TERMS]
    local_upper = 0.25 * acc_ref[pl.ds(octant_own * 16 + 9, 1), :][:, :TERMS] + split_nt(
        0.125 * far_top, operator(8)
    )
    upper_wide = jnp.broadcast_to(local_upper, (8, TERMS))
    which = lax.broadcasted_iota(jnp.int32, (8, TERMS), 0)
    local_mid = 0.5 * acc_ref[pl.ds(8, 8, stride=16), :][:, :TERMS]
    for octant in range(8):
        local_mid = local_mid + jnp.where(which == octant, split_nt(upper_wide, operator(octant)), 0.0)
    for octant in range(8):
        local = acc_ref[octant * 16 : octant * 16 + 8, :][:, :TERMS] + split_nt(local_mid, operator(octant))
        local_ref[octant * 8 : octant * 8 + 8, :] = widen(local)


def evaluate(local_ref, slope_ref, high_ref, low_ref, sums_ref, data_ref, live_ref, out_ref):
    local_leaf = local_ref[...]
    upper, lower = halves(local_leaf[:, :TERMS])
    slopes = jnp.dot(upper, slope_ref[...], preferred_element_type=F32) + jnp.dot(
        lower, slope_ref[...], preferred_element_type=F32
    )
    parts = [local_leaf] + [slopes[:, c * LANES : (c + 1) * LANES] for c in range(3)]
    split_parts = [halves(part[:, :KPAD]) for part in parts]
    row = lax.broadcasted_iota(jnp.int32, (16, LANES), 0)
    lane = lax.broadcasted_iota(jnp.int32, (16, LANES), 1)
    self_weight = lax.rsqrt(jnp.full((1, LANES), SOFTENING, F32))
    for parity in range(4):
        span = slice(parity * 16, parity * 16 + 16)
        coef_high = jnp.concatenate([part[0][span] for part in split_parts], axis=0)
        coef_low = jnp.concatenate([part[1][span] for part in split_parts], axis=0)
        coef = jnp.concatenate([coef_high, coef_low], axis=0)
        for group in range(4):
            x, y = (group >> 1) * 2 + (parity >> 1), (group & 1) * 2 + (parity & 1)
            tile = group * 4 + parity
            lanes = slice(tile * LANES, tile * LANES + LANES)
            both = jnp.dot(coef, high_ref[:, lanes], preferred_element_type=F32)
            value = both[:64] + both[64:] + jnp.dot(coef_high, low_ref[:, lanes], preferred_element_type=F32)
            hit = (row // 8 == lane // 32 % 2) & (row % 8 == group * 2 + lane // 64)
            sums = [
                jnp.sum(jnp.where(hit, value[16 * c : 16 * c + 16], 0.0), axis=0, keepdims=True) for c in range(4)
            ]
            near = [jnp.sum(sums_ref[x, y, c], axis=0, keepdims=True) for c in range(4)]
            live = live_ref[x, y : y + 1, :]
            near[0] = near[0] - data_ref[x, y, 3:4, :] * self_weight
            for c in range(4):
                value = near[c] + sums[c] if c == 0 else near[c] - sums[c]
                out_ref[c, x, y : y + 1, :] = value * live


def whole_kernel(
    nx,
    ny,
    nz,
    pos_hbm,
    chg_hbm,
    cnt_hbm,
    up_hbm,
    down_hbm,
    slope_hbm,
    lattice_hbm,
    far_hbm,
    out_ref,
    pos_ref,
    chg_ref,
    cnt_ref,
    up_ref,
    down_ref,
    slope_ref,
    lattice_ref,
    data_ref,
    live_ref,
    ext_ref,
    wide_ref,
    mids_ref,
    tops_ref,
    leaf_ref,
    mid_ref,
    top_ref,
    up_rows,
    down_rows,
    downs_ref,
    high_ref,
    low_ref,
    turned_ref,
    table_ref,
    sums_ref,
    whole_ref,
    aligned_ref,
    rows_ref,
    tiles_ref,
    upper_ref,
    coarse_ref,
    acc_ref,
    local_ref,
    send,
    recv,
    gsend,
    grecv,
    own,
    load,
):
    ix, iy, iz = lax.axis_index("gx"), lax.axis_index("gy"), lax.axis_index("gz")

    def at(dx, dy, dz):
        return {
            "gx": lax.rem(ix + (dx + nx), nx),
            "gy": lax.rem(iy + (dy + ny), ny),
            "gz": lax.rem(iz + (dz + nz), nz),
        }

    plane = [(0, b, c) for b in range(ny) for c in range(nz) if b or c]
    line = [(a, 0, 0) for a in range(1, nx)]
    wrapped = lambda step: (step[0] % nx, step[1] % ny, step[2] % nz)
    partners = sorted({wrapped(step) for step in DIRECTIONS} | set(plane) | set(line))
    barrier = pltpu.get_barrier_semaphore()
    for step in partners:
        pl.semaphore_signal(barrier, inc=1, device_id=at(*step), device_id_type=MESH)
    operands = ((pos_hbm, pos_ref), (chg_hbm, chg_ref), (cnt_hbm, cnt_ref), (up_hbm, up_ref))
    operands += ((down_hbm, down_ref), (slope_hbm, slope_ref), (lattice_hbm, lattice_ref))
    loads = [pltpu.make_async_copy(src, dst, load.at[k]) for k, (src, dst) in enumerate(operands)]
    pieces = []
    for k in range(PIECES):
        span = pl.ds(k * (25600 // PIECES), 25600 // PIECES)
        pieces.append(pltpu.make_async_copy(far_hbm.at[:, span], whole_ref.at[:, span], load.at[7 + k]))
    for copy in loads + pieces:
        copy.start()
    octant_own = (ix % 2) * 4 + (iy % 2) * 2 + iz % 2
    for copy in loads[:4]:
        copy.wait()

    prepare(pos_ref, chg_ref, cnt_ref, data_ref, live_ref)
    octant_operators(up_ref, up_rows)
    monomial_tiles(rows_from(data_ref), high_ref, low_ref)
    moments(data_ref, up_rows, leaf_ref, mid_ref, top_ref, high_ref, low_ref)

    pl.semaphore_wait(barrier, len(partners))

    def remote(src, dst, ssem, rsem, step):
        copy = pltpu.make_async_remote_copy(
            src_ref=src, dst_ref=dst, send_sem=ssem, recv_sem=rsem, device_id=at(*step), device_id_type=MESH
        )
        copy.start()
        return copy

    local = [
        pltpu.make_async_copy(data_ref, ext_ref.at[pl.ds(1, 4), pl.ds(1, 4), 1], own.at[0]),
        pltpu.make_async_copy(leaf_ref, wide_ref.at[pl.ds(1, 2), pl.ds(1, 2), pl.ds(1, 2)], own.at[1]),
        pltpu.make_async_copy(mid_ref, mids_ref.at[13], own.at[2]),
        pltpu.make_async_copy(top_ref, tops_ref.at[ix, iy, iz], own.at[3]),
    ]
    for copy in local:
        copy.start()
    halo = {}
    order = sorted(range(len(DIRECTIONS)), key=lambda i: sum(abs(d) for d in DIRECTIONS[i][:2]))
    for index in order:
        dx, dy, dz = DIRECTIONS[index]
        from_x, to_x = span_of(dx, 4, 1)
        from_y, to_y = span_of(dy, 4, 1)
        src, dst = data_ref.at[from_x, from_y], ext_ref.at[to_x, to_y, 1 - dz]
        halo[index] = remote(src, dst, send.at[0, index], recv.at[0, index], DIRECTIONS[index])
    first = [
        remote(top_ref, tops_ref.at[ix, iy, iz], gsend.at[k], grecv.at[k], step) for k, step in enumerate(plane)
    ]
    boxes = []
    for index, step in enumerate(DIRECTIONS):
        spans = [span_of(d, 2, 1) for d in step]
        src = leaf_ref.at[spans[0][0], spans[1][0], spans[2][0]]
        dst = wide_ref.at[spans[0][1], spans[1][1], spans[2][1]]
        boxes.append(remote(src, dst, send.at[1, index], recv.at[1, index], step))
        slot = ((1 - step[0]) * 3 + (1 - step[1])) * 3 + (1 - step[2])
        boxes.append(remote(mid_ref, mids_ref.at[slot], send.at[2, index], recv.at[2, index], step))

    for copy in loads[4:]:
        copy.wait()
    octant_operators(down_ref, down_rows)
    down_operators(octant_own, down_rows, downs_ref)
    clear_rows(rows_ref)
    done = 0
    for k in range(PIECES):
        pieces[k].wait()
        ready = OFFSETS if k == PIECES - 1 else ((k + 1) * (25600 // PIECES) - LANES) // TERMS
        align_operators(done, ready, whole_ref, aligned_ref)
        done = ready
    for copy in local:
        copy.wait()
    for index in order[:2]:
        halo[index].wait()
    inside = [(x, y) for x in range(1, 5) for y in range(1, 5)]
    fill_cells(inside, ext_ref, turned_ref, table_ref)
    near_inside((0, 1), data_ref, table_ref, sums_ref)
    for copy in first:
        copy.wait()
    second = [
        remote(tops_ref.at[ix], tops_ref.at[ix], gsend.at[32 + k], grecv.at[32 + k], step)
        for k, step in enumerate(line)
    ]
    near_inside((2, 3), data_ref, table_ref, sums_ref)
    for index in order[2:]:
        halo[index].wait()
    fill_cells(
        [(x, y) for x in range(6) for y in range(6) if (x, y) not in inside], ext_ref, turned_ref, table_ref
    )
    near_outside(data_ref, table_ref, sums_ref)
    for copy in boxes:
        copy.wait()
    gather_boxes(wide_ref, mids_ref, rows_ref)
    for copy in second:
        copy.wait()
    tops = (ix // 2, iy // 2, iz // 2)
    gather_upper(tops, tops_ref, rows_ref)
    operators = [octant_operator(up_rows, octant) for octant in range(8)]
    lattice_term = gather_top(tops, tops_ref, upper_ref, operators, lattice_ref, coarse_ref, rows_ref)
    convert_tiles(rows_ref, tiles_ref)
    extra = far_products(tiles_ref, aligned_ref, acc_ref)
    locals_down(octant_own, acc_ref, lattice_term + extra, downs_ref, local_ref)
    evaluate(local_ref, slope_ref, high_ref, low_ref, sums_ref, data_ref, live_ref, out_ref)


VMEM = pl.BlockSpec(memory_space=pltpu.VMEM)


def shape(*dims):
    return jax.ShapeDtypeStruct(dims, F32)


def whole_call(sizes, *operands):
    dma = pltpu.SemaphoreType.DMA
    return pl.pallas_call(
        functools.partial(whole_kernel, *sizes),
        out_shape=shape(4, 4, 4, LANES),
        in_specs=[pl.BlockSpec(memory_space=pltpu.HBM)] * 8,
        out_specs=VMEM,
        scratch_shapes=[
            pltpu.VMEM((3, 4, 4, LANES), F32),
            pltpu.VMEM((4, 4, LANES), F32),
            pltpu.VMEM((4, 4, 4), jnp.int32),
            pltpu.VMEM((TERMS, 8, TERMS), BF16),
            pltpu.VMEM((TERMS, 8, TERMS), BF16),
            pltpu.VMEM((TERMS, 3 * LANES), BF16),
            pltpu.VMEM((TERMS, TERMS), BF16),
            pltpu.VMEM((4, 4, 4, LANES), F32),
            pltpu.VMEM((4, 4, LANES), F32),
            pltpu.VMEM((6, 6, 3, 4, LANES), F32),
            pltpu.VMEM((4, 4, 4, 8, LANES), F32),
            pltpu.VMEM((27, 8, LANES), F32),
            pltpu.VMEM((*sizes, 1, LANES), F32),
            pltpu.VMEM((2, 2, 2, 8, LANES), F32),
            pltpu.VMEM((8, LANES), F32),
            pltpu.VMEM((1, LANES), F32),
            pltpu.VMEM((TERMS * 8, LANES), F32),
            pltpu.VMEM((TERMS * 8, LANES), F32),
            pltpu.VMEM((9, KPAD, LANES), BF16),
            pltpu.VMEM((KPAD, 2048), BF16),
            pltpu.VMEM((KPAD, 2048), BF16),
            pltpu.VMEM((6, 6, 3, 4, LANES), F32),
            pltpu.VMEM((6, 6, 3, 4, SLOTS, LANES), F32),
            pltpu.VMEM((4, 4, 4, 8, LANES), F32),
            pltpu.VMEM((TERMS, 25600), BF16),
            pltpu.VMEM((KPAD, OFFSETS * LANES), BF16),
            pltpu.VMEM((218 * 16, LANES), F32),
            pltpu.VMEM((218, 16, LANES), BF16),
            pltpu.VMEM((8, 32, LANES), F32),
            pltpu.VMEM((32, LANES), F32),
            pltpu.VMEM((LANES, LANES), F32),
            pltpu.VMEM((64, LANES), F32),
            dma((3, 26)),
            dma((3, 26)),
            dma((40,)),
            dma((40,)),
            dma((4,)),
            dma((7 + PIECES,)),
        ],
        compiler_params=pltpu.CompilerParams(collective_id=0, has_side_effects=True),
        name="whole",
    )(*operands)


def part_kernel(both_ref, pot_ref, field_ref):
    pot_ref[...] = both_ref[0]
    field_ref[...] = both_ref[1:4]


def part_call(both):
    return pl.pallas_call(
        part_kernel,
        out_shape=(shape(4, 4, LANES), shape(3, 4, 4, LANES)),
        in_specs=[VMEM],
        out_specs=(VMEM,) * 2,
        name="part",
    )(both)


def solution(mesh):
    sizes = tuple(mesh.shape[axis] for axis in ("gx", "gy", "gz"))

    def per_device(
        positions, charges, counts, moment_shift, far_operators, local_shift, lattice_operator
    ):
        slope = jnp.asarray(slope_matrix()).astype(BF16)
        native_up = jnp.transpose(moment_shift, (1, 0, 2))
        native_down = jnp.transpose(local_shift, (1, 0, 2))
        both = whole_call(
            sizes,
            positions,
            charges,
            counts,
            native_up,
            native_down,
            slope,
            lattice_operator,
            far_operators,
        )
        return part_call(both)

    placed = (
        P(None, "gx", "gy", "gz"),
        P("gx", "gy", "gz"),
        P("gx", "gy", "gz"),
        P(),
        P(),
        P(),
        P(),
    )
    return jax.shard_map(
        per_device,
        mesh=mesh,
        in_specs=placed,
        out_specs=(P("gx", "gy", "gz"), P(None, "gx", "gy", "gz")),
        check_vma=False,
    )
```

```python
import functools

import jax
import jax.numpy as jnp
import numpy as np
from jax import lax
from jax.experimental import pallas as pl
from jax.experimental.pallas import tpu as pltpu
from jax.sharding import PartitionSpec as P

ORDER = 8
SLOTS = 32
SOFTENING = 0.0625
TERMS = 81
KPAD = 96
LANES = 128
OFFSETS = 316
CHUNK = 2
PIECES = 4
MESH = pl.DeviceIdType.MESH
F32 = jnp.float32
BF16 = jnp.bfloat16


def offset_table():
    listed = []
    for shift_x in range(-3, 4):
        for shift_y in range(-3, 4):
            for shift_z in range(-3, 4):
                if max(abs(shift_x), abs(shift_y), abs(shift_z)) >= 2:
                    listed.append((shift_x, shift_y, shift_z))
    return listed


def admitted(shift):
    listed = []
    for parity in range(8):
        place = [shift[axis] + (parity >> (2 - axis) & 1) for axis in range(3)]
        if all(-2 <= c <= 3 for c in place):
            listed.append((parity, tuple(place)))
    return listed


def tile_of(place):
    around = [(c + 2) // 2 for c in place]
    inner = [(c + 2) % 2 for c in place]
    return ((around[0] * 3 + around[1]) * 3 + around[2]) * 8 + inner[0] * 4 + inner[1] * 2 + inner[2]


TOP_ROWS = {0: 10, 7: 11, 3: 12, 4: 13, 1: 14, 6: 15}
EXTRA_TILES = {2: 216, 5: 217}
TRIPLES = 106


def top_parity(shift):
    if min(shift) > -3:
        return 0
    if max(shift) < 3:
        return 7
    fits = [parity for parity, _ in admitted(shift) if parity in TOP_ROWS]
    return fits[0] if fits else None


def exponent_list():
    listed = []
    for accumulated in range(ORDER + 1):
        for height in (0, 1):
            for power_x in range(accumulated - height + 1):
                listed.append((power_x, accumulated - height - power_x, height))
    return listed


def triple_groups():
    shifts = offset_table()
    groups = {}
    for triple in range(TRIPLES):
        members = shifts[3 * triple : 3 * triple + 3]
        parities = tuple(sorted({parity for shift in members for parity, _ in admitted(shift)}))
        extra = [EXTRA_TILES[admitted(shift)[0][0]] for shift in members if top_parity(shift) is None]
        groups.setdefault((parities, bool(extra)), []).append(triple)
    return sorted(groups.items(), key=lambda item: (-len(item[0][0]), item[0]))


def slope_matrix():
    listed = exponent_list()
    place = {e: i for i, e in enumerate(listed)}
    matrix = np.zeros((TERMS, 3 * LANES), np.float32)
    for row, (a, b, c) in enumerate(listed):
        if a > 0:
            matrix[row, place[(a - 1, b, c)]] = a
        if b > 0:
            matrix[row, LANES + place[(a, b - 1, c)]] = b
        if c > 0:
            matrix[row, 2 * LANES + place[(a, b, c - 1)]] = c
    return matrix


def lanes_nt(lhs, rhs):
    return lax.dot_general(lhs, rhs, (((1,), (1,)), ((), ())), preferred_element_type=F32)


def halves(value):
    upper = value.astype(BF16)
    return upper, (value - upper.astype(F32)).astype(BF16)


def split_nt(value, rhs):
    rows = value.shape[0]
    if rows % 8:
        value = jnp.concatenate([value, jnp.zeros((8 - rows, value.shape[1]), F32)], axis=0)
    size = value.shape[0]
    both = lanes_nt(jnp.concatenate(halves(value), axis=0), rhs)
    return (both[:size] + both[size:])[:rows]


def widen(value):
    return jnp.concatenate([value, jnp.zeros((value.shape[0], LANES - value.shape[1]), F32)], axis=1)


def power_of(base, exponents):
    square = base * base
    fourth = square * square
    eighth = fourth * fourth
    result = jnp.where((exponents & 1) != 0, base, 1.0)
    result = result * jnp.where((exponents & 2) != 0, square, 1.0)
    result = result * jnp.where((exponents & 4) != 0, fourth, 1.0)
    return jnp.where(exponents == 8, eighth, result)


def exponents():
    row = lax.broadcasted_iota(jnp.int32, (KPAD, LANES), 0)
    degree = jnp.zeros((KPAD, LANES), jnp.int32)
    for n in range(1, ORDER + 1):
        degree = degree + (row >= n * n).astype(jnp.int32)
    place = row - degree * degree
    height = (place > degree).astype(jnp.int32)
    power_x = place - height * (degree + 1)
    return power_x, degree - height - power_x, height, row < TERMS


def monomial_tiles(rows_of, high_ref, low_ref):
    power_x, power_y, power_z, valid = exponents()
    for tile in range(16):
        px, py, ox, oy = tile >> 3, tile >> 2 & 1, tile >> 1 & 1, tile & 1
        row_x, row_y, row_z = rows_of(2 * px + ox, 2 * py + oy)
        full = lambda row: jnp.broadcast_to(row - 0.5, (KPAD, LANES))
        value = power_of(full(row_x), power_x) * power_of(full(row_y), power_y)
        value = value * jnp.where(power_z != 0, full(row_z), 1.0)
        value = jnp.where(valid, value, 0.0)
        upper, lower = halves(value)
        high_ref[:, tile * LANES : (tile + 1) * LANES] = upper
        low_ref[:, tile * LANES : (tile + 1) * LANES] = lower


def octant_operators(native_ref, rows_ref):
    rows_ref[:, :TERMS] = native_ref[...].astype(F32).reshape(TERMS * 8, TERMS)


def octant_operator(rows_ref, octant):
    return rows_ref[pl.ds(octant, TERMS, stride=8), :][:, :TERMS].astype(BF16)


def prepare(pos_ref, chg_ref, cnt_ref, data_ref, live_ref):
    counts = jnp.concatenate([cnt_ref[x] for x in range(4)], axis=0).astype(F32).astype(BF16)
    spread = (
        lax.broadcasted_iota(jnp.int32, (4, LANES), 1) // SLOTS == lax.broadcasted_iota(jnp.int32, (4, LANES), 0)
    ).astype(F32).astype(BF16)
    limit = jnp.dot(counts, spread, preferred_element_type=F32)
    slot_of = (lax.broadcasted_iota(jnp.int32, (16, LANES), 1) % SLOTS).astype(F32)
    live = (slot_of < limit).astype(F32)
    for x in range(4):
        live_ref[x] = live[4 * x : 4 * x + 4]
        for y in range(4):
            for c in range(3):
                data_ref[x, y, c : c + 1, :] = pos_ref[c, x, y : y + 1, :]
            data_ref[x, y, 3:4, :] = chg_ref[x, y : y + 1, :] * live[4 * x + y : 4 * x + y + 1]


def rows_from(data_ref):
    return lambda x, y: tuple(data_ref[x, y, c : c + 1, :] for c in range(3))


def moments(data_ref, operator_rows, leaf_ref, mid_ref, top_ref, high_ref, low_ref):
    row = lax.broadcasted_iota(jnp.int32, (16, LANES), 0)
    lane = lax.broadcasted_iota(jnp.int32, (16, LANES), 1)
    for group in range(4):
        px, py = group >> 1, group & 1
        pieces = []
        for tile in range(4):
            ox, oy = tile >> 1, tile & 1
            hit = (row // 8 == lane // 64) & (row % 8 == ox * 4 + oy * 2 + lane // 32 % 2)
            weight = jnp.broadcast_to(data_ref[2 * px + ox, 2 * py + oy, 3:4, :], (16, LANES))
            pieces.append(jnp.where(hit, weight, 0.0))
        upper, lower = halves(jnp.concatenate(pieces, axis=1))
        span = slice(group * 512, group * 512 + 512)
        both = lanes_nt(jnp.concatenate([upper, lower], axis=0), high_ref[:, span])
        total = widen(both[:16] + both[16:] + lanes_nt(upper, low_ref[:, span]))
        leaf_ref[px, py, 0] = total[:8]
        leaf_ref[px, py, 1] = total[8:]
    mid = jnp.zeros((8, TERMS), F32)
    top = jnp.zeros((8, TERMS), F32)
    which = lax.broadcasted_iota(jnp.int32, (8, TERMS), 0)
    tiles = [leaf_ref[p >> 2, p >> 1 & 1, p & 1] for p in range(8)]
    operators = [octant_operator(operator_rows, octant) for octant in range(8)]
    for octant in range(8):
        rows = jnp.concatenate([tile[octant : octant + 1] for tile in tiles], axis=0)
        mid = mid + split_nt(rows[:, :TERMS], operators[octant])
    mid_ref[...] = widen(mid)
    for octant in range(8):
        top = top + jnp.where(which == octant, split_nt(mid, operators[octant]), 0.0)
    top_ref[...] = widen(jnp.sum(top, axis=0, keepdims=True))


DIRECTIONS = [
    (dx, dy, dz) for dx in (-1, 0, 1) for dy in (-1, 0, 1) for dz in (-1, 0, 1) if (dx, dy, dz) != (0, 0, 0)
]


def span_of(step, own, first):
    if step == 0:
        return pl.ds(0, own), pl.ds(first, own)
    if step > 0:
        return pl.ds(own - 1, 1), pl.ds(first - 1, 1)
    return pl.ds(0, 1), pl.ds(first + own, 1)


def fill_cells(cells, ext_ref, turned_ref, table_ref):
    lane4 = lax.broadcasted_iota(jnp.int32, (4, LANES), 1)
    for x, y in cells:
        before, here, after = ext_ref[x, y, 0], ext_ref[x, y, 1], ext_ref[x, y, 2]
        turned_ref[x, y, 0] = pltpu.roll(jnp.where(lane4 >= 96, before, here), 32, 1)
        turned_ref[x, y, 1] = here
        turned_ref[x, y, 2] = pltpu.roll(jnp.where(lane4 < 32, after, here), 96, 1)
    lane = lax.broadcasted_iota(jnp.int32, (8, LANES), 1)
    base = lane // SLOTS * SLOTS + lax.broadcasted_iota(jnp.int32, (8, LANES), 0)

    def one_group(group, carry):
        pick = base + group * 8
        start = pl.multiple_of(group * 8, 8)
        for x, y in cells:
            for ez in range(3):
                for c in range(4):
                    row = jnp.broadcast_to(turned_ref[x, y, ez, c : c + 1, :], (8, LANES))
                    table_ref[x, y, ez, c, pl.ds(start, 8), :] = jnp.take_along_axis(row, pick, axis=1)
        return carry

    lax.fori_loop(0, 4, one_group, 0)


def load_wide(data_ref, x, y):
    mine = data_ref[x, y]
    return [jnp.broadcast_to(mine[c : c + 1], (8, LANES)) for c in range(3)]


def pair_sums(sums, here_x, here_y, here_z, x, y, table_ref):
    potential, field_x, field_y, field_z = sums
    for ez in range(3):
        for group in range(4):
            span = pl.ds(group * 8, 8)
            delta_x = here_x - table_ref[x, y, ez, 0, span, :]
            delta_y = here_y - table_ref[x, y, ez, 1, span, :]
            delta_z = here_z[ez] - table_ref[x, y, ez, 2, span, :]
            distance = delta_x * delta_x + delta_y * delta_y + (delta_z * delta_z + SOFTENING)
            inverse = lax.rsqrt(distance)
            weight = table_ref[x, y, ez, 3, span, :] * inverse
            cubic = weight * (inverse * inverse)
            potential = potential + weight
            field_x = field_x + cubic * delta_x
            field_y = field_y + cubic * delta_y
            field_z = field_z + cubic * delta_z
    return potential, field_x, field_y, field_z


def near_inside(rows, data_ref, table_ref, sums_ref):
    for y in rows:
        steps = [ey for ey in (-1, 0, 1) if 0 <= y + ey < 4]

        def along_x(x, carry):
            wide = load_wide(data_ref, x, y)
            here_z = [wide[2] - float(ez - 1) for ez in range(3)]

            def around(ex, sums):
                here_x = wide[0] - (ex - 1).astype(F32)
                for ey in steps:
                    sums = pair_sums(sums, here_x, wide[1] - float(ey), here_z, x + ex, y + ey + 1, table_ref)
                return sums

            zero = jnp.zeros((8, LANES), F32)
            low = 1 - jnp.minimum(x, 1)
            high = 2 + jnp.minimum(3 - x, 1)
            sums = lax.fori_loop(low, high, around, (zero, zero, zero, zero))
            for c in range(4):
                sums_ref[x, y, c] = sums[c]
            return carry

        lax.fori_loop(0, 4, along_x, 0)


def near_outside(data_ref, table_ref, sums_ref):
    for x, ex in ((0, -1), (3, 1)):

        def along_y(y, carry):
            wide = load_wide(data_ref, x, y)
            here_z = [wide[2] - float(ez - 1) for ez in range(3)]
            sums = tuple(sums_ref[x, y, c] for c in range(4))
            for ey in (-1, 0, 1):
                sums = pair_sums(
                    sums, wide[0] - float(ex), wide[1] - float(ey), here_z, x + ex + 1, y + ey + 1, table_ref
                )
            for c in range(4):
                sums_ref[x, y, c] = sums[c]
            return carry

        lax.fori_loop(0, 4, along_y, 0)
    for y, ey in ((0, -1), (3, 1)):
        for x in range(4):
            wide = load_wide(data_ref, x, y)
            here_z = [wide[2] - float(ez - 1) for ez in range(3)]
            sums = tuple(sums_ref[x, y, c] for c in range(4))
            for ex in (-1, 0, 1):
                if 0 <= x + ex < 4:
                    sums = pair_sums(
                        sums, wide[0] - float(ex), wide[1] - float(ey), here_z, x + ex + 1, y + ey + 1, table_ref
                    )
            for c in range(4):
                sums_ref[x, y, c] = sums[c]


def align_operators(first, last, whole_ref, aligned_ref):
    slots = {}
    for _, members in triple_groups():
        for triple in members:
            slots[triple] = len(slots)
    for triple in range(first, last):
        begin = triple * 3 * TERMS
        if begin + 256 <= whole_ref.shape[1]:
            piece = whole_ref[:, begin : begin + 256]
        else:
            tail = whole_ref[:, begin : OFFSETS * TERMS]
            piece = jnp.concatenate([tail, jnp.zeros((TERMS, 256 - tail.shape[1]), BF16)], axis=1)
        slot = slots[triple]
        aligned_ref[:TERMS, slot * 256 : (slot + 1) * 256] = piece


def clear_rows(rows_ref):
    def step(n, carry):
        for octant in range(8):
            rows_ref[pl.ds(pl.multiple_of(n * 128 + octant * 16 + 8, 8), 8), :] = jnp.zeros((8, LANES), F32)
        return carry

    lax.fori_loop(0, 27, step, 0)


def gather_boxes(wide_ref, mids_ref, rows_ref):
    for n in range(27):
        step_x, step_y, step_z = n // 9, n // 3 % 3, n % 3
        for parent in range(8):
            px, py, pz = parent >> 2, parent >> 1 & 1, parent & 1
            rows_ref[pl.ds(n * 128 + parent, 8, stride=16), :] = wide_ref[px + step_x, py + step_y, pz + step_z]
        rows_ref[pl.ds(n * 128 + 8, 8, stride=16), :] = mids_ref[n]


def gather_upper(tops, tops_ref, rows_ref):
    far_x = [lax.rem(tops[0] + step + 3, 4) * 2 for step in range(3)]
    far_y = [lax.rem(tops[1] + step + 1, 2) * 2 for step in range(3)]
    far_z = [lax.rem(tops[2] + step + 3, 4) * 2 for step in range(3)]
    for n in range(27):
        step_x, step_y, step_z = n // 9, n // 3 % 3, n % 3
        for octant in range(8):
            ox, oy, oz = octant >> 2, octant >> 1 & 1, octant & 1
            place = n * 128 + octant * 16 + 9
            rows_ref[place : place + 1, :] = tops_ref[far_x[step_x] + ox, far_y[step_y] + oy, far_z[step_z] + oz]


def convert_tiles(rows_ref, tiles_ref):
    lane = lax.broadcasted_iota(jnp.int32, (16, LANES), 1)
    zero = jnp.zeros((16, LANES), BF16)
    for tile in range(218):
        value = rows_ref[tile * 16 : tile * 16 + 16, :].astype(BF16)
        second = pltpu.roll(value, TERMS, 1)
        tiles_ref[0, tile] = value
        tiles_ref[1, tile] = jnp.where(lane >= TERMS, second, zero)
        tiles_ref[2, tile] = jnp.where(lane < TERMS, second, zero)
        tiles_ref[3, tile] = pltpu.roll(value, 2 * TERMS - LANES, 1)


def gather_top(tops, tops_ref, upper_ref, operators, lattice_ref, turned_ref, rows_ref):
    for octant in range(8):
        ox, oy, oz = octant >> 2, octant >> 1 & 1, octant & 1
        for box in range(32):
            bx, by, bz = box >> 3, box >> 2 & 1, box & 3
            upper_ref[octant, box : box + 1, :] = tops_ref[2 * bx + ox, 2 * by + oy, 2 * bz + oz]
    coarse = jnp.zeros((32, TERMS), F32)
    for octant in range(8):
        coarse = coarse + split_nt(upper_ref[octant][:, :TERMS], operators[octant])
    lattice_term = split_nt(jnp.sum(coarse, axis=0, keepdims=True), lattice_ref[...])
    row = lax.broadcasted_iota(jnp.int32, (32, 32), 0)
    column = lax.broadcasted_iota(jnp.int32, (32, 32), 1)
    wanted = (
        (row // 8 + tops[0]) % 4 * 8 + (row // 4 % 2 + tops[1]) % 2 * 4 + (row % 4 + tops[2]) % 4
    )
    turned_ref[...] = jnp.dot(
        (wanted == column).astype(F32).astype(BF16), widen(coarse).astype(BF16), preferred_element_type=F32
    )
    for shift in offset_table():
        parity = top_parity(shift)
        source = shift[0] % 4 * 8 + shift[1] % 2 * 4 + shift[2] % 4
        if parity is not None:
            place = [shift[axis] + (parity >> (2 - axis) & 1) for axis in range(3)]
            target = tile_of(place) * 16 + TOP_ROWS[parity]
            rows_ref[target : target + 1, :] = turned_ref[source : source + 1, :]
        else:
            target = EXTRA_TILES[admitted(shift)[0][0]] * 16
            which = lax.broadcasted_iota(jnp.int32, (16, LANES), 0)
            top = jnp.broadcast_to(turned_ref[source : source + 1, :], (16, LANES))
            rows_ref[target : target + 16, :] = jnp.where(which == 0, top, 0.0)
    return lattice_term


def far_products(tiles_ref, aligned_ref, acc_ref):
    total = [jnp.zeros((16, TERMS), F32) for _ in range(8)]
    extra = jnp.zeros((1, TERMS), F32)
    shifts = offset_table()
    empty = jnp.zeros((16, LANES), BF16)

    def lanes_of(sources):
        halves_of = ([], [])
        for position, tile in enumerate(sources):
            if tile is not None:
                for half, version in (((0, 0),), ((0, 1), (1, 2)), ((1, 3),))[position]:
                    halves_of[half].append(tiles_ref[version, tile])
        sides = [sum(side[1:], side[0]) if side else empty for side in halves_of]
        return jnp.concatenate(sides, axis=1)

    slot = 0
    for (parities, special), members in triple_groups():
        group = None
        for start in range(0, len(members), CHUNK):
            part = members[start : start + CHUNK]
            columns = []
            for triple in part:
                steps = shifts[3 * triple : 3 * triple + 3]
                places = [dict(admitted(step)) for step in steps]
                rows = [[tile_of(place[p]) if p in place else None for place in places] for p in parities]
                if special:
                    rows.append(
                        [EXTRA_TILES[admitted(step)[0][0]] if top_parity(step) is None else None for step in steps]
                    )
                columns.append(jnp.concatenate([lanes_of(sources) for sources in rows], axis=0))
            data = columns[0] if len(columns) == 1 else jnp.concatenate(columns, axis=1)
            product = lanes_nt(data, aligned_ref[:TERMS, slot * 256 : (slot + len(part)) * 256])
            slot += len(part)
            group = product if group is None else group + product
        for place, parity in enumerate(parities):
            total[parity] = total[parity] + group[place * 16 : place * 16 + 16]
        if special:
            extra = extra + group[len(parities) * 16 : len(parities) * 16 + 1]
    for parity in range(8):
        acc_ref[parity * 16 : parity * 16 + 16, :] = widen(total[parity])
    return extra


def down_operators(octant_own, down_rows, downs_ref):
    own = jnp.where(
        lax.broadcasted_iota(jnp.int32, (TERMS * 8, LANES), 0) % 8 == octant_own, down_rows[...], 0.0
    )
    downs_ref[8, :TERMS, :] = jnp.sum(own.reshape(TERMS, 8, LANES), axis=1).astype(BF16)
    for octant in range(8):
        downs_ref[octant, :TERMS, :TERMS] = octant_operator(down_rows, octant)


def locals_down(octant_own, acc_ref, lattice_term, downs_ref, local_ref):
    far_top = lattice_term
    for parity, place in TOP_ROWS.items():
        row = parity * 16 + place
        far_top = far_top + acc_ref[row : row + 1, :][:, :TERMS]
    operator = lambda octant: downs_ref[octant, :TERMS, :TERMS]
    local_upper = 0.25 * acc_ref[pl.ds(octant_own * 16 + 9, 1), :][:, :TERMS] + split_nt(
        0.125 * far_top, operator(8)
    )
    upper_wide = jnp.broadcast_to(local_upper, (8, TERMS))
    which = lax.broadcasted_iota(jnp.int32, (8, TERMS), 0)
    local_mid = 0.5 * acc_ref[pl.ds(8, 8, stride=16), :][:, :TERMS]
    for octant in range(8):
        local_mid = local_mid + jnp.where(which == octant, split_nt(upper_wide, operator(octant)), 0.0)
    for octant in range(8):
        local = acc_ref[octant * 16 : octant * 16 + 8, :][:, :TERMS] + split_nt(local_mid, operator(octant))
        local_ref[octant * 8 : octant * 8 + 8, :] = widen(local)


def evaluate(local_ref, slope_ref, high_ref, low_ref, sums_ref, data_ref, live_ref, out_ref):
    local_leaf = local_ref[...]
    upper, lower = halves(local_leaf[:, :TERMS])
    slopes = jnp.dot(upper, slope_ref[...], preferred_element_type=F32) + jnp.dot(
        lower, slope_ref[...], preferred_element_type=F32
    )
    parts = [local_leaf] + [slopes[:, c * LANES : (c + 1) * LANES] for c in range(3)]
    split_parts = [halves(part[:, :KPAD]) for part in parts]
    row = lax.broadcasted_iota(jnp.int32, (16, LANES), 0)
    lane = lax.broadcasted_iota(jnp.int32, (16, LANES), 1)
    self_weight = lax.rsqrt(jnp.full((1, LANES), SOFTENING, F32))
    for parity in range(4):
        span = slice(parity * 16, parity * 16 + 16)
        coef_high = jnp.concatenate([part[0][span] for part in split_parts], axis=0)
        coef_low = jnp.concatenate([part[1][span] for part in split_parts], axis=0)
        coef = jnp.concatenate([coef_high, coef_low], axis=0)
        for group in range(4):
            x, y = (group >> 1) * 2 + (parity >> 1), (group & 1) * 2 + (parity & 1)
            tile = group * 4 + parity
            lanes = slice(tile * LANES, tile * LANES + LANES)
            both = jnp.dot(coef, high_ref[:, lanes], preferred_element_type=F32)
            value = both[:64] + both[64:] + jnp.dot(coef_high, low_ref[:, lanes], preferred_element_type=F32)
            hit = (row // 8 == lane // 32 % 2) & (row % 8 == group * 2 + lane // 64)
            sums = [
                jnp.sum(jnp.where(hit, value[16 * c : 16 * c + 16], 0.0), axis=0, keepdims=True) for c in range(4)
            ]
            near = [jnp.sum(sums_ref[x, y, c], axis=0, keepdims=True) for c in range(4)]
            live = live_ref[x, y : y + 1, :]
            near[0] = near[0] - data_ref[x, y, 3:4, :] * self_weight
            for c in range(4):
                value = near[c] + sums[c] if c == 0 else near[c] - sums[c]
                out_ref[c, x, y : y + 1, :] = value * live


def whole_kernel(
    nx,
    ny,
    nz,
    pos_hbm,
    chg_hbm,
    cnt_hbm,
    up_hbm,
    down_hbm,
    slope_hbm,
    lattice_hbm,
    far_hbm,
    out_ref,
    pos_ref,
    chg_ref,
    cnt_ref,
    up_ref,
    down_ref,
    slope_ref,
    lattice_ref,
    data_ref,
    live_ref,
    ext_ref,
    wide_ref,
    mids_ref,
    tops_ref,
    leaf_ref,
    mid_ref,
    top_ref,
    up_rows,
    down_rows,
    downs_ref,
    high_ref,
    low_ref,
    turned_ref,
    table_ref,
    sums_ref,
    whole_ref,
    aligned_ref,
    rows_ref,
    tiles_ref,
    upper_ref,
    coarse_ref,
    acc_ref,
    local_ref,
    send,
    recv,
    gsend,
    grecv,
    own,
    load,
):
    ix, iy, iz = lax.axis_index("gx"), lax.axis_index("gy"), lax.axis_index("gz")

    def at(dx, dy, dz):
        return {
            "gx": lax.rem(ix + (dx + nx), nx),
            "gy": lax.rem(iy + (dy + ny), ny),
            "gz": lax.rem(iz + (dz + nz), nz),
        }

    plane = [(0, b, c) for b in range(ny) for c in range(nz) if b or c]
    line = [(a, 0, 0) for a in range(1, nx)]
    wrapped = lambda step: (step[0] % nx, step[1] % ny, step[2] % nz)
    partners = sorted({wrapped(step) for step in DIRECTIONS} | set(plane) | set(line))
    barrier = pltpu.get_barrier_semaphore()
    for step in partners:
        pl.semaphore_signal(barrier, inc=1, device_id=at(*step), device_id_type=MESH)
    operands = ((pos_hbm, pos_ref), (chg_hbm, chg_ref), (cnt_hbm, cnt_ref), (up_hbm, up_ref))
    operands += ((down_hbm, down_ref), (slope_hbm, slope_ref), (lattice_hbm, lattice_ref))
    loads = [pltpu.make_async_copy(src, dst, load.at[k]) for k, (src, dst) in enumerate(operands)]
    pieces = []
    for k in range(PIECES):
        span = pl.ds(k * (25600 // PIECES), 25600 // PIECES)
        pieces.append(pltpu.make_async_copy(far_hbm.at[:, span], whole_ref.at[:, span], load.at[7 + k]))
    for copy in loads + pieces:
        copy.start()
    octant_own = (ix % 2) * 4 + (iy % 2) * 2 + iz % 2
    for copy in loads[:4]:
        copy.wait()

    prepare(pos_ref, chg_ref, cnt_ref, data_ref, live_ref)
    octant_operators(up_ref, up_rows)
    monomial_tiles(rows_from(data_ref), high_ref, low_ref)
    moments(data_ref, up_rows, leaf_ref, mid_ref, top_ref, high_ref, low_ref)

    pl.semaphore_wait(barrier, len(partners))

    def remote(src, dst, ssem, rsem, step):
        copy = pltpu.make_async_remote_copy(
            src_ref=src, dst_ref=dst, send_sem=ssem, recv_sem=rsem, device_id=at(*step), device_id_type=MESH
        )
        copy.start()
        return copy

    local = [
        pltpu.make_async_copy(data_ref, ext_ref.at[pl.ds(1, 4), pl.ds(1, 4), 1], own.at[0]),
        pltpu.make_async_copy(leaf_ref, wide_ref.at[pl.ds(1, 2), pl.ds(1, 2), pl.ds(1, 2)], own.at[1]),
        pltpu.make_async_copy(mid_ref, mids_ref.at[13], own.at[2]),
        pltpu.make_async_copy(top_ref, tops_ref.at[ix, iy, iz], own.at[3]),
    ]
    for copy in local:
        copy.start()
    halo = {}
    order = sorted(range(len(DIRECTIONS)), key=lambda i: sum(abs(d) for d in DIRECTIONS[i][:2]))
    for index in order:
        dx, dy, dz = DIRECTIONS[index]
        from_x, to_x = span_of(dx, 4, 1)
        from_y, to_y = span_of(dy, 4, 1)
        src, dst = data_ref.at[from_x, from_y], ext_ref.at[to_x, to_y, 1 - dz]
        halo[index] = remote(src, dst, send.at[0, index], recv.at[0, index], DIRECTIONS[index])
    first = [
        remote(top_ref, tops_ref.at[ix, iy, iz], gsend.at[k], grecv.at[k], step) for k, step in enumerate(plane)
    ]
    boxes = []
    for index, step in enumerate(DIRECTIONS):
        spans = [span_of(d, 2, 1) for d in step]
        src = leaf_ref.at[spans[0][0], spans[1][0], spans[2][0]]
        dst = wide_ref.at[spans[0][1], spans[1][1], spans[2][1]]
        boxes.append(remote(src, dst, send.at[1, index], recv.at[1, index], step))
        slot = ((1 - step[0]) * 3 + (1 - step[1])) * 3 + (1 - step[2])
        boxes.append(remote(mid_ref, mids_ref.at[slot], send.at[2, index], recv.at[2, index], step))

    for copy in loads[4:]:
        copy.wait()
    octant_operators(down_ref, down_rows)
    down_operators(octant_own, down_rows, downs_ref)
    clear_rows(rows_ref)
    for copy in local:
        copy.wait()
    for index in order[:2]:
        halo[index].wait()
    inside = [(x, y) for x in range(1, 5) for y in range(1, 5)]
    fill_cells(inside, ext_ref, turned_ref, table_ref)
    near_inside((0, 1, 2, 3), data_ref, table_ref, sums_ref)
    for copy in first:
        copy.wait()
    second = [
        remote(tops_ref.at[ix], tops_ref.at[ix], gsend.at[32 + k], grecv.at[32 + k], step)
        for k, step in enumerate(line)
    ]
    for copy in pieces:
        copy.wait()
    align_operators(0, TRIPLES, whole_ref, aligned_ref)
    for index in order[2:]:
        halo[index].wait()
    fill_cells(
        [(x, y) for x in range(6) for y in range(6) if (x, y) not in inside], ext_ref, turned_ref, table_ref
    )
    near_outside(data_ref, table_ref, sums_ref)
    for copy in boxes:
        copy.wait()
    gather_boxes(wide_ref, mids_ref, rows_ref)
    for copy in second:
        copy.wait()
    tops = (ix // 2, iy // 2, iz // 2)
    gather_upper(tops, tops_ref, rows_ref)
    operators = [octant_operator(up_rows, octant) for octant in range(8)]
    lattice_term = gather_top(tops, tops_ref, upper_ref, operators, lattice_ref, coarse_ref, rows_ref)
    convert_tiles(rows_ref, tiles_ref)
    extra = far_products(tiles_ref, aligned_ref, acc_ref)
    locals_down(octant_own, acc_ref, lattice_term + extra, downs_ref, local_ref)
    evaluate(local_ref, slope_ref, high_ref, low_ref, sums_ref, data_ref, live_ref, out_ref)


VMEM = pl.BlockSpec(memory_space=pltpu.VMEM)


def shape(*dims):
    return jax.ShapeDtypeStruct(dims, F32)


def whole_call(sizes, *operands):
    dma = pltpu.SemaphoreType.DMA
    return pl.pallas_call(
        functools.partial(whole_kernel, *sizes),
        out_shape=shape(4, 4, 4, LANES),
        in_specs=[pl.BlockSpec(memory_space=pltpu.HBM)] * 8,
        out_specs=VMEM,
        scratch_shapes=[
            pltpu.VMEM((3, 4, 4, LANES), F32),
            pltpu.VMEM((4, 4, LANES), F32),
            pltpu.VMEM((4, 4, 4), jnp.int32),
            pltpu.VMEM((TERMS, 8, TERMS), BF16),
            pltpu.VMEM((TERMS, 8, TERMS), BF16),
            pltpu.VMEM((TERMS, 3 * LANES), BF16),
            pltpu.VMEM((TERMS, TERMS), BF16),
            pltpu.VMEM((4, 4, 4, LANES), F32),
            pltpu.VMEM((4, 4, LANES), F32),
            pltpu.VMEM((6, 6, 3, 4, LANES), F32),
            pltpu.VMEM((4, 4, 4, 8, LANES), F32),
            pltpu.VMEM((27, 8, LANES), F32),
            pltpu.VMEM((*sizes, 1, LANES), F32),
            pltpu.VMEM((2, 2, 2, 8, LANES), F32),
            pltpu.VMEM((8, LANES), F32),
            pltpu.VMEM((1, LANES), F32),
            pltpu.VMEM((TERMS * 8, LANES), F32),
            pltpu.VMEM((TERMS * 8, LANES), F32),
            pltpu.VMEM((9, KPAD, LANES), BF16),
            pltpu.VMEM((KPAD, 2048), BF16),
            pltpu.VMEM((KPAD, 2048), BF16),
            pltpu.VMEM((6, 6, 3, 4, LANES), F32),
            pltpu.VMEM((6, 6, 3, 4, SLOTS, LANES), F32),
            pltpu.VMEM((4, 4, 4, 8, LANES), F32),
            pltpu.VMEM((TERMS, 25600), BF16),
            pltpu.VMEM((KPAD, TRIPLES * 256), BF16),
            pltpu.VMEM((218 * 16, LANES), F32),
            pltpu.VMEM((4, 218, 16, LANES), BF16),
            pltpu.VMEM((8, 32, LANES), F32),
            pltpu.VMEM((32, LANES), F32),
            pltpu.VMEM((LANES, LANES), F32),
            pltpu.VMEM((64, LANES), F32),
            dma((3, 26)),
            dma((3, 26)),
            dma((40,)),
            dma((40,)),
            dma((4,)),
            dma((7 + PIECES,)),
        ],
        compiler_params=pltpu.CompilerParams(collective_id=0, has_side_effects=True),
        name="whole",
    )(*operands)


def part_kernel(both_ref, pot_ref, field_ref):
    pot_ref[...] = both_ref[0]
    field_ref[...] = both_ref[1:4]


def part_call(both):
    return pl.pallas_call(
        part_kernel,
        out_shape=(shape(4, 4, LANES), shape(3, 4, 4, LANES)),
        in_specs=[VMEM],
        out_specs=(VMEM,) * 2,
        name="part",
    )(both)


def solution(mesh):
    sizes = tuple(mesh.shape[axis] for axis in ("gx", "gy", "gz"))

    def per_device(
        positions, charges, counts, moment_shift, far_operators, local_shift, lattice_operator
    ):
        slope = jnp.asarray(slope_matrix()).astype(BF16)
        native_up = jnp.transpose(moment_shift, (1, 0, 2))
        native_down = jnp.transpose(local_shift, (1, 0, 2))
        both = whole_call(
            sizes,
            positions,
            charges,
            counts,
            native_up,
            native_down,
            slope,
            lattice_operator,
            far_operators,
        )
        return part_call(both)

    placed = (
        P(None, "gx", "gy", "gz"),
        P("gx", "gy", "gz"),
        P("gx", "gy", "gz"),
        P(),
        P(),
        P(),
        P(),
    )
    return jax.shard_map(
        per_device,
        mesh=mesh,
        in_specs=placed,
        out_specs=(P("gx", "gy", "gz"), P(None, "gx", "gy", "gz")),
        check_vma=False,
    )
```

```python
import functools

import jax
import jax.numpy as jnp
import numpy as np
from jax import lax
from jax.experimental import pallas as pl
from jax.experimental.pallas import tpu as pltpu
from jax.sharding import PartitionSpec as P

ORDER = 8
SLOTS = 32
SOFTENING = 0.0625
TERMS = 81
KPAD = 96
LANES = 128
OFFSETS = 316
CHUNK = 2
PIECES = 4
MESH = pl.DeviceIdType.MESH
F32 = jnp.float32
BF16 = jnp.bfloat16


def offset_table():
    listed = []
    for shift_x in range(-3, 4):
        for shift_y in range(-3, 4):
            for shift_z in range(-3, 4):
                if max(abs(shift_x), abs(shift_y), abs(shift_z)) >= 2:
                    listed.append((shift_x, shift_y, shift_z))
    return listed


def admitted(shift):
    listed = []
    for parity in range(8):
        place = [shift[axis] + (parity >> (2 - axis) & 1) for axis in range(3)]
        if all(-2 <= c <= 3 for c in place):
            listed.append((parity, tuple(place)))
    return listed


def tile_of(place):
    around = [(c + 2) // 2 for c in place]
    inner = [(c + 2) % 2 for c in place]
    return ((around[0] * 3 + around[1]) * 3 + around[2]) * 8 + inner[0] * 4 + inner[1] * 2 + inner[2]


TOP_ROWS = {0: 10, 7: 11, 3: 12, 4: 13, 1: 14, 6: 15}
EXTRA_TILES = {2: 216, 5: 217}
TRIPLES = 106


def top_parity(shift):
    if min(shift) > -3:
        return 0
    if max(shift) < 3:
        return 7
    fits = [parity for parity, _ in admitted(shift) if parity in TOP_ROWS]
    return fits[0] if fits else None


def exponent_list():
    listed = []
    for accumulated in range(ORDER + 1):
        for height in (0, 1):
            for power_x in range(accumulated - height + 1):
                listed.append((power_x, accumulated - height - power_x, height))
    return listed


def triple_groups():
    shifts = offset_table()
    groups = {}
    for triple in range(TRIPLES):
        members = shifts[3 * triple : 3 * triple + 3]
        parities = tuple(sorted({parity for shift in members for parity, _ in admitted(shift)}))
        extra = [EXTRA_TILES[admitted(shift)[0][0]] for shift in members if top_parity(shift) is None]
        groups.setdefault((parities, bool(extra)), []).append(triple)
    return sorted(groups.items(), key=lambda item: (-len(item[0][0]), item[0]))


def slope_matrix():
    listed = exponent_list()
    place = {e: i for i, e in enumerate(listed)}
    matrix = np.zeros((TERMS, 3 * LANES), np.float32)
    for row, (a, b, c) in enumerate(listed):
        if a > 0:
            matrix[row, place[(a - 1, b, c)]] = a
        if b > 0:
            matrix[row, LANES + place[(a, b - 1, c)]] = b
        if c > 0:
            matrix[row, 2 * LANES + place[(a, b, c - 1)]] = c
    return matrix


def lanes_nt(lhs, rhs):
    return lax.dot_general(lhs, rhs, (((1,), (1,)), ((), ())), preferred_element_type=F32)


def halves(value):
    upper = value.astype(BF16)
    return upper, (value - upper.astype(F32)).astype(BF16)


def split_nt(value, rhs):
    rows = value.shape[0]
    if rows % 8:
        value = jnp.concatenate([value, jnp.zeros((8 - rows, value.shape[1]), F32)], axis=0)
    size = value.shape[0]
    both = lanes_nt(jnp.concatenate(halves(value), axis=0), rhs)
    return (both[:size] + both[size:])[:rows]


def widen(value):
    return jnp.concatenate([value, jnp.zeros((value.shape[0], LANES - value.shape[1]), F32)], axis=1)


def power_of(base, exponents):
    square = base * base
    fourth = square * square
    eighth = fourth * fourth
    result = jnp.where((exponents & 1) != 0, base, 1.0)
    result = result * jnp.where((exponents & 2) != 0, square, 1.0)
    result = result * jnp.where((exponents & 4) != 0, fourth, 1.0)
    return jnp.where(exponents == 8, eighth, result)


def exponents():
    row = lax.broadcasted_iota(jnp.int32, (KPAD, LANES), 0)
    degree = jnp.zeros((KPAD, LANES), jnp.int32)
    for n in range(1, ORDER + 1):
        degree = degree + (row >= n * n).astype(jnp.int32)
    place = row - degree * degree
    height = (place > degree).astype(jnp.int32)
    power_x = place - height * (degree + 1)
    return power_x, degree - height - power_x, height, row < TERMS


def monomial_tiles(rows_of, high_ref, low_ref):
    power_x, power_y, power_z, valid = exponents()
    for tile in range(16):
        px, py, ox, oy = tile >> 3, tile >> 2 & 1, tile >> 1 & 1, tile & 1
        row_x, row_y, row_z = rows_of(2 * px + ox, 2 * py + oy)
        full = lambda row: jnp.broadcast_to(row - 0.5, (KPAD, LANES))
        value = power_of(full(row_x), power_x) * power_of(full(row_y), power_y)
        value = value * jnp.where(power_z != 0, full(row_z), 1.0)
        value = jnp.where(valid, value, 0.0)
        upper, lower = halves(value)
        high_ref[:, tile * LANES : (tile + 1) * LANES] = upper
        low_ref[:, tile * LANES : (tile + 1) * LANES] = lower


def octant_operators(native_ref, rows_ref):
    rows_ref[:, :TERMS] = native_ref[...].astype(F32).reshape(TERMS * 8, TERMS)


def octant_operator(rows_ref, octant):
    return rows_ref[pl.ds(octant, TERMS, stride=8), :][:, :TERMS].astype(BF16)


def prepare(pos_ref, chg_ref, cnt_ref, data_ref, live_ref):
    counts = jnp.concatenate([cnt_ref[x] for x in range(4)], axis=0).astype(F32).astype(BF16)
    spread = (
        lax.broadcasted_iota(jnp.int32, (4, LANES), 1) // SLOTS == lax.broadcasted_iota(jnp.int32, (4, LANES), 0)
    ).astype(F32).astype(BF16)
    limit = jnp.dot(counts, spread, preferred_element_type=F32)
    slot_of = (lax.broadcasted_iota(jnp.int32, (16, LANES), 1) % SLOTS).astype(F32)
    live = (slot_of < limit).astype(F32)
    for x in range(4):
        live_ref[x] = live[4 * x : 4 * x + 4]
        for y in range(4):
            for c in range(3):
                data_ref[x, y, c : c + 1, :] = pos_ref[c, x, y : y + 1, :]
            data_ref[x, y, 3:4, :] = chg_ref[x, y : y + 1, :] * live[4 * x + y : 4 * x + y + 1]


def rows_from(data_ref):
    return lambda x, y: tuple(data_ref[x, y, c : c + 1, :] for c in range(3))


def moments(data_ref, operator_rows, leaf_ref, mid_ref, top_ref, high_ref, low_ref):
    row = lax.broadcasted_iota(jnp.int32, (16, LANES), 0)
    lane = lax.broadcasted_iota(jnp.int32, (16, LANES), 1)
    for group in range(4):
        px, py = group >> 1, group & 1
        pieces = []
        for tile in range(4):
            ox, oy = tile >> 1, tile & 1
            hit = (row // 8 == lane // 64) & (row % 8 == ox * 4 + oy * 2 + lane // 32 % 2)
            weight = jnp.broadcast_to(data_ref[2 * px + ox, 2 * py + oy, 3:4, :], (16, LANES))
            pieces.append(jnp.where(hit, weight, 0.0))
        upper, lower = halves(jnp.concatenate(pieces, axis=1))
        span = slice(group * 512, group * 512 + 512)
        both = lanes_nt(jnp.concatenate([upper, lower], axis=0), high_ref[:, span])
        total = widen(both[:16] + both[16:] + lanes_nt(upper, low_ref[:, span]))
        leaf_ref[px, py, 0] = total[:8]
        leaf_ref[px, py, 1] = total[8:]
    mid = jnp.zeros((8, TERMS), F32)
    top = jnp.zeros((8, TERMS), F32)
    which = lax.broadcasted_iota(jnp.int32, (8, TERMS), 0)
    tiles = [leaf_ref[p >> 2, p >> 1 & 1, p & 1] for p in range(8)]
    operators = [octant_operator(operator_rows, octant) for octant in range(8)]
    for octant in range(8):
        rows = jnp.concatenate([tile[octant : octant + 1] for tile in tiles], axis=0)
        mid = mid + split_nt(rows[:, :TERMS], operators[octant])
    mid_ref[...] = widen(mid)
    for octant in range(8):
        top = top + jnp.where(which == octant, split_nt(mid, operators[octant]), 0.0)
    top_ref[...] = widen(jnp.sum(top, axis=0, keepdims=True))


DIRECTIONS = [
    (dx, dy, dz) for dx in (-1, 0, 1) for dy in (-1, 0, 1) for dz in (-1, 0, 1) if (dx, dy, dz) != (0, 0, 0)
]


def span_of(step, own, first):
    if step == 0:
        return pl.ds(0, own), pl.ds(first, own)
    if step > 0:
        return pl.ds(own - 1, 1), pl.ds(first - 1, 1)
    return pl.ds(0, 1), pl.ds(first + own, 1)


def fill_cells(cells, ext_ref, turned_ref, table_ref):
    lane4 = lax.broadcasted_iota(jnp.int32, (4, LANES), 1)
    for x, y in cells:
        before, here, after = ext_ref[x, y, 0], ext_ref[x, y, 1], ext_ref[x, y, 2]
        turned_ref[x, y, 0] = pltpu.roll(jnp.where(lane4 >= 96, before, here), 32, 1)
        turned_ref[x, y, 1] = here
        turned_ref[x, y, 2] = pltpu.roll(jnp.where(lane4 < 32, after, here), 96, 1)
    lane = lax.broadcasted_iota(jnp.int32, (8, LANES), 1)
    base = lane // SLOTS * SLOTS + lax.broadcasted_iota(jnp.int32, (8, LANES), 0)

    def one_group(group, carry):
        pick = base + group * 8
        start = pl.multiple_of(group * 8, 8)
        for x, y in cells:
            for ez in range(3):
                for c in range(4):
                    row = jnp.broadcast_to(turned_ref[x, y, ez, c : c + 1, :], (8, LANES))
                    table_ref[x, y, ez, c, pl.ds(start, 8), :] = jnp.take_along_axis(row, pick, axis=1)
        return carry

    lax.fori_loop(0, 4, one_group, 0)


def load_wide(data_ref, x, y):
    mine = data_ref[x, y]
    return [jnp.broadcast_to(mine[c : c + 1], (8, LANES)) for c in range(3)]


def pair_sums(sums, here_x, here_y, here_z, x, y, table_ref):
    potential, field_x, field_y, field_z = sums
    for ez in range(3):
        for group in range(4):
            span = pl.ds(group * 8, 8)
            delta_x = here_x - table_ref[x, y, ez, 0, span, :]
            delta_y = here_y - table_ref[x, y, ez, 1, span, :]
            delta_z = here_z[ez] - table_ref[x, y, ez, 2, span, :]
            distance = delta_x * delta_x + delta_y * delta_y + (delta_z * delta_z + SOFTENING)
            inverse = lax.rsqrt(distance)
            weight = table_ref[x, y, ez, 3, span, :] * inverse
            cubic = weight * (inverse * inverse)
            potential = potential + weight
            field_x = field_x + cubic * delta_x
            field_y = field_y + cubic * delta_y
            field_z = field_z + cubic * delta_z
    return potential, field_x, field_y, field_z


def near_inside(rows, data_ref, table_ref, sums_ref):
    for y in rows:
        steps = [ey for ey in (-1, 0, 1) if 0 <= y + ey < 4]

        def along_x(x, carry):
            wide = load_wide(data_ref, x, y)
            here_z = [wide[2] - float(ez - 1) for ez in range(3)]

            def around(ex, sums):
                here_x = wide[0] - (ex - 1).astype(F32)
                for ey in steps:
                    sums = pair_sums(sums, here_x, wide[1] - float(ey), here_z, x + ex, y + ey + 1, table_ref)
                return sums

            zero = jnp.zeros((8, LANES), F32)
            low = 1 - jnp.minimum(x, 1)
            high = 2 + jnp.minimum(3 - x, 1)
            sums = lax.fori_loop(low, high, around, (zero, zero, zero, zero))
            for c in range(4):
                sums_ref[x, y, c] = sums[c]
            return carry

        lax.fori_loop(0, 4, along_x, 0)


def near_outside(data_ref, table_ref, sums_ref):
    for x, ex in ((0, -1), (3, 1)):

        def along_y(y, carry):
            wide = load_wide(data_ref, x, y)
            here_z = [wide[2] - float(ez - 1) for ez in range(3)]
            sums = tuple(sums_ref[x, y, c] for c in range(4))
            for ey in (-1, 0, 1):
                sums = pair_sums(
                    sums, wide[0] - float(ex), wide[1] - float(ey), here_z, x + ex + 1, y + ey + 1, table_ref
                )
            for c in range(4):
                sums_ref[x, y, c] = sums[c]
            return carry

        lax.fori_loop(0, 4, along_y, 0)
    for y, ey in ((0, -1), (3, 1)):
        for x in range(4):
            wide = load_wide(data_ref, x, y)
            here_z = [wide[2] - float(ez - 1) for ez in range(3)]
            sums = tuple(sums_ref[x, y, c] for c in range(4))
            for ex in (-1, 0, 1):
                if 0 <= x + ex < 4:
                    sums = pair_sums(
                        sums, wide[0] - float(ex), wide[1] - float(ey), here_z, x + ex + 1, y + ey + 1, table_ref
                    )
            for c in range(4):
                sums_ref[x, y, c] = sums[c]


def near_rows(sums_ref, data_ref, near_ref):
    self_weight = lax.rsqrt(jnp.full((1, LANES), SOFTENING, F32))
    for x in range(4):
        for y in range(4):
            near = [jnp.sum(sums_ref[x, y, c], axis=0, keepdims=True) for c in range(4)]
            near[0] = near[0] - data_ref[x, y, 3:4, :] * self_weight
            for c in range(4):
                near_ref[c, x, y : y + 1, :] = near[c]


def align_operators(first, last, whole_ref, aligned_ref):
    slots = {}
    for _, members in triple_groups():
        for triple in members:
            slots[triple] = len(slots)
    for triple in range(first, last):
        begin = triple * 3 * TERMS
        if begin + 256 <= whole_ref.shape[1]:
            piece = whole_ref[:, begin : begin + 256]
        else:
            tail = whole_ref[:, begin : OFFSETS * TERMS]
            piece = jnp.concatenate([tail, jnp.zeros((TERMS, 256 - tail.shape[1]), BF16)], axis=1)
        slot = slots[triple]
        aligned_ref[:TERMS, slot * 256 : (slot + 1) * 256] = piece


def clear_rows(rows_ref):
    def step(n, carry):
        for octant in range(8):
            rows_ref[pl.ds(pl.multiple_of(n * 128 + octant * 16 + 8, 8), 8), :] = jnp.zeros((8, LANES), F32)
        return carry

    lax.fori_loop(0, 27, step, 0)


def gather_boxes(wide_ref, mids_ref, rows_ref):
    for n in range(27):
        step_x, step_y, step_z = n // 9, n // 3 % 3, n % 3
        for parent in range(8):
            px, py, pz = parent >> 2, parent >> 1 & 1, parent & 1
            rows_ref[pl.ds(n * 128 + parent, 8, stride=16), :] = wide_ref[px + step_x, py + step_y, pz + step_z]
        rows_ref[pl.ds(n * 128 + 8, 8, stride=16), :] = mids_ref[n]


def gather_upper(tops, tops_ref, rows_ref):
    far_x = [lax.rem(tops[0] + step + 3, 4) * 2 for step in range(3)]
    far_y = [lax.rem(tops[1] + step + 1, 2) * 2 for step in range(3)]
    far_z = [lax.rem(tops[2] + step + 3, 4) * 2 for step in range(3)]
    for n in range(27):
        step_x, step_y, step_z = n // 9, n // 3 % 3, n % 3
        for octant in range(8):
            ox, oy, oz = octant >> 2, octant >> 1 & 1, octant & 1
            place = n * 128 + octant * 16 + 9
            rows_ref[place : place + 1, :] = tops_ref[far_x[step_x] + ox, far_y[step_y] + oy, far_z[step_z] + oz]


def convert_tiles(rows_ref, tiles_ref):
    lane = lax.broadcasted_iota(jnp.int32, (16, LANES), 1)
    zero = jnp.zeros((16, LANES), BF16)
    for tile in range(218):
        value = rows_ref[tile * 16 : tile * 16 + 16, :].astype(BF16)
        second = pltpu.roll(value, TERMS, 1)
        tiles_ref[0, tile] = value
        tiles_ref[1, tile] = jnp.where(lane >= TERMS, second, zero)
        tiles_ref[2, tile] = jnp.where(lane < TERMS, second, zero)
        tiles_ref[3, tile] = pltpu.roll(value, 2 * TERMS - LANES, 1)


def gather_top(tops, tops_ref, upper_ref, operators, lattice_ref, turned_ref, rows_ref):
    for octant in range(8):
        ox, oy, oz = octant >> 2, octant >> 1 & 1, octant & 1
        for box in range(32):
            bx, by, bz = box >> 3, box >> 2 & 1, box & 3
            upper_ref[octant, box : box + 1, :] = tops_ref[2 * bx + ox, 2 * by + oy, 2 * bz + oz]
    coarse = jnp.zeros((32, TERMS), F32)
    for octant in range(8):
        coarse = coarse + split_nt(upper_ref[octant][:, :TERMS], operators[octant])
    lattice_term = split_nt(jnp.sum(coarse, axis=0, keepdims=True), lattice_ref[...])
    row = lax.broadcasted_iota(jnp.int32, (32, 32), 0)
    column = lax.broadcasted_iota(jnp.int32, (32, 32), 1)
    wanted = (
        (row // 8 + tops[0]) % 4 * 8 + (row // 4 % 2 + tops[1]) % 2 * 4 + (row % 4 + tops[2]) % 4
    )
    turned_ref[...] = jnp.dot(
        (wanted == column).astype(F32).astype(BF16), widen(coarse).astype(BF16), preferred_element_type=F32
    )
    for shift in offset_table():
        parity = top_parity(shift)
        source = shift[0] % 4 * 8 + shift[1] % 2 * 4 + shift[2] % 4
        if parity is not None:
            place = [shift[axis] + (parity >> (2 - axis) & 1) for axis in range(3)]
            target = tile_of(place) * 16 + TOP_ROWS[parity]
            rows_ref[target : target + 1, :] = turned_ref[source : source + 1, :]
        else:
            target = EXTRA_TILES[admitted(shift)[0][0]] * 16
            which = lax.broadcasted_iota(jnp.int32, (16, LANES), 0)
            top = jnp.broadcast_to(turned_ref[source : source + 1, :], (16, LANES))
            rows_ref[target : target + 16, :] = jnp.where(which == 0, top, 0.0)
    return lattice_term


def far_products(tiles_ref, aligned_ref, acc_ref):
    total = [jnp.zeros((16, TERMS), F32) for _ in range(8)]
    extra = jnp.zeros((1, TERMS), F32)
    shifts = offset_table()
    empty = jnp.zeros((16, LANES), BF16)

    def lanes_of(sources):
        halves_of = ([], [])
        for position, tile in enumerate(sources):
            if tile is not None:
                for half, version in (((0, 0),), ((0, 1), (1, 2)), ((1, 3),))[position]:
                    halves_of[half].append(tiles_ref[version, tile])
        sides = [sum(side[1:], side[0]) if side else empty for side in halves_of]
        return jnp.concatenate(sides, axis=1)

    slot = 0
    for (parities, special), members in triple_groups():
        group = None
        for start in range(0, len(members), CHUNK):
            part = members[start : start + CHUNK]
            columns = []
            for triple in part:
                steps = shifts[3 * triple : 3 * triple + 3]
                places = [dict(admitted(step)) for step in steps]
                rows = [[tile_of(place[p]) if p in place else None for place in places] for p in parities]
                if special:
                    rows.append(
                        [EXTRA_TILES[admitted(step)[0][0]] if top_parity(step) is None else None for step in steps]
                    )
                columns.append(jnp.concatenate([lanes_of(sources) for sources in rows], axis=0))
            data = columns[0] if len(columns) == 1 else jnp.concatenate(columns, axis=1)
            product = lanes_nt(data, aligned_ref[:TERMS, slot * 256 : (slot + len(part)) * 256])
            slot += len(part)
            group = product if group is None else group + product
        for place, parity in enumerate(parities):
            total[parity] = total[parity] + group[place * 16 : place * 16 + 16]
        if special:
            extra = extra + group[len(parities) * 16 : len(parities) * 16 + 1]
    for parity in range(8):
        acc_ref[parity * 16 : parity * 16 + 16, :] = widen(total[parity])
    return extra


def down_operators(octant_own, down_rows, downs_ref):
    own = jnp.where(
        lax.broadcasted_iota(jnp.int32, (TERMS * 8, LANES), 0) % 8 == octant_own, down_rows[...], 0.0
    )
    downs_ref[8, :TERMS, :] = jnp.sum(own.reshape(TERMS, 8, LANES), axis=1).astype(BF16)
    for octant in range(8):
        downs_ref[octant, :TERMS, :TERMS] = octant_operator(down_rows, octant)


def locals_down(octant_own, acc_ref, lattice_term, downs_ref, local_ref):
    far_top = lattice_term
    for parity, place in TOP_ROWS.items():
        row = parity * 16 + place
        far_top = far_top + acc_ref[row : row + 1, :][:, :TERMS]
    operator = lambda octant: downs_ref[octant, :TERMS, :TERMS]
    local_upper = 0.25 * acc_ref[pl.ds(octant_own * 16 + 9, 1), :][:, :TERMS] + split_nt(
        0.125 * far_top, operator(8)
    )
    upper_wide = jnp.broadcast_to(local_upper, (8, TERMS))
    which = lax.broadcasted_iota(jnp.int32, (8, TERMS), 0)
    local_mid = 0.5 * acc_ref[pl.ds(8, 8, stride=16), :][:, :TERMS]
    for octant in range(8):
        local_mid = local_mid + jnp.where(which == octant, split_nt(upper_wide, operator(octant)), 0.0)
    for octant in range(8):
        local = acc_ref[octant * 16 : octant * 16 + 8, :][:, :TERMS] + split_nt(local_mid, operator(octant))
        local_ref[octant * 8 : octant * 8 + 8, :] = widen(local)


def evaluate(local_ref, slope_ref, high_ref, low_ref, near_ref, live_ref, out_ref):
    local_leaf = local_ref[...]
    upper, lower = halves(local_leaf[:, :TERMS])
    slopes = jnp.dot(upper, slope_ref[...], preferred_element_type=F32) + jnp.dot(
        lower, slope_ref[...], preferred_element_type=F32
    )
    parts = [local_leaf] + [slopes[:, c * LANES : (c + 1) * LANES] for c in range(3)]
    split_parts = [halves(part[:, :KPAD]) for part in parts]
    row = lax.broadcasted_iota(jnp.int32, (16, LANES), 0)
    lane = lax.broadcasted_iota(jnp.int32, (16, LANES), 1)
    for parity in range(4):
        span = slice(parity * 16, parity * 16 + 16)
        coef_high = jnp.concatenate([part[0][span] for part in split_parts], axis=0)
        coef_low = jnp.concatenate([part[1][span] for part in split_parts], axis=0)
        coef = jnp.concatenate([coef_high, coef_low], axis=0)
        for group in range(4):
            x, y = (group >> 1) * 2 + (parity >> 1), (group & 1) * 2 + (parity & 1)
            tile = group * 4 + parity
            lanes = slice(tile * LANES, tile * LANES + LANES)
            both = jnp.dot(coef, high_ref[:, lanes], preferred_element_type=F32)
            value = both[:64] + both[64:] + jnp.dot(coef_high, low_ref[:, lanes], preferred_element_type=F32)
            hit = (row // 8 == lane // 32 % 2) & (row % 8 == group * 2 + lane // 64)
            sums = [
                jnp.sum(jnp.where(hit, value[16 * c : 16 * c + 16], 0.0), axis=0, keepdims=True) for c in range(4)
            ]
            live = live_ref[x, y : y + 1, :]
            for c in range(4):
                near = near_ref[c, x, y : y + 1, :]
                value = near + sums[c] if c == 0 else near - sums[c]
                out_ref[c, x, y : y + 1, :] = value * live


def whole_kernel(
    nx,
    ny,
    nz,
    pos_hbm,
    chg_hbm,
    cnt_hbm,
    up_hbm,
    down_hbm,
    slope_hbm,
    lattice_hbm,
    far_hbm,
    out_ref,
    pos_ref,
    chg_ref,
    cnt_ref,
    up_ref,
    down_ref,
    slope_ref,
    lattice_ref,
    data_ref,
    live_ref,
    ext_ref,
    wide_ref,
    mids_ref,
    tops_ref,
    leaf_ref,
    mid_ref,
    top_ref,
    up_rows,
    down_rows,
    downs_ref,
    high_ref,
    low_ref,
    turned_ref,
    table_ref,
    sums_ref,
    near_ref,
    whole_ref,
    aligned_ref,
    rows_ref,
    tiles_ref,
    upper_ref,
    coarse_ref,
    acc_ref,
    local_ref,
    send,
    recv,
    gsend,
    grecv,
    own,
    load,
):
    ix, iy, iz = lax.axis_index("gx"), lax.axis_index("gy"), lax.axis_index("gz")

    def at(dx, dy, dz):
        return {
            "gx": lax.rem(ix + (dx + nx), nx),
            "gy": lax.rem(iy + (dy + ny), ny),
            "gz": lax.rem(iz + (dz + nz), nz),
        }

    plane = [(0, b, c) for b in range(ny) for c in range(nz) if b or c]
    line = [(a, 0, 0) for a in range(1, nx)]
    wrapped = lambda step: (step[0] % nx, step[1] % ny, step[2] % nz)
    partners = sorted({wrapped(step) for step in DIRECTIONS} | set(plane) | set(line))
    operands = ((pos_hbm, pos_ref), (chg_hbm, chg_ref), (cnt_hbm, cnt_ref), (up_hbm, up_ref))
    operands += ((down_hbm, down_ref), (slope_hbm, slope_ref), (lattice_hbm, lattice_ref))
    loads = [pltpu.make_async_copy(src, dst, load.at[k]) for k, (src, dst) in enumerate(operands)]
    pieces = []
    for k in range(PIECES):
        span = pl.ds(k * (25600 // PIECES), 25600 // PIECES)
        pieces.append(pltpu.make_async_copy(far_hbm.at[:, span], whole_ref.at[:, span], load.at[7 + k]))
    for copy in loads[:4]:
        copy.start()
    barrier = pltpu.get_barrier_semaphore()
    for step in partners:
        pl.semaphore_signal(barrier, inc=1, device_id=at(*step), device_id_type=MESH)
    for copy in pieces[:2] + loads[4:]:
        copy.start()
    octant_own = (ix % 2) * 4 + (iy % 2) * 2 + iz % 2
    for copy in loads[:4]:
        copy.wait()

    prepare(pos_ref, chg_ref, cnt_ref, data_ref, live_ref)
    octant_operators(up_ref, up_rows)
    monomial_tiles(rows_from(data_ref), high_ref, low_ref)

    pl.semaphore_wait(barrier, len(partners))

    def remote(src, dst, ssem, rsem, step):
        copy = pltpu.make_async_remote_copy(
            src_ref=src, dst_ref=dst, send_sem=ssem, recv_sem=rsem, device_id=at(*step), device_id_type=MESH
        )
        copy.start()
        return copy

    halo = {}
    order = sorted(range(len(DIRECTIONS)), key=lambda i: sum(abs(d) for d in DIRECTIONS[i][:2]))
    for index in order:
        dx, dy, dz = DIRECTIONS[index]
        from_x, to_x = span_of(dx, 4, 1)
        from_y, to_y = span_of(dy, 4, 1)
        src, dst = data_ref.at[from_x, from_y], ext_ref.at[to_x, to_y, 1 - dz]
        halo[index] = remote(src, dst, send.at[0, index], recv.at[0, index], DIRECTIONS[index])
    for copy in pieces[2:]:
        copy.start()
    moments(data_ref, up_rows, leaf_ref, mid_ref, top_ref, high_ref, low_ref)
    local = [
        pltpu.make_async_copy(data_ref, ext_ref.at[pl.ds(1, 4), pl.ds(1, 4), 1], own.at[0]),
        pltpu.make_async_copy(leaf_ref, wide_ref.at[pl.ds(1, 2), pl.ds(1, 2), pl.ds(1, 2)], own.at[1]),
        pltpu.make_async_copy(mid_ref, mids_ref.at[13], own.at[2]),
        pltpu.make_async_copy(top_ref, tops_ref.at[ix, iy, iz], own.at[3]),
    ]
    for copy in local:
        copy.start()
    first = [
        remote(top_ref, tops_ref.at[ix, iy, iz], gsend.at[k], grecv.at[k], step) for k, step in enumerate(plane)
    ]
    boxes = []
    for index, step in enumerate(DIRECTIONS):
        spans = [span_of(d, 2, 1) for d in step]
        src = leaf_ref.at[spans[0][0], spans[1][0], spans[2][0]]
        dst = wide_ref.at[spans[0][1], spans[1][1], spans[2][1]]
        boxes.append(remote(src, dst, send.at[1, index], recv.at[1, index], step))
        slot = ((1 - step[0]) * 3 + (1 - step[1])) * 3 + (1 - step[2])
        boxes.append(remote(mid_ref, mids_ref.at[slot], send.at[2, index], recv.at[2, index], step))

    clear_rows(rows_ref)
    done = 0
    for k in range(PIECES - 1):
        pieces[k].wait()
        ready = ((k + 1) * (25600 // PIECES) - 256) // (3 * TERMS)
        align_operators(done, ready, whole_ref, aligned_ref)
        done = ready
    for copy in local:
        copy.wait()
    for index in order[:2]:
        halo[index].wait()
    inside = [(x, y) for x in range(1, 5) for y in range(1, 5)]
    fill_cells(inside, ext_ref, turned_ref, table_ref)
    near_inside((0, 1, 2, 3), data_ref, table_ref, sums_ref)
    for copy in first:
        copy.wait()
    second = [
        remote(tops_ref.at[ix], tops_ref.at[ix], gsend.at[32 + k], grecv.at[32 + k], step)
        for k, step in enumerate(line)
    ]
    pieces[-1].wait()
    align_operators(done, TRIPLES, whole_ref, aligned_ref)
    for copy in loads[4:]:
        copy.wait()
    octant_operators(down_ref, down_rows)
    down_operators(octant_own, down_rows, downs_ref)
    for index in order[2:]:
        halo[index].wait()
    fill_cells(
        [(x, y) for x in range(6) for y in range(6) if (x, y) not in inside], ext_ref, turned_ref, table_ref
    )
    near_outside(data_ref, table_ref, sums_ref)
    near_rows(sums_ref, data_ref, near_ref)
    for copy in boxes:
        copy.wait()
    gather_boxes(wide_ref, mids_ref, rows_ref)
    for copy in second:
        copy.wait()
    tops = (ix // 2, iy // 2, iz // 2)
    gather_upper(tops, tops_ref, rows_ref)
    operators = [octant_operator(up_rows, octant) for octant in range(8)]
    lattice_term = gather_top(tops, tops_ref, upper_ref, operators, lattice_ref, coarse_ref, rows_ref)
    convert_tiles(rows_ref, tiles_ref)
    extra = far_products(tiles_ref, aligned_ref, acc_ref)
    locals_down(octant_own, acc_ref, lattice_term + extra, downs_ref, local_ref)
    evaluate(local_ref, slope_ref, high_ref, low_ref, near_ref, live_ref, out_ref)


VMEM = pl.BlockSpec(memory_space=pltpu.VMEM)


def shape(*dims):
    return jax.ShapeDtypeStruct(dims, F32)


def whole_call(sizes, *operands):
    dma = pltpu.SemaphoreType.DMA
    return pl.pallas_call(
        functools.partial(whole_kernel, *sizes),
        out_shape=shape(4, 4, 4, LANES),
        in_specs=[pl.BlockSpec(memory_space=pltpu.HBM)] * 8,
        out_specs=VMEM,
        scratch_shapes=[
            pltpu.VMEM((3, 4, 4, LANES), F32),
            pltpu.VMEM((4, 4, LANES), F32),
            pltpu.VMEM((4, 4, 4), jnp.int32),
            pltpu.VMEM((TERMS, 8, TERMS), BF16),
            pltpu.VMEM((TERMS, 8, TERMS), BF16),
            pltpu.VMEM((TERMS, 3 * LANES), BF16),
            pltpu.VMEM((TERMS, TERMS), BF16),
            pltpu.VMEM((4, 4, 4, LANES), F32),
            pltpu.VMEM((4, 4, LANES), F32),
            pltpu.VMEM((6, 6, 3, 4, LANES), F32),
            pltpu.VMEM((4, 4, 4, 8, LANES), F32),
            pltpu.VMEM((27, 8, LANES), F32),
            pltpu.VMEM((*sizes, 1, LANES), F32),
            pltpu.VMEM((2, 2, 2, 8, LANES), F32),
            pltpu.VMEM((8, LANES), F32),
            pltpu.VMEM((1, LANES), F32),
            pltpu.VMEM((TERMS * 8, LANES), F32),
            pltpu.VMEM((TERMS * 8, LANES), F32),
            pltpu.VMEM((9, KPAD, LANES), BF16),
            pltpu.VMEM((KPAD, 2048), BF16),
            pltpu.VMEM((KPAD, 2048), BF16),
            pltpu.VMEM((6, 6, 3, 4, LANES), F32),
            pltpu.VMEM((6, 6, 3, 4, SLOTS, LANES), F32),
            pltpu.VMEM((4, 4, 4, 8, LANES), F32),
            pltpu.VMEM((4, 4, 4, LANES), F32),
            pltpu.VMEM((TERMS, 25600), BF16),
            pltpu.VMEM((KPAD, TRIPLES * 256), BF16),
            pltpu.VMEM((218 * 16, LANES), F32),
            pltpu.VMEM((4, 218, 16, LANES), BF16),
            pltpu.VMEM((8, 32, LANES), F32),
            pltpu.VMEM((32, LANES), F32),
            pltpu.VMEM((LANES, LANES), F32),
            pltpu.VMEM((64, LANES), F32),
            dma((3, 26)),
            dma((3, 26)),
            dma((40,)),
            dma((40,)),
            dma((4,)),
            dma((7 + PIECES,)),
        ],
        compiler_params=pltpu.CompilerParams(collective_id=0, has_side_effects=True),
        name="whole",
    )(*operands)


def part_kernel(both_ref, pot_ref, field_ref):
    pot_ref[...] = both_ref[0]
    field_ref[...] = both_ref[1:4]


def part_call(both):
    return pl.pallas_call(
        part_kernel,
        out_shape=(shape(4, 4, LANES), shape(3, 4, 4, LANES)),
        in_specs=[VMEM],
        out_specs=(VMEM,) * 2,
        name="part",
    )(both)


def solution(mesh):
    sizes = tuple(mesh.shape[axis] for axis in ("gx", "gy", "gz"))

    def per_device(
        positions, charges, counts, moment_shift, far_operators, local_shift, lattice_operator
    ):
        slope = jnp.asarray(slope_matrix()).astype(BF16)
        native_up = jnp.transpose(moment_shift, (1, 0, 2))
        native_down = jnp.transpose(local_shift, (1, 0, 2))
        both = whole_call(
            sizes,
            positions,
            charges,
            counts,
            native_up,
            native_down,
            slope,
            lattice_operator,
            far_operators,
        )
        return part_call(both)

    placed = (
        P(None, "gx", "gy", "gz"),
        P("gx", "gy", "gz"),
        P("gx", "gy", "gz"),
        P(),
        P(),
        P(),
        P(),
    )
    return jax.shard_map(
        per_device,
        mesh=mesh,
        in_specs=placed,
        out_specs=(P("gx", "gy", "gz"), P(None, "gx", "gy", "gz")),
        check_vma=False,
    )
```

```python
import functools

import jax
import jax.numpy as jnp
import numpy as np
from jax import lax
from jax.experimental import pallas as pl
from jax.experimental.pallas import tpu as pltpu
from jax.sharding import PartitionSpec as P

ORDER = 8
SLOTS = 32
SOFTENING = 0.0625
TERMS = 81
KPAD = 96
LANES = 128
OFFSETS = 316
CHUNK = 2
PIECES = 4
MESH = pl.DeviceIdType.MESH
F32 = jnp.float32
BF16 = jnp.bfloat16


def offset_table():
    listed = []
    for shift_x in range(-3, 4):
        for shift_y in range(-3, 4):
            for shift_z in range(-3, 4):
                if max(abs(shift_x), abs(shift_y), abs(shift_z)) >= 2:
                    listed.append((shift_x, shift_y, shift_z))
    return listed


def admitted(shift):
    listed = []
    for parity in range(8):
        place = [shift[axis] + (parity >> (2 - axis) & 1) for axis in range(3)]
        if all(-2 <= c <= 3 for c in place):
            listed.append((parity, tuple(place)))
    return listed


def tile_of(place):
    around = [(c + 2) // 2 for c in place]
    inner = [(c + 2) % 2 for c in place]
    return ((around[0] * 3 + around[1]) * 3 + around[2]) * 8 + inner[0] * 4 + inner[1] * 2 + inner[2]


TOP_ROWS = {0: 10, 7: 11, 3: 12, 4: 13, 1: 14, 6: 15}
EXTRA_TILES = {2: 216, 5: 217}
TRIPLES = 106


def top_parity(shift):
    if min(shift) > -3:
        return 0
    if max(shift) < 3:
        return 7
    fits = [parity for parity, _ in admitted(shift) if parity in TOP_ROWS]
    return fits[0] if fits else None


def exponent_list():
    listed = []
    for accumulated in range(ORDER + 1):
        for height in (0, 1):
            for power_x in range(accumulated - height + 1):
                listed.append((power_x, accumulated - height - power_x, height))
    return listed


def triple_groups():
    shifts = offset_table()
    groups = {}
    for triple in range(TRIPLES):
        members = shifts[3 * triple : 3 * triple + 3]
        parities = tuple(sorted({parity for shift in members for parity, _ in admitted(shift)}))
        extra = [EXTRA_TILES[admitted(shift)[0][0]] for shift in members if top_parity(shift) is None]
        groups.setdefault((parities, bool(extra)), []).append(triple)
    return sorted(groups.items(), key=lambda item: (-len(item[0][0]), item[0]))


def slope_matrix():
    listed = exponent_list()
    place = {e: i for i, e in enumerate(listed)}
    matrix = np.zeros((TERMS, 3 * LANES), np.float32)
    for row, (a, b, c) in enumerate(listed):
        if a > 0:
            matrix[row, place[(a - 1, b, c)]] = a
        if b > 0:
            matrix[row, LANES + place[(a, b - 1, c)]] = b
        if c > 0:
            matrix[row, 2 * LANES + place[(a, b, c - 1)]] = c
    return matrix


def lanes_nt(lhs, rhs):
    return lax.dot_general(lhs, rhs, (((1,), (1,)), ((), ())), preferred_element_type=F32)


def halves(value):
    upper = value.astype(BF16)
    return upper, (value - upper.astype(F32)).astype(BF16)


def split_nt(value, rhs):
    rows = value.shape[0]
    if rows % 8:
        value = jnp.concatenate([value, jnp.zeros((8 - rows, value.shape[1]), F32)], axis=0)
    size = value.shape[0]
    both = lanes_nt(jnp.concatenate(halves(value), axis=0), rhs)
    return (both[:size] + both[size:])[:rows]


def widen(value):
    return jnp.concatenate([value, jnp.zeros((value.shape[0], LANES - value.shape[1]), F32)], axis=1)


def power_of(base, exponents):
    square = base * base
    fourth = square * square
    eighth = fourth * fourth
    result = jnp.where((exponents & 1) != 0, base, 1.0)
    result = result * jnp.where((exponents & 2) != 0, square, 1.0)
    result = result * jnp.where((exponents & 4) != 0, fourth, 1.0)
    return jnp.where(exponents == 8, eighth, result)


def exponents():
    row = lax.broadcasted_iota(jnp.int32, (KPAD, LANES), 0)
    degree = jnp.zeros((KPAD, LANES), jnp.int32)
    for n in range(1, ORDER + 1):
        degree = degree + (row >= n * n).astype(jnp.int32)
    place = row - degree * degree
    height = (place > degree).astype(jnp.int32)
    power_x = place - height * (degree + 1)
    return power_x, degree - height - power_x, height, row < TERMS


def monomial_tiles(rows_of, high_ref, low_ref):
    power_x, power_y, power_z, valid = exponents()
    for tile in range(16):
        px, py, ox, oy = tile >> 3, tile >> 2 & 1, tile >> 1 & 1, tile & 1
        row_x, row_y, row_z = rows_of(2 * px + ox, 2 * py + oy)
        full = lambda row: jnp.broadcast_to(row - 0.5, (KPAD, LANES))
        value = power_of(full(row_x), power_x) * power_of(full(row_y), power_y)
        value = value * jnp.where(power_z != 0, full(row_z), 1.0)
        value = jnp.where(valid, value, 0.0)
        upper, lower = halves(value)
        high_ref[:, tile * LANES : (tile + 1) * LANES] = upper
        low_ref[:, tile * LANES : (tile + 1) * LANES] = lower


def octant_operators(native_ref, rows_ref):
    rows_ref[:, :TERMS] = native_ref[...].astype(F32).reshape(TERMS * 8, TERMS)


def octant_operator(rows_ref, octant):
    return rows_ref[pl.ds(octant, TERMS, stride=8), :][:, :TERMS].astype(BF16)


def prepare(pos_ref, chg_ref, cnt_ref, data_ref, live_ref):
    counts = jnp.concatenate([cnt_ref[x] for x in range(4)], axis=0).astype(F32).astype(BF16)
    spread = (
        lax.broadcasted_iota(jnp.int32, (4, LANES), 1) // SLOTS == lax.broadcasted_iota(jnp.int32, (4, LANES), 0)
    ).astype(F32).astype(BF16)
    limit = jnp.dot(counts, spread, preferred_element_type=F32)
    slot_of = (lax.broadcasted_iota(jnp.int32, (16, LANES), 1) % SLOTS).astype(F32)
    live = (slot_of < limit).astype(F32)
    for x in range(4):
        live_ref[x] = live[4 * x : 4 * x + 4]
        for y in range(4):
            for c in range(3):
                data_ref[x, y, c : c + 1, :] = pos_ref[c, x, y : y + 1, :]
            data_ref[x, y, 3:4, :] = chg_ref[x, y : y + 1, :] * live[4 * x + y : 4 * x + y + 1]


def rows_from(data_ref):
    return lambda x, y: tuple(data_ref[x, y, c : c + 1, :] for c in range(3))


def moments(data_ref, operator_rows, leaf_ref, mid_ref, top_ref, high_ref, low_ref):
    row = lax.broadcasted_iota(jnp.int32, (16, LANES), 0)
    lane = lax.broadcasted_iota(jnp.int32, (16, LANES), 1)
    for group in range(4):
        px, py = group >> 1, group & 1
        pieces = []
        for tile in range(4):
            ox, oy = tile >> 1, tile & 1
            hit = (row // 8 == lane // 64) & (row % 8 == ox * 4 + oy * 2 + lane // 32 % 2)
            weight = jnp.broadcast_to(data_ref[2 * px + ox, 2 * py + oy, 3:4, :], (16, LANES))
            pieces.append(jnp.where(hit, weight, 0.0))
        upper, lower = halves(jnp.concatenate(pieces, axis=1))
        span = slice(group * 512, group * 512 + 512)
        both = lanes_nt(jnp.concatenate([upper, lower], axis=0), high_ref[:, span])
        total = widen(both[:16] + both[16:] + lanes_nt(upper, low_ref[:, span]))
        leaf_ref[px, py, 0] = total[:8]
        leaf_ref[px, py, 1] = total[8:]
    mid = jnp.zeros((8, TERMS), F32)
    top = jnp.zeros((8, TERMS), F32)
    which = lax.broadcasted_iota(jnp.int32, (8, TERMS), 0)
    tiles = [leaf_ref[p >> 2, p >> 1 & 1, p & 1] for p in range(8)]
    operators = [octant_operator(operator_rows, octant) for octant in range(8)]
    for octant in range(8):
        rows = jnp.concatenate([tile[octant : octant + 1] for tile in tiles], axis=0)
        mid = mid + split_nt(rows[:, :TERMS], operators[octant])
    mid_ref[...] = widen(mid)
    for octant in range(8):
        top = top + jnp.where(which == octant, split_nt(mid, operators[octant]), 0.0)
    top_ref[...] = widen(jnp.sum(top, axis=0, keepdims=True))


DIRECTIONS = [
    (dx, dy, dz) for dx in (-1, 0, 1) for dy in (-1, 0, 1) for dz in (-1, 0, 1) if (dx, dy, dz) != (0, 0, 0)
]


def span_of(step, own, first):
    if step == 0:
        return pl.ds(0, own), pl.ds(first, own)
    if step > 0:
        return pl.ds(own - 1, 1), pl.ds(first - 1, 1)
    return pl.ds(0, 1), pl.ds(first + own, 1)


def fill_cells(cells, ext_ref, turned_ref, table_ref):
    lane4 = lax.broadcasted_iota(jnp.int32, (4, LANES), 1)
    for x, y in cells:
        before, here, after = ext_ref[x, y, 0], ext_ref[x, y, 1], ext_ref[x, y, 2]
        turned_ref[x, y, 0] = pltpu.roll(jnp.where(lane4 >= 96, before, here), 32, 1)
        turned_ref[x, y, 1] = here
        turned_ref[x, y, 2] = pltpu.roll(jnp.where(lane4 < 32, after, here), 96, 1)
    lane = lax.broadcasted_iota(jnp.int32, (8, LANES), 1)
    base = lane // SLOTS * SLOTS + lax.broadcasted_iota(jnp.int32, (8, LANES), 0)

    def one_group(group, carry):
        pick = base + group * 8
        start = pl.multiple_of(group * 8, 8)
        for x, y in cells:
            for ez in range(3):
                for c in range(4):
                    row = jnp.broadcast_to(turned_ref[x, y, ez, c : c + 1, :], (8, LANES))
                    table_ref[x, y, ez, c, pl.ds(start, 8), :] = jnp.take_along_axis(row, pick, axis=1)
        return carry

    lax.fori_loop(0, 4, one_group, 0)


def load_wide(data_ref, x, y):
    mine = data_ref[x, y]
    return [jnp.broadcast_to(mine[c : c + 1], (8, LANES)) for c in range(3)]


def pair_sums(sums, here_x, here_y, here_z, x, y, table_ref):
    potential, field_x, field_y, field_z = sums
    for ez in range(3):
        for group in range(4):
            span = pl.ds(group * 8, 8)
            delta_x = here_x - table_ref[x, y, ez, 0, span, :]
            delta_y = here_y - table_ref[x, y, ez, 1, span, :]
            delta_z = here_z[ez] - table_ref[x, y, ez, 2, span, :]
            distance = delta_x * delta_x + delta_y * delta_y + (delta_z * delta_z + SOFTENING)
            inverse = lax.rsqrt(distance)
            weight = table_ref[x, y, ez, 3, span, :] * inverse
            cubic = weight * (inverse * inverse)
            potential = potential + weight
            field_x = field_x + cubic * delta_x
            field_y = field_y + cubic * delta_y
            field_z = field_z + cubic * delta_z
    return potential, field_x, field_y, field_z


def near_inside(rows, data_ref, table_ref, sums_ref):
    for y in rows:
        steps = [ey for ey in (-1, 0, 1) if 0 <= y + ey < 4]

        def along_x(x, carry):
            wide = load_wide(data_ref, x, y)
            here_z = [wide[2] - float(ez - 1) for ez in range(3)]

            def around(ex, sums):
                here_x = wide[0] - (ex - 1).astype(F32)
                for ey in steps:
                    sums = pair_sums(sums, here_x, wide[1] - float(ey), here_z, x + ex, y + ey + 1, table_ref)
                return sums

            zero = jnp.zeros((8, LANES), F32)
            low = 1 - jnp.minimum(x, 1)
            high = 2 + jnp.minimum(3 - x, 1)
            sums = lax.fori_loop(low, high, around, (zero, zero, zero, zero))
            for c in range(4):
                sums_ref[x, y, c] = sums[c]
            return carry

        lax.fori_loop(0, 4, along_x, 0)


def near_outside(data_ref, table_ref, sums_ref):
    for x, ex in ((0, -1), (3, 1)):

        def along_y(y, carry):
            wide = load_wide(data_ref, x, y)
            here_z = [wide[2] - float(ez - 1) for ez in range(3)]
            sums = tuple(sums_ref[x, y, c] for c in range(4))
            for ey in (-1, 0, 1):
                sums = pair_sums(
                    sums, wide[0] - float(ex), wide[1] - float(ey), here_z, x + ex + 1, y + ey + 1, table_ref
                )
            for c in range(4):
                sums_ref[x, y, c] = sums[c]
            return carry

        lax.fori_loop(0, 4, along_y, 0)
    for y, ey in ((0, -1), (3, 1)):
        for x in range(4):
            wide = load_wide(data_ref, x, y)
            here_z = [wide[2] - float(ez - 1) for ez in range(3)]
            sums = tuple(sums_ref[x, y, c] for c in range(4))
            for ex in (-1, 0, 1):
                if 0 <= x + ex < 4:
                    sums = pair_sums(
                        sums, wide[0] - float(ex), wide[1] - float(ey), here_z, x + ex + 1, y + ey + 1, table_ref
                    )
            for c in range(4):
                sums_ref[x, y, c] = sums[c]


def near_rows(sums_ref, data_ref, near_ref):
    self_weight = lax.rsqrt(jnp.full((1, LANES), SOFTENING, F32))
    for x in range(4):
        for y in range(4):
            near = [jnp.sum(sums_ref[x, y, c], axis=0, keepdims=True) for c in range(4)]
            near[0] = near[0] - data_ref[x, y, 3:4, :] * self_weight
            for c in range(4):
                near_ref[c, x, y : y + 1, :] = near[c]


def align_operators(first, last, whole_ref, aligned_ref):
    slots = {}
    for _, members in triple_groups():
        for triple in members:
            slots[triple] = len(slots)
    for triple in range(first, last):
        begin = triple * 3 * TERMS
        if begin + 256 <= whole_ref.shape[1]:
            piece = whole_ref[:, begin : begin + 256]
        else:
            tail = whole_ref[:, begin : OFFSETS * TERMS]
            piece = jnp.concatenate([tail, jnp.zeros((TERMS, 256 - tail.shape[1]), BF16)], axis=1)
        slot = slots[triple]
        aligned_ref[:TERMS, slot * 256 : (slot + 1) * 256] = piece


def clear_rows(rows_ref):
    def step(n, carry):
        for octant in range(8):
            rows_ref[pl.ds(pl.multiple_of(n * 128 + octant * 16 + 8, 8), 8), :] = jnp.zeros((8, LANES), F32)
        return carry

    lax.fori_loop(0, 27, step, 0)


def gather_boxes(wide_ref, mids_ref, rows_ref):
    for n in range(27):
        step_x, step_y, step_z = n // 9, n // 3 % 3, n % 3
        for parent in range(8):
            px, py, pz = parent >> 2, parent >> 1 & 1, parent & 1
            rows_ref[pl.ds(n * 128 + parent, 8, stride=16), :] = wide_ref[px + step_x, py + step_y, pz + step_z]
        rows_ref[pl.ds(n * 128 + 8, 8, stride=16), :] = mids_ref[n]


def gather_upper(tops, tops_ref, rows_ref):
    far_x = [lax.rem(tops[0] + step + 3, 4) * 2 for step in range(3)]
    far_y = [lax.rem(tops[1] + step + 1, 2) * 2 for step in range(3)]
    far_z = [lax.rem(tops[2] + step + 3, 4) * 2 for step in range(3)]
    for n in range(27):
        step_x, step_y, step_z = n // 9, n // 3 % 3, n % 3
        for octant in range(8):
            ox, oy, oz = octant >> 2, octant >> 1 & 1, octant & 1
            place = n * 128 + octant * 16 + 9
            rows_ref[place : place + 1, :] = tops_ref[far_x[step_x] + ox, far_y[step_y] + oy, far_z[step_z] + oz]


def convert_tiles(rows_ref, tiles_ref):
    lane = lax.broadcasted_iota(jnp.int32, (16, LANES), 1)
    zero = jnp.zeros((16, LANES), BF16)
    for tile in range(218):
        value = rows_ref[tile * 16 : tile * 16 + 16, :].astype(BF16)
        second = pltpu.roll(value, TERMS, 1)
        tiles_ref[0, tile] = value
        tiles_ref[1, tile] = jnp.where(lane >= TERMS, second, zero)
        tiles_ref[2, tile] = jnp.where(lane < TERMS, second, zero)
        tiles_ref[3, tile] = pltpu.roll(value, 2 * TERMS - LANES, 1)


def gather_top(tops, tops_ref, upper_ref, operators, lattice_ref, turned_ref, rows_ref):
    for octant in range(8):
        ox, oy, oz = octant >> 2, octant >> 1 & 1, octant & 1
        for box in range(32):
            bx, by, bz = box >> 3, box >> 2 & 1, box & 3
            upper_ref[octant, box : box + 1, :] = tops_ref[2 * bx + ox, 2 * by + oy, 2 * bz + oz]
    coarse = jnp.zeros((32, TERMS), F32)
    for octant in range(8):
        coarse = coarse + split_nt(upper_ref[octant][:, :TERMS], operators[octant])
    lattice_term = split_nt(jnp.sum(coarse, axis=0, keepdims=True), lattice_ref[...])
    row = lax.broadcasted_iota(jnp.int32, (32, 32), 0)
    column = lax.broadcasted_iota(jnp.int32, (32, 32), 1)
    wanted = (
        (row // 8 + tops[0]) % 4 * 8 + (row // 4 % 2 + tops[1]) % 2 * 4 + (row % 4 + tops[2]) % 4
    )
    turned_ref[...] = jnp.dot(
        (wanted == column).astype(F32).astype(BF16), widen(coarse).astype(BF16), preferred_element_type=F32
    )
    for shift in offset_table():
        parity = top_parity(shift)
        source = shift[0] % 4 * 8 + shift[1] % 2 * 4 + shift[2] % 4
        if parity is not None:
            place = [shift[axis] + (parity >> (2 - axis) & 1) for axis in range(3)]
            target = tile_of(place) * 16 + TOP_ROWS[parity]
            rows_ref[target : target + 1, :] = turned_ref[source : source + 1, :]
        else:
            target = EXTRA_TILES[admitted(shift)[0][0]] * 16
            which = lax.broadcasted_iota(jnp.int32, (16, LANES), 0)
            top = jnp.broadcast_to(turned_ref[source : source + 1, :], (16, LANES))
            rows_ref[target : target + 16, :] = jnp.where(which == 0, top, 0.0)
    return lattice_term


def far_products(tiles_ref, aligned_ref, acc_ref):
    total = [jnp.zeros((16, TERMS), F32) for _ in range(8)]
    extra = jnp.zeros((1, TERMS), F32)
    shifts = offset_table()
    empty = jnp.zeros((16, LANES), BF16)

    def lanes_of(sources):
        halves_of = ([], [])
        for position, tile in enumerate(sources):
            if tile is not None:
                for half, version in (((0, 0),), ((0, 1), (1, 2)), ((1, 3),))[position]:
                    halves_of[half].append(tiles_ref[version, tile])
        sides = [sum(side[1:], side[0]) if side else empty for side in halves_of]
        return jnp.concatenate(sides, axis=1)

    slot = 0
    for (parities, special), members in triple_groups():
        group = None
        for start in range(0, len(members), CHUNK):
            part = members[start : start + CHUNK]
            columns = []
            for triple in part:
                steps = shifts[3 * triple : 3 * triple + 3]
                places = [dict(admitted(step)) for step in steps]
                rows = [[tile_of(place[p]) if p in place else None for place in places] for p in parities]
                if special:
                    rows.append(
                        [EXTRA_TILES[admitted(step)[0][0]] if top_parity(step) is None else None for step in steps]
                    )
                columns.append(jnp.concatenate([lanes_of(sources) for sources in rows], axis=0))
            data = columns[0] if len(columns) == 1 else jnp.concatenate(columns, axis=1)
            product = lanes_nt(data, aligned_ref[:TERMS, slot * 256 : (slot + len(part)) * 256])
            slot += len(part)
            group = product if group is None else group + product
        for place, parity in enumerate(parities):
            total[parity] = total[parity] + group[place * 16 : place * 16 + 16]
        if special:
            extra = extra + group[len(parities) * 16 : len(parities) * 16 + 1]
    for parity in range(8):
        acc_ref[parity * 16 : parity * 16 + 16, :] = widen(total[parity])
    return extra


def down_operators(octant_own, down_rows, downs_ref):
    own = jnp.where(
        lax.broadcasted_iota(jnp.int32, (TERMS * 8, LANES), 0) % 8 == octant_own, down_rows[...], 0.0
    )
    downs_ref[8, :TERMS, :] = jnp.sum(own.reshape(TERMS, 8, LANES), axis=1).astype(BF16)
    for octant in range(8):
        downs_ref[octant, :TERMS, :TERMS] = octant_operator(down_rows, octant)


def locals_down(octant_own, acc_ref, lattice_term, downs_ref, local_ref):
    far_top = lattice_term
    for parity, place in TOP_ROWS.items():
        row = parity * 16 + place
        far_top = far_top + acc_ref[row : row + 1, :][:, :TERMS]
    operator = lambda octant: downs_ref[octant, :TERMS, :TERMS]
    local_upper = 0.25 * acc_ref[pl.ds(octant_own * 16 + 9, 1), :][:, :TERMS] + split_nt(
        0.125 * far_top, operator(8)
    )
    upper_wide = jnp.broadcast_to(local_upper, (8, TERMS))
    which = lax.broadcasted_iota(jnp.int32, (8, TERMS), 0)
    local_mid = 0.5 * acc_ref[pl.ds(8, 8, stride=16), :][:, :TERMS]
    for octant in range(8):
        local_mid = local_mid + jnp.where(which == octant, split_nt(upper_wide, operator(octant)), 0.0)
    for octant in range(8):
        local = acc_ref[octant * 16 : octant * 16 + 8, :][:, :TERMS] + split_nt(local_mid, operator(octant))
        local_ref[octant * 8 : octant * 8 + 8, :] = widen(local)


def evaluate(local_ref, slope_ref, high_ref, low_ref, near_ref, live_ref, out_ref):
    local_leaf = local_ref[...]
    upper, lower = halves(local_leaf[:, :TERMS])
    slopes = jnp.dot(upper, slope_ref[...], preferred_element_type=F32) + jnp.dot(
        lower, slope_ref[...], preferred_element_type=F32
    )
    parts = [local_leaf] + [slopes[:, c * LANES : (c + 1) * LANES] for c in range(3)]
    split_parts = [halves(part[:, :KPAD]) for part in parts]
    row = lax.broadcasted_iota(jnp.int32, (16, LANES), 0)
    lane = lax.broadcasted_iota(jnp.int32, (16, LANES), 1)
    for parity in range(4):
        span = slice(parity * 16, parity * 16 + 16)
        coef_high = jnp.concatenate([part[0][span] for part in split_parts], axis=0)
        coef_low = jnp.concatenate([part[1][span] for part in split_parts], axis=0)
        coef = jnp.concatenate([coef_high, coef_low], axis=0)
        for group in range(4):
            x, y = (group >> 1) * 2 + (parity >> 1), (group & 1) * 2 + (parity & 1)
            tile = group * 4 + parity
            lanes = slice(tile * LANES, tile * LANES + LANES)
            both = jnp.dot(coef, high_ref[:, lanes], preferred_element_type=F32)
            value = both[:64] + both[64:] + jnp.dot(coef_high, low_ref[:, lanes], preferred_element_type=F32)
            hit = (row // 8 == lane // 32 % 2) & (row % 8 == group * 2 + lane // 64)
            sums = [
                jnp.sum(jnp.where(hit, value[16 * c : 16 * c + 16], 0.0), axis=0, keepdims=True) for c in range(4)
            ]
            live = live_ref[x, y : y + 1, :]
            for c in range(4):
                near = near_ref[c, x, y : y + 1, :]
                value = near + sums[c] if c == 0 else near - sums[c]
                out_ref[c, x, y : y + 1, :] = value * live


def whole_kernel(
    nx,
    ny,
    nz,
    pos_hbm,
    chg_hbm,
    cnt_hbm,
    up_hbm,
    down_hbm,
    slope_hbm,
    lattice_hbm,
    far_hbm,
    out_ref,
    pos_ref,
    chg_ref,
    cnt_ref,
    up_ref,
    down_ref,
    slope_ref,
    lattice_ref,
    data_ref,
    live_ref,
    ext_ref,
    wide_ref,
    mids_ref,
    tops_ref,
    leaf_ref,
    mid_ref,
    top_ref,
    up_rows,
    down_rows,
    downs_ref,
    high_ref,
    low_ref,
    turned_ref,
    table_ref,
    sums_ref,
    near_ref,
    whole_ref,
    aligned_ref,
    rows_ref,
    tiles_ref,
    upper_ref,
    coarse_ref,
    acc_ref,
    local_ref,
    pool_ref,
    line_ref,
    send,
    recv,
    load,
):
    ix, iy, iz = lax.axis_index("gx"), lax.axis_index("gy"), lax.axis_index("gz")

    def at(dx, dy, dz):
        return {
            "gx": lax.rem(ix + (dx + nx), nx),
            "gy": lax.rem(iy + (dy + ny), ny),
            "gz": lax.rem(iz + (dz + nz), nz),
        }

    plane = [(0, b, c) for b in range(ny) for c in range(nz) if b or c]
    line = [(a, 0, 0) for a in range(1, nx)]
    wrapped = lambda step: (step[0] % nx, step[1] % ny, step[2] % nz)
    partners = sorted({wrapped(step) for step in DIRECTIONS} | set(plane) | set(line))
    operands = ((pos_hbm, pos_ref), (chg_hbm, chg_ref), (cnt_hbm, cnt_ref), (up_hbm, up_ref))
    operands += ((down_hbm, down_ref), (slope_hbm, slope_ref), (lattice_hbm, lattice_ref))
    loads = [pltpu.make_async_copy(src, dst, load.at[k]) for k, (src, dst) in enumerate(operands)]
    pieces = []
    for k in range(PIECES):
        span = pl.ds(k * (25600 // PIECES), 25600 // PIECES)
        pieces.append(pltpu.make_async_copy(far_hbm.at[:, span], whole_ref.at[:, span], load.at[7 + k]))
    for copy in loads[:4]:
        copy.start()
    barrier = pltpu.get_barrier_semaphore()
    for step in partners:
        pl.semaphore_signal(barrier, inc=1, device_id=at(*step), device_id_type=MESH)
    for copy in pieces[:2] + loads[4:]:
        copy.start()
    octant_own = (ix % 2) * 4 + (iy % 2) * 2 + iz % 2
    for copy in loads[:4]:
        copy.wait()

    prepare(pos_ref, chg_ref, cnt_ref, data_ref, live_ref)
    octant_operators(up_ref, up_rows)
    monomial_tiles(rows_from(data_ref), high_ref, low_ref)

    pl.semaphore_wait(barrier, len(partners))

    def remote(src, dst, ssem, rsem, step):
        copy = pltpu.make_async_remote_copy(
            src_ref=src, dst_ref=dst, send_sem=ssem, recv_sem=rsem, device_id=at(*step), device_id_type=MESH
        )
        copy.start()
        return copy

    order = sorted(range(len(DIRECTIONS)), key=lambda i: sum(abs(d) for d in DIRECTIONS[i][:2]))
    for rank, index in enumerate(order):
        dx, dy, dz = DIRECTIONS[index]
        from_x, to_x = span_of(dx, 4, 1)
        from_y, to_y = span_of(dy, 4, 1)
        src, dst = data_ref.at[from_x, from_y], ext_ref.at[to_x, to_y, 1 - dz]
        remote(src, dst, send.at[0], recv.at[0 if rank < 2 else 1], DIRECTIONS[index])
    for copy in pieces[2:]:
        copy.start()
    moments(data_ref, up_rows, leaf_ref, mid_ref, top_ref, high_ref, low_ref)
    pltpu.make_async_copy(data_ref, ext_ref.at[pl.ds(1, 4), pl.ds(1, 4), 1], recv.at[0]).start()
    pltpu.make_async_copy(top_ref, tops_ref.at[ix, iy, iz], recv.at[2]).start()
    pltpu.make_async_copy(leaf_ref, wide_ref.at[pl.ds(1, 2), pl.ds(1, 2), pl.ds(1, 2)], recv.at[4]).start()
    pltpu.make_async_copy(mid_ref, mids_ref.at[13], recv.at[4]).start()
    for step in plane:
        remote(top_ref, tops_ref.at[ix, iy, iz], send.at[1], recv.at[2], step)
    for step in DIRECTIONS:
        spans = [span_of(d, 2, 1) for d in step]
        src = leaf_ref.at[spans[0][0], spans[1][0], spans[2][0]]
        dst = wide_ref.at[spans[0][1], spans[1][1], spans[2][1]]
        remote(src, dst, send.at[0], recv.at[4], step)
        slot = ((1 - step[0]) * 3 + (1 - step[1])) * 3 + (1 - step[2])
        remote(mid_ref, mids_ref.at[slot], send.at[0], recv.at[4], step)

    def drain(view, semaphore):
        pltpu.make_async_copy(view, view, semaphore).wait()

    clear_rows(rows_ref)
    done = 0
    for k in range(PIECES - 1):
        pieces[k].wait()
        ready = ((k + 1) * (25600 // PIECES) - 256) // (3 * TERMS)
        align_operators(done, ready, whole_ref, aligned_ref)
        done = ready
    drain(ext_ref.at[pl.ds(0, 4), pl.ds(0, 4), pl.ds(0, 3)], recv.at[0])
    inside = [(x, y) for x in range(1, 5) for y in range(1, 5)]
    fill_cells(inside, ext_ref, turned_ref, table_ref)
    near_inside((0, 1, 2, 3), data_ref, table_ref, sums_ref)
    drain(tops_ref.at[ix], recv.at[2])
    for step in line:
        remote(tops_ref.at[ix], tops_ref.at[ix], send.at[0], recv.at[3], step)
    pieces[-1].wait()
    align_operators(done, TRIPLES, whole_ref, aligned_ref)
    for copy in loads[4:]:
        copy.wait()
    octant_operators(down_ref, down_rows)
    down_operators(octant_own, down_rows, downs_ref)
    drain(ext_ref.at[pl.ds(0, 5), pl.ds(0, 4)], recv.at[1])
    fill_cells(
        [(x, y) for x in range(6) for y in range(6) if (x, y) not in inside], ext_ref, turned_ref, table_ref
    )
    near_outside(data_ref, table_ref, sums_ref)
    near_rows(sums_ref, data_ref, near_ref)
    drain(pool_ref.at[pl.ds(0, 728)], recv.at[4])
    gather_boxes(wide_ref, mids_ref, rows_ref)
    drain(tops_ref.at[pl.ds(0, 7)], recv.at[3])
    tops = (ix // 2, iy // 2, iz // 2)
    gather_upper(tops, tops_ref, rows_ref)
    operators = [octant_operator(up_rows, octant) for octant in range(8)]
    lattice_term = gather_top(tops, tops_ref, upper_ref, operators, lattice_ref, coarse_ref, rows_ref)
    convert_tiles(rows_ref, tiles_ref)
    extra = far_products(tiles_ref, aligned_ref, acc_ref)
    locals_down(octant_own, acc_ref, lattice_term + extra, downs_ref, local_ref)
    evaluate(local_ref, slope_ref, high_ref, low_ref, near_ref, live_ref, out_ref)
    drain(pool_ref, send.at[0])
    drain(line_ref, send.at[1])


VMEM = pl.BlockSpec(memory_space=pltpu.VMEM)


def shape(*dims):
    return jax.ShapeDtypeStruct(dims, F32)


def whole_call(sizes, *operands):
    dma = pltpu.SemaphoreType.DMA
    return pl.pallas_call(
        functools.partial(whole_kernel, *sizes),
        out_shape=shape(4, 4, 4, LANES),
        in_specs=[pl.BlockSpec(memory_space=pltpu.HBM)] * 8,
        out_specs=VMEM,
        scratch_shapes=[
            pltpu.VMEM((3, 4, 4, LANES), F32),
            pltpu.VMEM((4, 4, LANES), F32),
            pltpu.VMEM((4, 4, 4), jnp.int32),
            pltpu.VMEM((TERMS, 8, TERMS), BF16),
            pltpu.VMEM((TERMS, 8, TERMS), BF16),
            pltpu.VMEM((TERMS, 3 * LANES), BF16),
            pltpu.VMEM((TERMS, TERMS), BF16),
            pltpu.VMEM((4, 4, 4, LANES), F32),
            pltpu.VMEM((4, 4, LANES), F32),
            pltpu.VMEM((6, 6, 3, 4, LANES), F32),
            pltpu.VMEM((4, 4, 4, 8, LANES), F32),
            pltpu.VMEM((27, 8, LANES), F32),
            pltpu.VMEM((*sizes, 1, LANES), F32),
            pltpu.VMEM((2, 2, 2, 8, LANES), F32),
            pltpu.VMEM((8, LANES), F32),
            pltpu.VMEM((1, LANES), F32),
            pltpu.VMEM((TERMS * 8, LANES), F32),
            pltpu.VMEM((TERMS * 8, LANES), F32),
            pltpu.VMEM((9, KPAD, LANES), BF16),
            pltpu.VMEM((KPAD, 2048), BF16),
            pltpu.VMEM((KPAD, 2048), BF16),
            pltpu.VMEM((6, 6, 3, 4, LANES), F32),
            pltpu.VMEM((6, 6, 3, 4, SLOTS, LANES), F32),
            pltpu.VMEM((4, 4, 4, 8, LANES), F32),
            pltpu.VMEM((4, 4, 4, LANES), F32),
            pltpu.VMEM((TERMS, 25600), BF16),
            pltpu.VMEM((KPAD, TRIPLES * 256), BF16),
            pltpu.VMEM((218 * 16, LANES), F32),
            pltpu.VMEM((4, 218, 16, LANES), BF16),
            pltpu.VMEM((8, 32, LANES), F32),
            pltpu.VMEM((32, LANES), F32),
            pltpu.VMEM((LANES, LANES), F32),
            pltpu.VMEM((64, LANES), F32),
            pltpu.VMEM((1248, LANES), F32),
            pltpu.VMEM((31, 1, LANES), F32),
            dma((2,)),
            dma((5,)),
            dma((7 + PIECES,)),
        ],
        compiler_params=pltpu.CompilerParams(collective_id=0, has_side_effects=True),
        name="whole",
    )(*operands)


def part_kernel(both_ref, pot_ref, field_ref):
    pot_ref[...] = both_ref[0]
    field_ref[...] = both_ref[1:4]


def part_call(both):
    return pl.pallas_call(
        part_kernel,
        out_shape=(shape(4, 4, LANES), shape(3, 4, 4, LANES)),
        in_specs=[VMEM],
        out_specs=(VMEM,) * 2,
        name="part",
    )(both)


def solution(mesh):
    sizes = tuple(mesh.shape[axis] for axis in ("gx", "gy", "gz"))

    def per_device(
        positions, charges, counts, moment_shift, far_operators, local_shift, lattice_operator
    ):
        slope = jnp.asarray(slope_matrix()).astype(BF16)
        native_up = jnp.transpose(moment_shift, (1, 0, 2))
        native_down = jnp.transpose(local_shift, (1, 0, 2))
        both = whole_call(
            sizes,
            positions,
            charges,
            counts,
            native_up,
            native_down,
            slope,
            lattice_operator,
            far_operators,
        )
        return part_call(both)

    placed = (
        P(None, "gx", "gy", "gz"),
        P("gx", "gy", "gz"),
        P("gx", "gy", "gz"),
        P(),
        P(),
        P(),
        P(),
    )
    return jax.shard_map(
        per_device,
        mesh=mesh,
        in_specs=placed,
        out_specs=(P("gx", "gy", "gz"), P(None, "gx", "gy", "gz")),
        check_vma=False,
    )
```

```python
import functools

import jax
import jax.numpy as jnp
import numpy as np
from jax import lax
from jax.experimental import pallas as pl
from jax.experimental.pallas import tpu as pltpu
from jax.sharding import PartitionSpec as P

ORDER = 8
SLOTS = 32
SOFTENING = 0.0625
TERMS = 81
KPAD = 96
LANES = 128
OFFSETS = 316
CHUNK = 2
PIECES = 4
MESH = pl.DeviceIdType.MESH
F32 = jnp.float32
BF16 = jnp.bfloat16


def offset_table():
    listed = []
    for shift_x in range(-3, 4):
        for shift_y in range(-3, 4):
            for shift_z in range(-3, 4):
                if max(abs(shift_x), abs(shift_y), abs(shift_z)) >= 2:
                    listed.append((shift_x, shift_y, shift_z))
    return listed


def admitted(shift):
    listed = []
    for parity in range(8):
        place = [shift[axis] + (parity >> (2 - axis) & 1) for axis in range(3)]
        if all(-2 <= c <= 3 for c in place):
            listed.append((parity, tuple(place)))
    return listed


def tile_of(place):
    around = [(c + 2) // 2 for c in place]
    inner = [(c + 2) % 2 for c in place]
    return ((around[0] * 3 + around[1]) * 3 + around[2]) * 8 + inner[0] * 4 + inner[1] * 2 + inner[2]


TOP_ROWS = {0: 10, 7: 11, 3: 12, 4: 13, 1: 14, 6: 15}
EXTRA_TILES = {2: 216, 5: 217}
TRIPLES = 106


def top_parity(shift):
    if min(shift) > -3:
        return 0
    if max(shift) < 3:
        return 7
    fits = [parity for parity, _ in admitted(shift) if parity in TOP_ROWS]
    return fits[0] if fits else None


def exponent_list():
    listed = []
    for accumulated in range(ORDER + 1):
        for height in (0, 1):
            for power_x in range(accumulated - height + 1):
                listed.append((power_x, accumulated - height - power_x, height))
    return listed


def triple_groups():
    shifts = offset_table()
    groups = {}
    for triple in range(TRIPLES):
        members = shifts[3 * triple : 3 * triple + 3]
        parities = tuple(sorted({parity for shift in members for parity, _ in admitted(shift)}))
        extra = [EXTRA_TILES[admitted(shift)[0][0]] for shift in members if top_parity(shift) is None]
        groups.setdefault((parities, bool(extra)), []).append(triple)
    return sorted(groups.items(), key=lambda item: (-len(item[0][0]), item[0]))


def slope_matrix():
    listed = exponent_list()
    place = {e: i for i, e in enumerate(listed)}
    matrix = np.zeros((TERMS, 3 * LANES), np.float32)
    for row, (a, b, c) in enumerate(listed):
        if a > 0:
            matrix[row, place[(a - 1, b, c)]] = a
        if b > 0:
            matrix[row, LANES + place[(a, b - 1, c)]] = b
        if c > 0:
            matrix[row, 2 * LANES + place[(a, b, c - 1)]] = c
    return matrix


def lanes_nt(lhs, rhs):
    return lax.dot_general(lhs, rhs, (((1,), (1,)), ((), ())), preferred_element_type=F32)


def halves(value):
    upper = value.astype(BF16)
    return upper, (value - upper.astype(F32)).astype(BF16)


def split_nt(value, rhs):
    rows = value.shape[0]
    if rows % 8:
        value = jnp.concatenate([value, jnp.zeros((8 - rows, value.shape[1]), F32)], axis=0)
    size = value.shape[0]
    both = lanes_nt(jnp.concatenate(halves(value), axis=0), rhs)
    return (both[:size] + both[size:])[:rows]


def widen(value):
    return jnp.concatenate([value, jnp.zeros((value.shape[0], LANES - value.shape[1]), F32)], axis=1)


def power_of(base, exponents):
    square = base * base
    fourth = square * square
    eighth = fourth * fourth
    result = jnp.where((exponents & 1) != 0, base, 1.0)
    result = result * jnp.where((exponents & 2) != 0, square, 1.0)
    result = result * jnp.where((exponents & 4) != 0, fourth, 1.0)
    return jnp.where(exponents == 8, eighth, result)


def exponents():
    row = lax.broadcasted_iota(jnp.int32, (KPAD, LANES), 0)
    degree = jnp.zeros((KPAD, LANES), jnp.int32)
    for n in range(1, ORDER + 1):
        degree = degree + (row >= n * n).astype(jnp.int32)
    place = row - degree * degree
    height = (place > degree).astype(jnp.int32)
    power_x = place - height * (degree + 1)
    return power_x, degree - height - power_x, height, row < TERMS


def monomial_tiles(rows_of, high_ref, low_ref):
    power_x, power_y, power_z, valid = exponents()
    for tile in range(16):
        px, py, ox, oy = tile >> 3, tile >> 2 & 1, tile >> 1 & 1, tile & 1
        row_x, row_y, row_z = rows_of(2 * px + ox, 2 * py + oy)
        full = lambda row: jnp.broadcast_to(row - 0.5, (KPAD, LANES))
        value = power_of(full(row_x), power_x) * power_of(full(row_y), power_y)
        value = value * jnp.where(power_z != 0, full(row_z), 1.0)
        value = jnp.where(valid, value, 0.0)
        upper, lower = halves(value)
        high_ref[:, tile * LANES : (tile + 1) * LANES] = upper
        low_ref[:, tile * LANES : (tile + 1) * LANES] = lower


def octant_operators(native_ref, rows_ref):
    rows_ref[:, :TERMS] = native_ref[...].astype(F32).reshape(TERMS * 8, TERMS)


def octant_operator(rows_ref, octant):
    return rows_ref[pl.ds(octant, TERMS, stride=8), :][:, :TERMS].astype(BF16)


def prepare(pos_ref, chg_ref, cnt_ref, data_ref, live_ref):
    counts = jnp.concatenate([cnt_ref[x] for x in range(4)], axis=0).astype(F32).astype(BF16)
    spread = (
        lax.broadcasted_iota(jnp.int32, (4, LANES), 1) // SLOTS == lax.broadcasted_iota(jnp.int32, (4, LANES), 0)
    ).astype(F32).astype(BF16)
    limit = jnp.dot(counts, spread, preferred_element_type=F32)
    slot_of = (lax.broadcasted_iota(jnp.int32, (16, LANES), 1) % SLOTS).astype(F32)
    live = (slot_of < limit).astype(F32)
    for x in range(4):
        live_ref[x] = live[4 * x : 4 * x + 4]
        for y in range(4):
            for c in range(3):
                data_ref[x, y, c : c + 1, :] = pos_ref[c, x, y : y + 1, :]
            data_ref[x, y, 3:4, :] = chg_ref[x, y : y + 1, :] * live[4 * x + y : 4 * x + y + 1]


def rows_from(data_ref):
    return lambda x, y: tuple(data_ref[x, y, c : c + 1, :] for c in range(3))


def moments(data_ref, operator_rows, leaf_ref, mid_ref, top_ref, high_ref, low_ref):
    row = lax.broadcasted_iota(jnp.int32, (16, LANES), 0)
    lane = lax.broadcasted_iota(jnp.int32, (16, LANES), 1)
    for group in range(4):
        px, py = group >> 1, group & 1
        pieces = []
        for tile in range(4):
            ox, oy = tile >> 1, tile & 1
            hit = (row // 8 == lane // 64) & (row % 8 == ox * 4 + oy * 2 + lane // 32 % 2)
            weight = jnp.broadcast_to(data_ref[2 * px + ox, 2 * py + oy, 3:4, :], (16, LANES))
            pieces.append(jnp.where(hit, weight, 0.0))
        upper, lower = halves(jnp.concatenate(pieces, axis=1))
        span = slice(group * 512, group * 512 + 512)
        both = lanes_nt(jnp.concatenate([upper, lower], axis=0), high_ref[:, span])
        total = widen(both[:16] + both[16:] + lanes_nt(upper, low_ref[:, span]))
        leaf_ref[px, py, 0] = total[:8]
        leaf_ref[px, py, 1] = total[8:]
    mid = jnp.zeros((8, TERMS), F32)
    top = jnp.zeros((8, TERMS), F32)
    which = lax.broadcasted_iota(jnp.int32, (8, TERMS), 0)
    tiles = [leaf_ref[p >> 2, p >> 1 & 1, p & 1] for p in range(8)]
    operators = [octant_operator(operator_rows, octant) for octant in range(8)]
    for octant in range(8):
        rows = jnp.concatenate([tile[octant : octant + 1] for tile in tiles], axis=0)
        mid = mid + split_nt(rows[:, :TERMS], operators[octant])
    mid_ref[...] = widen(mid)
    for octant in range(8):
        top = top + jnp.where(which == octant, split_nt(mid, operators[octant]), 0.0)
    top_ref[...] = widen(jnp.sum(top, axis=0, keepdims=True))


DIRECTIONS = [
    (dx, dy, dz) for dx in (-1, 0, 1) for dy in (-1, 0, 1) for dz in (-1, 0, 1) if (dx, dy, dz) != (0, 0, 0)
]


def span_of(step, own, first):
    if step == 0:
        return pl.ds(0, own), pl.ds(first, own)
    if step > 0:
        return pl.ds(own - 1, 1), pl.ds(first - 1, 1)
    return pl.ds(0, 1), pl.ds(first + own, 1)


def turn_cells(cells, ext_ref, turned_ref):
    lane4 = lax.broadcasted_iota(jnp.int32, (4, LANES), 1)
    for x, y in cells:
        before, here, after = ext_ref[x, y, 0], ext_ref[x, y, 1], ext_ref[x, y, 2]
        turned_ref[x, y, 0] = pltpu.roll(jnp.where(lane4 >= 96, before, here), 32, 1)
        turned_ref[x, y, 1] = here
        turned_ref[x, y, 2] = pltpu.roll(jnp.where(lane4 < 32, after, here), 96, 1)


def fill_cells(cells, shifts, rows_of, table_ref):
    lane = lax.broadcasted_iota(jnp.int32, (8, LANES), 1)
    base = lane // SLOTS * SLOTS + lax.broadcasted_iota(jnp.int32, (8, LANES), 0)

    def one_group(group, carry):
        pick = base + group * 8
        start = pl.multiple_of(group * 8, 8)
        for x, y in cells:
            for ez in shifts:
                rows = rows_of(x, y, ez)
                for c in range(4):
                    row = jnp.broadcast_to(rows[c : c + 1, :], (8, LANES))
                    table_ref[x, y, ez, c, pl.ds(start, 8), :] = jnp.take_along_axis(row, pick, axis=1)
        return carry

    lax.fori_loop(0, 4, one_group, 0)


def load_wide(data_ref, x, y):
    mine = data_ref[x, y]
    return [jnp.broadcast_to(mine[c : c + 1], (8, LANES)) for c in range(3)]


def pair_sums(sums, here_x, here_y, here_z, x, y, table_ref):
    potential, field_x, field_y, field_z = sums
    for ez in range(3):
        for group in range(4):
            span = pl.ds(group * 8, 8)
            delta_x = here_x - table_ref[x, y, ez, 0, span, :]
            delta_y = here_y - table_ref[x, y, ez, 1, span, :]
            delta_z = here_z[ez] - table_ref[x, y, ez, 2, span, :]
            distance = delta_x * delta_x + delta_y * delta_y + (delta_z * delta_z + SOFTENING)
            inverse = lax.rsqrt(distance)
            weight = table_ref[x, y, ez, 3, span, :] * inverse
            cubic = weight * (inverse * inverse)
            potential = potential + weight
            field_x = field_x + cubic * delta_x
            field_y = field_y + cubic * delta_y
            field_z = field_z + cubic * delta_z
    return potential, field_x, field_y, field_z


def near_inside(rows, data_ref, table_ref, sums_ref):
    for y in rows:
        steps = [ey for ey in (-1, 0, 1) if 0 <= y + ey < 4]

        def along_x(x, carry):
            wide = load_wide(data_ref, x, y)
            here_z = [wide[2] - float(ez - 1) for ez in range(3)]

            def around(ex, sums):
                here_x = wide[0] - (ex - 1).astype(F32)
                for ey in steps:
                    sums = pair_sums(sums, here_x, wide[1] - float(ey), here_z, x + ex, y + ey + 1, table_ref)
                return sums

            zero = jnp.zeros((8, LANES), F32)
            low = 1 - jnp.minimum(x, 1)
            high = 2 + jnp.minimum(3 - x, 1)
            sums = lax.fori_loop(low, high, around, (zero, zero, zero, zero))
            for c in range(4):
                sums_ref[x, y, c] = sums[c]
            return carry

        lax.fori_loop(0, 4, along_x, 0)


def near_outside(data_ref, table_ref, sums_ref):
    for x, ex in ((0, -1), (3, 1)):

        def along_y(y, carry):
            wide = load_wide(data_ref, x, y)
            here_z = [wide[2] - float(ez - 1) for ez in range(3)]
            sums = tuple(sums_ref[x, y, c] for c in range(4))
            for ey in (-1, 0, 1):
                sums = pair_sums(
                    sums, wide[0] - float(ex), wide[1] - float(ey), here_z, x + ex + 1, y + ey + 1, table_ref
                )
            for c in range(4):
                sums_ref[x, y, c] = sums[c]
            return carry

        lax.fori_loop(0, 4, along_y, 0)
    for y, ey in ((0, -1), (3, 1)):
        for x in range(4):
            wide = load_wide(data_ref, x, y)
            here_z = [wide[2] - float(ez - 1) for ez in range(3)]
            sums = tuple(sums_ref[x, y, c] for c in range(4))
            for ex in (-1, 0, 1):
                if 0 <= x + ex < 4:
                    sums = pair_sums(
                        sums, wide[0] - float(ex), wide[1] - float(ey), here_z, x + ex + 1, y + ey + 1, table_ref
                    )
            for c in range(4):
                sums_ref[x, y, c] = sums[c]


def near_rows(sums_ref, data_ref, near_ref):
    self_weight = lax.rsqrt(jnp.full((1, LANES), SOFTENING, F32))
    for x in range(4):
        for y in range(4):
            near = [jnp.sum(sums_ref[x, y, c], axis=0, keepdims=True) for c in range(4)]
            near[0] = near[0] - data_ref[x, y, 3:4, :] * self_weight
            for c in range(4):
                near_ref[c, x, y : y + 1, :] = near[c]


def align_operators(first, last, whole_ref, aligned_ref):
    slots = {}
    for _, members in triple_groups():
        for triple in members:
            slots[triple] = len(slots)
    for triple in range(first, last):
        begin = triple * 3 * TERMS
        if begin + 256 <= whole_ref.shape[1]:
            piece = whole_ref[:, begin : begin + 256]
        else:
            tail = whole_ref[:, begin : OFFSETS * TERMS]
            piece = jnp.concatenate([tail, jnp.zeros((TERMS, 256 - tail.shape[1]), BF16)], axis=1)
        slot = slots[triple]
        aligned_ref[:TERMS, slot * 256 : (slot + 1) * 256] = piece


def clear_rows(rows_ref):
    def step(n, carry):
        for octant in range(8):
            rows_ref[pl.ds(pl.multiple_of(n * 128 + octant * 16 + 8, 8), 8), :] = jnp.zeros((8, LANES), F32)
        return carry

    lax.fori_loop(0, 27, step, 0)


def gather_boxes(wide_ref, mids_ref, rows_ref):
    for n in range(27):
        step_x, step_y, step_z = n // 9, n // 3 % 3, n % 3
        for parent in range(8):
            px, py, pz = parent >> 2, parent >> 1 & 1, parent & 1
            rows_ref[pl.ds(n * 128 + parent, 8, stride=16), :] = wide_ref[px + step_x, py + step_y, pz + step_z]
        rows_ref[pl.ds(n * 128 + 8, 8, stride=16), :] = mids_ref[n]


def gather_upper(tops, tops_ref, rows_ref):
    far_x = [lax.rem(tops[0] + step + 3, 4) * 2 for step in range(3)]
    far_y = [lax.rem(tops[1] + step + 1, 2) * 2 for step in range(3)]
    far_z = [lax.rem(tops[2] + step + 3, 4) * 2 for step in range(3)]
    for n in range(27):
        step_x, step_y, step_z = n // 9, n // 3 % 3, n % 3
        for octant in range(8):
            ox, oy, oz = octant >> 2, octant >> 1 & 1, octant & 1
            place = n * 128 + octant * 16 + 9
            rows_ref[place : place + 1, :] = tops_ref[far_x[step_x] + ox, far_y[step_y] + oy, far_z[step_z] + oz]


def convert_tiles(rows_ref, tiles_ref):
    lane = lax.broadcasted_iota(jnp.int32, (16, LANES), 1)
    zero = jnp.zeros((16, LANES), BF16)
    for tile in range(218):
        value = rows_ref[tile * 16 : tile * 16 + 16, :].astype(BF16)
        second = pltpu.roll(value, TERMS, 1)
        tiles_ref[0, tile] = value
        tiles_ref[1, tile] = jnp.where(lane >= TERMS, second, zero)
        tiles_ref[2, tile] = jnp.where(lane < TERMS, second, zero)
        tiles_ref[3, tile] = pltpu.roll(value, 2 * TERMS - LANES, 1)


def gather_top(tops, tops_ref, upper_ref, operators, lattice_ref, turned_ref, rows_ref):
    for octant in range(8):
        ox, oy, oz = octant >> 2, octant >> 1 & 1, octant & 1
        for box in range(32):
            bx, by, bz = box >> 3, box >> 2 & 1, box & 3
            upper_ref[octant, box : box + 1, :] = tops_ref[2 * bx + ox, 2 * by + oy, 2 * bz + oz]
    coarse = jnp.zeros((32, TERMS), F32)
    for octant in range(8):
        coarse = coarse + split_nt(upper_ref[octant][:, :TERMS], operators[octant])
    lattice_term = split_nt(jnp.sum(coarse, axis=0, keepdims=True), lattice_ref[...])
    row = lax.broadcasted_iota(jnp.int32, (32, 32), 0)
    column = lax.broadcasted_iota(jnp.int32, (32, 32), 1)
    wanted = (
        (row // 8 + tops[0]) % 4 * 8 + (row // 4 % 2 + tops[1]) % 2 * 4 + (row % 4 + tops[2]) % 4
    )
    turned_ref[...] = jnp.dot(
        (wanted == column).astype(F32).astype(BF16), widen(coarse).astype(BF16), preferred_element_type=F32
    )
    for shift in offset_table():
        parity = top_parity(shift)
        source = shift[0] % 4 * 8 + shift[1] % 2 * 4 + shift[2] % 4
        if parity is not None:
            place = [shift[axis] + (parity >> (2 - axis) & 1) for axis in range(3)]
            target = tile_of(place) * 16 + TOP_ROWS[parity]
            rows_ref[target : target + 1, :] = turned_ref[source : source + 1, :]
        else:
            target = EXTRA_TILES[admitted(shift)[0][0]] * 16
            which = lax.broadcasted_iota(jnp.int32, (16, LANES), 0)
            top = jnp.broadcast_to(turned_ref[source : source + 1, :], (16, LANES))
            rows_ref[target : target + 16, :] = jnp.where(which == 0, top, 0.0)
    return lattice_term


def far_products(tiles_ref, aligned_ref, acc_ref):
    total = [jnp.zeros((16, TERMS), F32) for _ in range(8)]
    extra = jnp.zeros((1, TERMS), F32)
    shifts = offset_table()
    empty = jnp.zeros((16, LANES), BF16)

    def lanes_of(sources):
        halves_of = ([], [])
        for position, tile in enumerate(sources):
            if tile is not None:
                for half, version in (((0, 0),), ((0, 1), (1, 2)), ((1, 3),))[position]:
                    halves_of[half].append(tiles_ref[version, tile])
        sides = [sum(side[1:], side[0]) if side else empty for side in halves_of]
        return jnp.concatenate(sides, axis=1)

    slot = 0
    for (parities, special), members in triple_groups():
        group = None
        for start in range(0, len(members), CHUNK):
            part = members[start : start + CHUNK]
            columns = []
            for triple in part:
                steps = shifts[3 * triple : 3 * triple + 3]
                places = [dict(admitted(step)) for step in steps]
                rows = [[tile_of(place[p]) if p in place else None for place in places] for p in parities]
                if special:
                    rows.append(
                        [EXTRA_TILES[admitted(step)[0][0]] if top_parity(step) is None else None for step in steps]
                    )
                columns.append(jnp.concatenate([lanes_of(sources) for sources in rows], axis=0))
            data = columns[0] if len(columns) == 1 else jnp.concatenate(columns, axis=1)
            product = lanes_nt(data, aligned_ref[:TERMS, slot * 256 : (slot + len(part)) * 256])
            slot += len(part)
            group = product if group is None else group + product
        for place, parity in enumerate(parities):
            total[parity] = total[parity] + group[place * 16 : place * 16 + 16]
        if special:
            extra = extra + group[len(parities) * 16 : len(parities) * 16 + 1]
    for parity in range(8):
        acc_ref[parity * 16 : parity * 16 + 16, :] = widen(total[parity])
    return extra


def down_operators(octant_own, down_rows, downs_ref):
    own = jnp.where(
        lax.broadcasted_iota(jnp.int32, (TERMS * 8, LANES), 0) % 8 == octant_own, down_rows[...], 0.0
    )
    downs_ref[8, :TERMS, :] = jnp.sum(own.reshape(TERMS, 8, LANES), axis=1).astype(BF16)
    for octant in range(8):
        downs_ref[octant, :TERMS, :TERMS] = octant_operator(down_rows, octant)


def locals_down(octant_own, acc_ref, lattice_term, downs_ref, local_ref):
    far_top = lattice_term
    for parity, place in TOP_ROWS.items():
        row = parity * 16 + place
        far_top = far_top + acc_ref[row : row + 1, :][:, :TERMS]
    operator = lambda octant: downs_ref[octant, :TERMS, :TERMS]
    local_upper = 0.25 * acc_ref[pl.ds(octant_own * 16 + 9, 1), :][:, :TERMS] + split_nt(
        0.125 * far_top, operator(8)
    )
    upper_wide = jnp.broadcast_to(local_upper, (8, TERMS))
    which = lax.broadcasted_iota(jnp.int32, (8, TERMS), 0)
    local_mid = 0.5 * acc_ref[pl.ds(8, 8, stride=16), :][:, :TERMS]
    for octant in range(8):
        local_mid = local_mid + jnp.where(which == octant, split_nt(upper_wide, operator(octant)), 0.0)
    for octant in range(8):
        local = acc_ref[octant * 16 : octant * 16 + 8, :][:, :TERMS] + split_nt(local_mid, operator(octant))
        local_ref[octant * 8 : octant * 8 + 8, :] = widen(local)


def evaluate(local_ref, slope_ref, high_ref, low_ref, near_ref, live_ref, out_ref):
    local_leaf = local_ref[...]
    upper, lower = halves(local_leaf[:, :TERMS])
    slopes = jnp.dot(upper, slope_ref[...], preferred_element_type=F32) + jnp.dot(
        lower, slope_ref[...], preferred_element_type=F32
    )
    parts = [local_leaf] + [slopes[:, c * LANES : (c + 1) * LANES] for c in range(3)]
    split_parts = [halves(part[:, :KPAD]) for part in parts]
    row = lax.broadcasted_iota(jnp.int32, (16, LANES), 0)
    lane = lax.broadcasted_iota(jnp.int32, (16, LANES), 1)
    for parity in range(4):
        span = slice(parity * 16, parity * 16 + 16)
        coef_high = jnp.concatenate([part[0][span] for part in split_parts], axis=0)
        coef_low = jnp.concatenate([part[1][span] for part in split_parts], axis=0)
        coef = jnp.concatenate([coef_high, coef_low], axis=0)
        for group in range(4):
            x, y = (group >> 1) * 2 + (parity >> 1), (group & 1) * 2 + (parity & 1)
            tile = group * 4 + parity
            lanes = slice(tile * LANES, tile * LANES + LANES)
            both = jnp.dot(coef, high_ref[:, lanes], preferred_element_type=F32)
            value = both[:64] + both[64:] + jnp.dot(coef_high, low_ref[:, lanes], preferred_element_type=F32)
            hit = (row // 8 == lane // 32 % 2) & (row % 8 == group * 2 + lane // 64)
            sums = [
                jnp.sum(jnp.where(hit, value[16 * c : 16 * c + 16], 0.0), axis=0, keepdims=True) for c in range(4)
            ]
            live = live_ref[x, y : y + 1, :]
            for c in range(4):
                near = near_ref[c, x, y : y + 1, :]
                value = near + sums[c] if c == 0 else near - sums[c]
                out_ref[c, x, y : y + 1, :] = value * live


def whole_kernel(
    nx,
    ny,
    nz,
    pos_hbm,
    chg_hbm,
    cnt_hbm,
    up_hbm,
    down_hbm,
    slope_hbm,
    lattice_hbm,
    far_hbm,
    out_ref,
    pos_ref,
    chg_ref,
    cnt_ref,
    up_ref,
    down_ref,
    slope_ref,
    lattice_ref,
    data_ref,
    live_ref,
    ext_ref,
    wide_ref,
    mids_ref,
    tops_ref,
    leaf_ref,
    mid_ref,
    top_ref,
    up_rows,
    down_rows,
    downs_ref,
    high_ref,
    low_ref,
    turned_ref,
    table_ref,
    sums_ref,
    near_ref,
    whole_ref,
    aligned_ref,
    rows_ref,
    tiles_ref,
    upper_ref,
    coarse_ref,
    acc_ref,
    local_ref,
    pool_ref,
    line_ref,
    send,
    recv,
    load,
):
    ix, iy, iz = lax.axis_index("gx"), lax.axis_index("gy"), lax.axis_index("gz")

    def at(dx, dy, dz):
        return {
            "gx": lax.rem(ix + (dx + nx), nx),
            "gy": lax.rem(iy + (dy + ny), ny),
            "gz": lax.rem(iz + (dz + nz), nz),
        }

    plane = [(0, b, c) for b in range(ny) for c in range(nz) if b or c]
    line = [(a, 0, 0) for a in range(1, nx)]
    wrapped = lambda step: (step[0] % nx, step[1] % ny, step[2] % nz)
    partners = sorted({wrapped(step) for step in DIRECTIONS} | set(plane) | set(line))
    operands = ((pos_hbm, pos_ref), (chg_hbm, chg_ref), (cnt_hbm, cnt_ref), (up_hbm, up_ref))
    operands += ((down_hbm, down_ref), (slope_hbm, slope_ref), (lattice_hbm, lattice_ref))
    loads = [pltpu.make_async_copy(src, dst, load.at[k]) for k, (src, dst) in enumerate(operands)]
    pieces = []
    for k in range(PIECES):
        span = pl.ds(k * (25600 // PIECES), 25600 // PIECES)
        pieces.append(pltpu.make_async_copy(far_hbm.at[:, span], whole_ref.at[:, span], load.at[7 + k]))
    for copy in loads[:4]:
        copy.start()
    barrier = pltpu.get_barrier_semaphore()
    for step in partners:
        pl.semaphore_signal(barrier, inc=1, device_id=at(*step), device_id_type=MESH)
    for copy in pieces + loads[4:]:
        copy.start()
    octant_own = (ix % 2) * 4 + (iy % 2) * 2 + iz % 2
    for copy in loads[:4]:
        copy.wait()

    prepare(pos_ref, chg_ref, cnt_ref, data_ref, live_ref)
    octant_operators(up_ref, up_rows)
    monomial_tiles(rows_from(data_ref), high_ref, low_ref)

    pl.semaphore_wait(barrier, len(partners))

    def remote(src, dst, ssem, rsem, step):
        copy = pltpu.make_async_remote_copy(
            src_ref=src, dst_ref=dst, send_sem=ssem, recv_sem=rsem, device_id=at(*step), device_id_type=MESH
        )
        copy.start()
        return copy

    order = sorted(range(len(DIRECTIONS)), key=lambda i: sum(abs(d) for d in DIRECTIONS[i][:2]))
    for rank, index in enumerate(order):
        dx, dy, dz = DIRECTIONS[index]
        from_x, to_x = span_of(dx, 4, 1)
        from_y, to_y = span_of(dy, 4, 1)
        src, dst = data_ref.at[from_x, from_y], ext_ref.at[to_x, to_y, 1 - dz]
        remote(src, dst, send.at[0], recv.at[0 if rank < 2 else 1], DIRECTIONS[index])
    moments(data_ref, up_rows, leaf_ref, mid_ref, top_ref, high_ref, low_ref)
    pltpu.make_async_copy(data_ref, ext_ref.at[pl.ds(1, 4), pl.ds(1, 4), 1], recv.at[0]).start()
    pltpu.make_async_copy(top_ref, tops_ref.at[ix, iy, iz], recv.at[2]).start()
    pltpu.make_async_copy(leaf_ref, wide_ref.at[pl.ds(1, 2), pl.ds(1, 2), pl.ds(1, 2)], recv.at[4]).start()
    pltpu.make_async_copy(mid_ref, mids_ref.at[13], recv.at[4]).start()
    for step in plane:
        remote(top_ref, tops_ref.at[ix, iy, iz], send.at[1], recv.at[2], step)
    for step in DIRECTIONS:
        spans = [span_of(d, 2, 1) for d in step]
        src = leaf_ref.at[spans[0][0], spans[1][0], spans[2][0]]
        dst = wide_ref.at[spans[0][1], spans[1][1], spans[2][1]]
        remote(src, dst, send.at[0], recv.at[4], step)
        slot = ((1 - step[0]) * 3 + (1 - step[1])) * 3 + (1 - step[2])
        remote(mid_ref, mids_ref.at[slot], send.at[0], recv.at[4], step)

    def drain(view, semaphore):
        pltpu.make_async_copy(view, view, semaphore).wait()

    clear_rows(rows_ref)
    done = 0
    inside = [(x, y) for x in range(1, 5) for y in range(1, 5)]
    fill_cells(inside, (1,), lambda x, y, ez: data_ref.at[x - 1, y - 1], table_ref)
    for copy in loads[4:]:
        copy.wait()
    octant_operators(down_ref, down_rows)
    down_operators(octant_own, down_rows, downs_ref)
    for k in range(PIECES):
        pieces[k].wait()
        ready = TRIPLES if k == PIECES - 1 else ((k + 1) * (25600 // PIECES) - 256) // (3 * TERMS)
        align_operators(done, ready, whole_ref, aligned_ref)
        done = ready
    drain(ext_ref.at[pl.ds(0, 4), pl.ds(0, 4), pl.ds(0, 3)], recv.at[0])
    turn_cells(inside, ext_ref, turned_ref)
    turned = lambda x, y, ez: turned_ref.at[x, y, ez]
    fill_cells(inside, (0, 2), turned, table_ref)
    near_inside((0, 1, 2, 3), data_ref, table_ref, sums_ref)
    drain(tops_ref.at[ix], recv.at[2])
    for step in line:
        remote(tops_ref.at[ix], tops_ref.at[ix], send.at[0], recv.at[3], step)
    drain(ext_ref.at[pl.ds(0, 5), pl.ds(0, 4)], recv.at[1])
    outside = [(x, y) for x in range(6) for y in range(6) if (x, y) not in inside]
    turn_cells(outside, ext_ref, turned_ref)
    fill_cells(outside, (0, 1, 2), turned, table_ref)
    near_outside(data_ref, table_ref, sums_ref)
    near_rows(sums_ref, data_ref, near_ref)
    drain(pool_ref.at[pl.ds(0, 728)], recv.at[4])
    gather_boxes(wide_ref, mids_ref, rows_ref)
    drain(tops_ref.at[pl.ds(0, 7)], recv.at[3])
    tops = (ix // 2, iy // 2, iz // 2)
    gather_upper(tops, tops_ref, rows_ref)
    operators = [octant_operator(up_rows, octant) for octant in range(8)]
    lattice_term = gather_top(tops, tops_ref, upper_ref, operators, lattice_ref, coarse_ref, rows_ref)
    convert_tiles(rows_ref, tiles_ref)
    extra = far_products(tiles_ref, aligned_ref, acc_ref)
    locals_down(octant_own, acc_ref, lattice_term + extra, downs_ref, local_ref)
    evaluate(local_ref, slope_ref, high_ref, low_ref, near_ref, live_ref, out_ref)
    drain(pool_ref, send.at[0])
    drain(line_ref, send.at[1])


VMEM = pl.BlockSpec(memory_space=pltpu.VMEM)


def shape(*dims):
    return jax.ShapeDtypeStruct(dims, F32)


def whole_call(sizes, *operands):
    dma = pltpu.SemaphoreType.DMA
    return pl.pallas_call(
        functools.partial(whole_kernel, *sizes),
        out_shape=shape(4, 4, 4, LANES),
        in_specs=[pl.BlockSpec(memory_space=pltpu.HBM)] * 8,
        out_specs=VMEM,
        scratch_shapes=[
            pltpu.VMEM((3, 4, 4, LANES), F32),
            pltpu.VMEM((4, 4, LANES), F32),
            pltpu.VMEM((4, 4, 4), jnp.int32),
            pltpu.VMEM((TERMS, 8, TERMS), BF16),
            pltpu.VMEM((TERMS, 8, TERMS), BF16),
            pltpu.VMEM((TERMS, 3 * LANES), BF16),
            pltpu.VMEM((TERMS, TERMS), BF16),
            pltpu.VMEM((4, 4, 4, LANES), F32),
            pltpu.VMEM((4, 4, LANES), F32),
            pltpu.VMEM((6, 6, 3, 4, LANES), F32),
            pltpu.VMEM((4, 4, 4, 8, LANES), F32),
            pltpu.VMEM((27, 8, LANES), F32),
            pltpu.VMEM((*sizes, 1, LANES), F32),
            pltpu.VMEM((2, 2, 2, 8, LANES), F32),
            pltpu.VMEM((8, LANES), F32),
            pltpu.VMEM((1, LANES), F32),
            pltpu.VMEM((TERMS * 8, LANES), F32),
            pltpu.VMEM((TERMS * 8, LANES), F32),
            pltpu.VMEM((9, KPAD, LANES), BF16),
            pltpu.VMEM((KPAD, 2048), BF16),
            pltpu.VMEM((KPAD, 2048), BF16),
            pltpu.VMEM((6, 6, 3, 4, LANES), F32),
            pltpu.VMEM((6, 6, 3, 4, SLOTS, LANES), F32),
            pltpu.VMEM((4, 4, 4, 8, LANES), F32),
            pltpu.VMEM((4, 4, 4, LANES), F32),
            pltpu.VMEM((TERMS, 25600), BF16),
            pltpu.VMEM((KPAD, TRIPLES * 256), BF16),
            pltpu.VMEM((218 * 16, LANES), F32),
            pltpu.VMEM((4, 218, 16, LANES), BF16),
            pltpu.VMEM((8, 32, LANES), F32),
            pltpu.VMEM((32, LANES), F32),
            pltpu.VMEM((LANES, LANES), F32),
            pltpu.VMEM((64, LANES), F32),
            pltpu.VMEM((1248, LANES), F32),
            pltpu.VMEM((31, 1, LANES), F32),
            dma((2,)),
            dma((5,)),
            dma((7 + PIECES,)),
        ],
        compiler_params=pltpu.CompilerParams(collective_id=0, has_side_effects=True),
        name="whole",
    )(*operands)


def part_kernel(both_ref, pot_ref, field_ref):
    pot_ref[...] = both_ref[0]
    field_ref[...] = both_ref[1:4]


def part_call(both):
    return pl.pallas_call(
        part_kernel,
        out_shape=(shape(4, 4, LANES), shape(3, 4, 4, LANES)),
        in_specs=[VMEM],
        out_specs=(VMEM,) * 2,
        name="part",
    )(both)


def solution(mesh):
    sizes = tuple(mesh.shape[axis] for axis in ("gx", "gy", "gz"))

    def per_device(
        positions, charges, counts, moment_shift, far_operators, local_shift, lattice_operator
    ):
        slope = jnp.asarray(slope_matrix()).astype(BF16)
        native_up = jnp.transpose(moment_shift, (1, 0, 2))
        native_down = jnp.transpose(local_shift, (1, 0, 2))
        both = whole_call(
            sizes,
            positions,
            charges,
            counts,
            native_up,
            native_down,
            slope,
            lattice_operator,
            far_operators,
        )
        return part_call(both)

    placed = (
        P(None, "gx", "gy", "gz"),
        P("gx", "gy", "gz"),
        P("gx", "gy", "gz"),
        P(),
        P(),
        P(),
        P(),
    )
    return jax.shard_map(
        per_device,
        mesh=mesh,
        in_specs=placed,
        out_specs=(P("gx", "gy", "gz"), P(None, "gx", "gy", "gz")),
        check_vma=False,
    )
```

```python
import functools

import jax
import jax.numpy as jnp
import numpy as np
from jax import lax
from jax.experimental import pallas as pl
from jax.experimental.pallas import tpu as pltpu
from jax.sharding import PartitionSpec as P

ORDER = 8
SLOTS = 32
SOFTENING = 0.0625
TERMS = 81
KPAD = 96
LANES = 128
OFFSETS = 316
CHUNK = 2
PIECES = 4
MESH = pl.DeviceIdType.MESH
F32 = jnp.float32
BF16 = jnp.bfloat16


def offset_table():
    listed = []
    for shift_x in range(-3, 4):
        for shift_y in range(-3, 4):
            for shift_z in range(-3, 4):
                if max(abs(shift_x), abs(shift_y), abs(shift_z)) >= 2:
                    listed.append((shift_x, shift_y, shift_z))
    return listed


def admitted(shift):
    listed = []
    for parity in range(8):
        place = [shift[axis] + (parity >> (2 - axis) & 1) for axis in range(3)]
        if all(-2 <= c <= 3 for c in place):
            listed.append((parity, tuple(place)))
    return listed


def tile_of(place):
    around = [(c + 2) // 2 for c in place]
    inner = [(c + 2) % 2 for c in place]
    return ((around[0] * 3 + around[1]) * 3 + around[2]) * 8 + inner[0] * 4 + inner[1] * 2 + inner[2]


TOP_ROWS = {0: 10, 7: 11, 3: 12, 4: 13, 1: 14, 6: 15}
EXTRA_TILES = {2: 216, 5: 217}
TRIPLES = 106


def top_parity(shift):
    if min(shift) > -3:
        return 0
    if max(shift) < 3:
        return 7
    fits = [parity for parity, _ in admitted(shift) if parity in TOP_ROWS]
    return fits[0] if fits else None


def exponent_list():
    listed = []
    for accumulated in range(ORDER + 1):
        for height in (0, 1):
            for power_x in range(accumulated - height + 1):
                listed.append((power_x, accumulated - height - power_x, height))
    return listed


def triple_groups():
    shifts = offset_table()
    groups = {}
    for triple in range(TRIPLES):
        members = shifts[3 * triple : 3 * triple + 3]
        parities = tuple(sorted({parity for shift in members for parity, _ in admitted(shift)}))
        extra = [EXTRA_TILES[admitted(shift)[0][0]] for shift in members if top_parity(shift) is None]
        groups.setdefault((parities, bool(extra)), []).append(triple)
    return sorted(groups.items(), key=lambda item: (-len(item[0][0]), item[0]))


def slope_matrix():
    listed = exponent_list()
    place = {e: i for i, e in enumerate(listed)}
    matrix = np.zeros((TERMS, 3 * LANES), np.float32)
    for row, (a, b, c) in enumerate(listed):
        if a > 0:
            matrix[row, place[(a - 1, b, c)]] = a
        if b > 0:
            matrix[row, LANES + place[(a, b - 1, c)]] = b
        if c > 0:
            matrix[row, 2 * LANES + place[(a, b, c - 1)]] = c
    return matrix


def lanes_nt(lhs, rhs):
    return lax.dot_general(lhs, rhs, (((1,), (1,)), ((), ())), preferred_element_type=F32)


def halves(value):
    upper = value.astype(BF16)
    return upper, (value - upper.astype(F32)).astype(BF16)


def split_nt(value, rhs):
    rows = value.shape[0]
    if rows % 8:
        value = jnp.concatenate([value, jnp.zeros((8 - rows, value.shape[1]), F32)], axis=0)
    size = value.shape[0]
    both = lanes_nt(jnp.concatenate(halves(value), axis=0), rhs)
    return (both[:size] + both[size:])[:rows]


def widen(value):
    return jnp.concatenate([value, jnp.zeros((value.shape[0], LANES - value.shape[1]), F32)], axis=1)


def power_of(base, exponents):
    square = base * base
    fourth = square * square
    eighth = fourth * fourth
    result = jnp.where((exponents & 1) != 0, base, 1.0)
    result = result * jnp.where((exponents & 2) != 0, square, 1.0)
    result = result * jnp.where((exponents & 4) != 0, fourth, 1.0)
    return jnp.where(exponents == 8, eighth, result)


def exponents():
    row = lax.broadcasted_iota(jnp.int32, (KPAD, LANES), 0)
    degree = jnp.zeros((KPAD, LANES), jnp.int32)
    for n in range(1, ORDER + 1):
        degree = degree + (row >= n * n).astype(jnp.int32)
    place = row - degree * degree
    height = (place > degree).astype(jnp.int32)
    power_x = place - height * (degree + 1)
    return power_x, degree - height - power_x, height, row < TERMS


def monomial_tiles(rows_of, high_ref, low_ref):
    power_x, power_y, power_z, valid = exponents()
    for tile in range(16):
        px, py, ox, oy = tile >> 3, tile >> 2 & 1, tile >> 1 & 1, tile & 1
        row_x, row_y, row_z = rows_of(2 * px + ox, 2 * py + oy)
        full = lambda row: jnp.broadcast_to(row - 0.5, (KPAD, LANES))
        value = power_of(full(row_x), power_x) * power_of(full(row_y), power_y)
        value = value * jnp.where(power_z != 0, full(row_z), 1.0)
        value = jnp.where(valid, value, 0.0)
        upper, lower = halves(value)
        high_ref[:, tile * LANES : (tile + 1) * LANES] = upper
        low_ref[:, tile * LANES : (tile + 1) * LANES] = lower


def octant_operators(native_ref, rows_ref):
    rows_ref[:, :TERMS] = native_ref[...].astype(F32).reshape(TERMS * 8, TERMS)


def octant_operator(rows_ref, octant):
    return rows_ref[pl.ds(octant, TERMS, stride=8), :][:, :TERMS].astype(BF16)


def prepare(pos_ref, chg_ref, cnt_ref, data_ref, live_ref):
    counts = jnp.concatenate([cnt_ref[x] for x in range(4)], axis=0).astype(F32).astype(BF16)
    spread = (
        lax.broadcasted_iota(jnp.int32, (4, LANES), 1) // SLOTS == lax.broadcasted_iota(jnp.int32, (4, LANES), 0)
    ).astype(F32).astype(BF16)
    limit = jnp.dot(counts, spread, preferred_element_type=F32)
    slot_of = (lax.broadcasted_iota(jnp.int32, (16, LANES), 1) % SLOTS).astype(F32)
    live = (slot_of < limit).astype(F32)
    for x in range(4):
        live_ref[x] = live[4 * x : 4 * x + 4]
        for y in range(4):
            for c in range(3):
                data_ref[x, y, c : c + 1, :] = pos_ref[c, x, y : y + 1, :]
            data_ref[x, y, 3:4, :] = chg_ref[x, y : y + 1, :] * live[4 * x + y : 4 * x + y + 1]


def rows_from(data_ref):
    return lambda x, y: tuple(data_ref[x, y, c : c + 1, :] for c in range(3))


def moments(data_ref, operator_rows, leaf_ref, mid_ref, top_ref, high_ref, low_ref):
    row = lax.broadcasted_iota(jnp.int32, (16, LANES), 0)
    lane = lax.broadcasted_iota(jnp.int32, (16, LANES), 1)
    for group in range(4):
        px, py = group >> 1, group & 1
        pieces = []
        for tile in range(4):
            ox, oy = tile >> 1, tile & 1
            hit = (row // 8 == lane // 64) & (row % 8 == ox * 4 + oy * 2 + lane // 32 % 2)
            weight = jnp.broadcast_to(data_ref[2 * px + ox, 2 * py + oy, 3:4, :], (16, LANES))
            pieces.append(jnp.where(hit, weight, 0.0))
        upper, lower = halves(jnp.concatenate(pieces, axis=1))
        span = slice(group * 512, group * 512 + 512)
        both = lanes_nt(jnp.concatenate([upper, lower], axis=0), high_ref[:, span])
        total = widen(both[:16] + both[16:] + lanes_nt(upper, low_ref[:, span]))
        leaf_ref[px, py, 0] = total[:8]
        leaf_ref[px, py, 1] = total[8:]
    mid = jnp.zeros((8, TERMS), F32)
    top = jnp.zeros((8, TERMS), F32)
    which = lax.broadcasted_iota(jnp.int32, (8, TERMS), 0)
    tiles = [leaf_ref[p >> 2, p >> 1 & 1, p & 1] for p in range(8)]
    operators = [octant_operator(operator_rows, octant) for octant in range(8)]
    for octant in range(8):
        rows = jnp.concatenate([tile[octant : octant + 1] for tile in tiles], axis=0)
        mid = mid + split_nt(rows[:, :TERMS], operators[octant])
    mid_ref[...] = widen(mid)
    for octant in range(8):
        top = top + jnp.where(which == octant, split_nt(mid, operators[octant]), 0.0)
    top_ref[...] = widen(jnp.sum(top, axis=0, keepdims=True))


DIRECTIONS = [
    (dx, dy, dz) for dx in (-1, 0, 1) for dy in (-1, 0, 1) for dz in (-1, 0, 1) if (dx, dy, dz) != (0, 0, 0)
]


def span_of(step, own, first):
    if step == 0:
        return pl.ds(0, own), pl.ds(first, own)
    if step > 0:
        return pl.ds(own - 1, 1), pl.ds(first - 1, 1)
    return pl.ds(0, 1), pl.ds(first + own, 1)


def turn_cells(cells, ext_ref, turned_ref):
    lane4 = lax.broadcasted_iota(jnp.int32, (4, LANES), 1)
    for x, y in cells:
        before, here, after = ext_ref[x, y, 0], ext_ref[x, y, 1], ext_ref[x, y, 2]
        turned_ref[x, y, 0] = pltpu.roll(jnp.where(lane4 >= 96, before, here), 32, 1)
        turned_ref[x, y, 1] = here
        turned_ref[x, y, 2] = pltpu.roll(jnp.where(lane4 < 32, after, here), 96, 1)


def fill_cells(cells, shifts, rows_of, table_ref):
    lane = lax.broadcasted_iota(jnp.int32, (8, LANES), 1)
    base = lane // SLOTS * SLOTS + lax.broadcasted_iota(jnp.int32, (8, LANES), 0)

    def one_group(group, carry):
        pick = base + group * 8
        start = pl.multiple_of(group * 8, 8)
        for x, y in cells:
            for ez in shifts:
                rows = rows_of(x, y, ez)
                for c in range(4):
                    row = jnp.broadcast_to(rows[c : c + 1, :], (8, LANES))
                    table_ref[x, y, ez, c, pl.ds(start, 8), :] = jnp.take_along_axis(row, pick, axis=1)
        return carry

    lax.fori_loop(0, 4, one_group, 0)


def load_wide(data_ref, x, y):
    mine = data_ref[x, y]
    return [jnp.broadcast_to(mine[c : c + 1], (8, LANES)) for c in range(3)]


def pair_sums(sums, here_x, here_y, here_z, x, y, table_ref):
    potential, field_x, field_y, field_z = sums
    for ez in range(3):
        for group in range(4):
            span = pl.ds(group * 8, 8)
            delta_x = here_x - table_ref[x, y, ez, 0, span, :]
            delta_y = here_y - table_ref[x, y, ez, 1, span, :]
            delta_z = here_z[ez] - table_ref[x, y, ez, 2, span, :]
            distance = delta_x * delta_x + delta_y * delta_y + (delta_z * delta_z + SOFTENING)
            inverse = lax.rsqrt(distance)
            weight = table_ref[x, y, ez, 3, span, :] * inverse
            cubic = weight * (inverse * inverse)
            potential = potential + weight
            field_x = field_x + cubic * delta_x
            field_y = field_y + cubic * delta_y
            field_z = field_z + cubic * delta_z
    return potential, field_x, field_y, field_z


def near_inside(rows, data_ref, table_ref, sums_ref):
    for y in rows:
        steps = [ey for ey in (-1, 0, 1) if 0 <= y + ey < 4]

        def along_x(x, carry):
            wide = load_wide(data_ref, x, y)
            here_z = [wide[2] - float(ez - 1) for ez in range(3)]

            def around(ex, sums):
                here_x = wide[0] - (ex - 1).astype(F32)
                for ey in steps:
                    sums = pair_sums(sums, here_x, wide[1] - float(ey), here_z, x + ex, y + ey + 1, table_ref)
                return sums

            zero = jnp.zeros((8, LANES), F32)
            low = 1 - jnp.minimum(x, 1)
            high = 2 + jnp.minimum(3 - x, 1)
            sums = lax.fori_loop(low, high, around, (zero, zero, zero, zero))
            for c in range(4):
                sums_ref[x, y, c] = sums[c]
            return carry

        lax.fori_loop(0, 4, along_x, 0)


def near_outside(data_ref, table_ref, sums_ref):
    for x, ex in ((0, -1), (3, 1)):

        def along_y(y, carry):
            wide = load_wide(data_ref, x, y)
            here_z = [wide[2] - float(ez - 1) for ez in range(3)]
            sums = tuple(sums_ref[x, y, c] for c in range(4))
            for ey in (-1, 0, 1):
                sums = pair_sums(
                    sums, wide[0] - float(ex), wide[1] - float(ey), here_z, x + ex + 1, y + ey + 1, table_ref
                )
            for c in range(4):
                sums_ref[x, y, c] = sums[c]
            return carry

        lax.fori_loop(0, 4, along_y, 0)
    for y, ey in ((0, -1), (3, 1)):
        for x in range(4):
            wide = load_wide(data_ref, x, y)
            here_z = [wide[2] - float(ez - 1) for ez in range(3)]
            sums = tuple(sums_ref[x, y, c] for c in range(4))
            for ex in (-1, 0, 1):
                if 0 <= x + ex < 4:
                    sums = pair_sums(
                        sums, wide[0] - float(ex), wide[1] - float(ey), here_z, x + ex + 1, y + ey + 1, table_ref
                    )
            for c in range(4):
                sums_ref[x, y, c] = sums[c]


def near_rows(sums_ref, data_ref, near_ref):
    self_weight = lax.rsqrt(jnp.full((1, LANES), SOFTENING, F32))
    for x in range(4):
        for y in range(4):
            near = [jnp.sum(sums_ref[x, y, c], axis=0, keepdims=True) for c in range(4)]
            near[0] = near[0] - data_ref[x, y, 3:4, :] * self_weight
            for c in range(4):
                near_ref[c, x, y : y + 1, :] = near[c]


def align_operators(first, last, whole_ref, aligned_ref):
    slots = {}
    for _, members in triple_groups():
        for triple in members:
            slots[triple] = len(slots)
    for triple in range(first, last):
        begin = triple * 3 * TERMS
        if begin + 256 <= whole_ref.shape[1]:
            piece = whole_ref[:, begin : begin + 256]
        else:
            tail = whole_ref[:, begin : OFFSETS * TERMS]
            piece = jnp.concatenate([tail, jnp.zeros((TERMS, 256 - tail.shape[1]), BF16)], axis=1)
        slot = slots[triple]
        aligned_ref[:TERMS, slot * 256 : (slot + 1) * 256] = piece


def clear_rows(rows_ref):
    def step(n, carry):
        for octant in range(8):
            rows_ref[pl.ds(pl.multiple_of(n * 128 + octant * 16 + 8, 8), 8), :] = jnp.zeros((8, LANES), F32)
        return carry

    lax.fori_loop(0, 27, step, 0)


def gather_boxes(wide_ref, mids_ref, rows_ref):
    for n in range(27):
        step_x, step_y, step_z = n // 9, n // 3 % 3, n % 3
        for parent in range(8):
            px, py, pz = parent >> 2, parent >> 1 & 1, parent & 1
            rows_ref[pl.ds(n * 128 + parent, 8, stride=16), :] = wide_ref[px + step_x, py + step_y, pz + step_z]
        rows_ref[pl.ds(n * 128 + 8, 8, stride=16), :] = mids_ref[n]


def gather_upper(tops, tops_ref, rows_ref):
    far_x = [lax.rem(tops[0] + step + 3, 4) * 2 for step in range(3)]
    far_y = [lax.rem(tops[1] + step + 1, 2) * 2 for step in range(3)]
    far_z = [lax.rem(tops[2] + step + 3, 4) * 2 for step in range(3)]
    for n in range(27):
        step_x, step_y, step_z = n // 9, n // 3 % 3, n % 3
        for octant in range(8):
            ox, oy, oz = octant >> 2, octant >> 1 & 1, octant & 1
            place = n * 128 + octant * 16 + 9
            rows_ref[place : place + 1, :] = tops_ref[far_x[step_x] + ox, far_y[step_y] + oy, far_z[step_z] + oz]


def convert_tiles(rows_ref, tiles_ref):
    lane = lax.broadcasted_iota(jnp.int32, (16, LANES), 1)
    zero = jnp.zeros((16, LANES), BF16)
    for tile in range(218):
        value = rows_ref[tile * 16 : tile * 16 + 16, :].astype(BF16)
        second = pltpu.roll(value, TERMS, 1)
        tiles_ref[0, tile] = value
        tiles_ref[1, tile] = jnp.where(lane >= TERMS, second, zero)
        tiles_ref[2, tile] = jnp.where(lane < TERMS, second, zero)
        tiles_ref[3, tile] = pltpu.roll(value, 2 * TERMS - LANES, 1)


def gather_top(tops, tops_ref, upper_ref, operators, lattice_ref, turned_ref, rows_ref):
    for octant in range(8):
        ox, oy, oz = octant >> 2, octant >> 1 & 1, octant & 1
        for box in range(32):
            bx, by, bz = box >> 3, box >> 2 & 1, box & 3
            upper_ref[octant, box : box + 1, :] = tops_ref[2 * bx + ox, 2 * by + oy, 2 * bz + oz]
    coarse = jnp.zeros((32, TERMS), F32)
    for octant in range(8):
        coarse = coarse + split_nt(upper_ref[octant][:, :TERMS], operators[octant])
    lattice_term = split_nt(jnp.sum(coarse, axis=0, keepdims=True), lattice_ref[...])
    row = lax.broadcasted_iota(jnp.int32, (32, 32), 0)
    column = lax.broadcasted_iota(jnp.int32, (32, 32), 1)
    wanted = (
        (row // 8 + tops[0]) % 4 * 8 + (row // 4 % 2 + tops[1]) % 2 * 4 + (row % 4 + tops[2]) % 4
    )
    turned_ref[...] = jnp.dot(
        (wanted == column).astype(F32).astype(BF16), widen(coarse).astype(BF16), preferred_element_type=F32
    )
    for shift in offset_table():
        parity = top_parity(shift)
        source = shift[0] % 4 * 8 + shift[1] % 2 * 4 + shift[2] % 4
        if parity is not None:
            place = [shift[axis] + (parity >> (2 - axis) & 1) for axis in range(3)]
            target = tile_of(place) * 16 + TOP_ROWS[parity]
            rows_ref[target : target + 1, :] = turned_ref[source : source + 1, :]
        else:
            target = EXTRA_TILES[admitted(shift)[0][0]] * 16
            which = lax.broadcasted_iota(jnp.int32, (16, LANES), 0)
            top = jnp.broadcast_to(turned_ref[source : source + 1, :], (16, LANES))
            rows_ref[target : target + 16, :] = jnp.where(which == 0, top, 0.0)
    return lattice_term


def far_products(tiles_ref, aligned_ref, acc_ref):
    total = [jnp.zeros((16, TERMS), F32) for _ in range(8)]
    extra = jnp.zeros((1, TERMS), F32)
    shifts = offset_table()
    empty = jnp.zeros((16, LANES), BF16)

    def lanes_of(sources):
        halves_of = ([], [])
        for position, tile in enumerate(sources):
            if tile is not None:
                for half, version in (((0, 0),), ((0, 1), (1, 2)), ((1, 3),))[position]:
                    halves_of[half].append(tiles_ref[version, tile])
        sides = [sum(side[1:], side[0]) if side else empty for side in halves_of]
        return jnp.concatenate(sides, axis=1)

    slot = 0
    for (parities, special), members in triple_groups():
        group = None
        for start in range(0, len(members), CHUNK):
            part = members[start : start + CHUNK]
            columns = []
            for triple in part:
                steps = shifts[3 * triple : 3 * triple + 3]
                places = [dict(admitted(step)) for step in steps]
                rows = [[tile_of(place[p]) if p in place else None for place in places] for p in parities]
                if special:
                    rows.append(
                        [EXTRA_TILES[admitted(step)[0][0]] if top_parity(step) is None else None for step in steps]
                    )
                columns.append(jnp.concatenate([lanes_of(sources) for sources in rows], axis=0))
            data = columns[0] if len(columns) == 1 else jnp.concatenate(columns, axis=1)
            product = lanes_nt(data, aligned_ref[:TERMS, slot * 256 : (slot + len(part)) * 256])
            slot += len(part)
            group = product if group is None else group + product
        for place, parity in enumerate(parities):
            total[parity] = total[parity] + group[place * 16 : place * 16 + 16]
        if special:
            extra = extra + group[len(parities) * 16 : len(parities) * 16 + 1]
    for parity in range(8):
        acc_ref[parity * 16 : parity * 16 + 16, :] = widen(total[parity])
    return extra


def down_operators(octant_own, down_rows, downs_ref):
    own = jnp.where(
        lax.broadcasted_iota(jnp.int32, (TERMS * 8, LANES), 0) % 8 == octant_own, down_rows[...], 0.0
    )
    downs_ref[8, :TERMS, :] = jnp.sum(own.reshape(TERMS, 8, LANES), axis=1).astype(BF16)
    for octant in range(8):
        downs_ref[octant, :TERMS, :TERMS] = octant_operator(down_rows, octant)


def locals_down(octant_own, acc_ref, lattice_term, downs_ref, local_ref):
    far_top = lattice_term
    for parity, place in TOP_ROWS.items():
        row = parity * 16 + place
        far_top = far_top + acc_ref[row : row + 1, :][:, :TERMS]
    operator = lambda octant: downs_ref[octant, :TERMS, :TERMS]
    local_upper = 0.25 * acc_ref[pl.ds(octant_own * 16 + 9, 1), :][:, :TERMS] + split_nt(
        0.125 * far_top, operator(8)
    )
    upper_wide = jnp.broadcast_to(local_upper, (8, TERMS))
    which = lax.broadcasted_iota(jnp.int32, (8, TERMS), 0)
    local_mid = 0.5 * acc_ref[pl.ds(8, 8, stride=16), :][:, :TERMS]
    for octant in range(8):
        local_mid = local_mid + jnp.where(which == octant, split_nt(upper_wide, operator(octant)), 0.0)
    for octant in range(8):
        local = acc_ref[octant * 16 : octant * 16 + 8, :][:, :TERMS] + split_nt(local_mid, operator(octant))
        local_ref[octant * 8 : octant * 8 + 8, :] = widen(local)


def evaluate(local_ref, slope_ref, high_ref, low_ref, near_ref, live_ref, out_ref):
    local_leaf = local_ref[...]
    upper, lower = halves(local_leaf[:, :TERMS])
    slopes = jnp.dot(upper, slope_ref[...], preferred_element_type=F32) + jnp.dot(
        lower, slope_ref[...], preferred_element_type=F32
    )
    parts = [local_leaf] + [slopes[:, c * LANES : (c + 1) * LANES] for c in range(3)]
    split_parts = [halves(part[:, :KPAD]) for part in parts]
    row = lax.broadcasted_iota(jnp.int32, (16, LANES), 0)
    lane = lax.broadcasted_iota(jnp.int32, (16, LANES), 1)
    for parity in range(4):
        span = slice(parity * 16, parity * 16 + 16)
        coef_high = jnp.concatenate([part[0][span] for part in split_parts], axis=0)
        coef_low = jnp.concatenate([part[1][span] for part in split_parts], axis=0)
        coef = jnp.concatenate([coef_high, coef_low], axis=0)
        for group in range(4):
            x, y = (group >> 1) * 2 + (parity >> 1), (group & 1) * 2 + (parity & 1)
            tile = group * 4 + parity
            lanes = slice(tile * LANES, tile * LANES + LANES)
            both = jnp.dot(coef, high_ref[:, lanes], preferred_element_type=F32)
            value = both[:64] + both[64:] + jnp.dot(coef_high, low_ref[:, lanes], preferred_element_type=F32)
            hit = (row // 8 == lane // 32 % 2) & (row % 8 == group * 2 + lane // 64)
            sums = [
                jnp.sum(jnp.where(hit, value[16 * c : 16 * c + 16], 0.0), axis=0, keepdims=True) for c in range(4)
            ]
            live = live_ref[x, y : y + 1, :]
            for c in range(4):
                near = near_ref[c, x, y : y + 1, :]
                value = near + sums[c] if c == 0 else near - sums[c]
                out_ref[c, x, y : y + 1, :] = value * live


def whole_kernel(
    nx,
    ny,
    nz,
    pos_hbm,
    chg_hbm,
    cnt_hbm,
    up_hbm,
    down_hbm,
    slope_hbm,
    lattice_hbm,
    far_hbm,
    out_ref,
    pos_ref,
    chg_ref,
    cnt_ref,
    up_ref,
    down_ref,
    slope_ref,
    lattice_ref,
    data_ref,
    live_ref,
    ext_ref,
    wide_ref,
    mids_ref,
    tops_ref,
    leaf_ref,
    mid_ref,
    top_ref,
    up_rows,
    down_rows,
    downs_ref,
    high_ref,
    low_ref,
    turned_ref,
    table_ref,
    sums_ref,
    near_ref,
    whole_ref,
    aligned_ref,
    rows_ref,
    tiles_ref,
    upper_ref,
    coarse_ref,
    acc_ref,
    local_ref,
    pool_ref,
    line_ref,
    send,
    recv,
    load,
):
    ix, iy, iz = lax.axis_index("gx"), lax.axis_index("gy"), lax.axis_index("gz")

    def at(dx, dy, dz):
        return {
            "gx": lax.rem(ix + (dx + nx), nx),
            "gy": lax.rem(iy + (dy + ny), ny),
            "gz": lax.rem(iz + (dz + nz), nz),
        }

    plane = [(0, b, c) for b in range(ny) for c in range(nz) if b or c]
    line = [(a, 0, 0) for a in range(1, nx)]
    wrapped = lambda step: (step[0] % nx, step[1] % ny, step[2] % nz)
    partners = sorted({wrapped(step) for step in DIRECTIONS} | set(plane) | set(line))
    operands = ((pos_hbm, pos_ref), (chg_hbm, chg_ref), (cnt_hbm, cnt_ref), (up_hbm, up_ref))
    operands += ((down_hbm, down_ref), (slope_hbm, slope_ref), (lattice_hbm, lattice_ref))
    loads = [pltpu.make_async_copy(src, dst, load.at[k]) for k, (src, dst) in enumerate(operands)]
    pieces = []
    for k in range(PIECES):
        span = pl.ds(k * (25600 // PIECES), 25600 // PIECES)
        pieces.append(pltpu.make_async_copy(far_hbm.at[:, span], whole_ref.at[:, span], load.at[7 + k]))
    for copy in loads[:4]:
        copy.start()
    barrier = pltpu.get_barrier_semaphore()
    for step in partners:
        pl.semaphore_signal(barrier, inc=1, device_id=at(*step), device_id_type=MESH)
    for copy in pieces[:2] + loads[4:]:
        copy.start()
    octant_own = (ix % 2) * 4 + (iy % 2) * 2 + iz % 2
    for copy in loads[:4]:
        copy.wait()

    prepare(pos_ref, chg_ref, cnt_ref, data_ref, live_ref)
    octant_operators(up_ref, up_rows)
    monomial_tiles(rows_from(data_ref), high_ref, low_ref)

    pl.semaphore_wait(barrier, len(partners))

    def remote(src, dst, ssem, rsem, step):
        copy = pltpu.make_async_remote_copy(
            src_ref=src, dst_ref=dst, send_sem=ssem, recv_sem=rsem, device_id=at(*step), device_id_type=MESH
        )
        copy.start()
        return copy

    order = sorted(range(len(DIRECTIONS)), key=lambda i: sum(abs(d) for d in DIRECTIONS[i][:2]))
    for rank, index in enumerate(order):
        dx, dy, dz = DIRECTIONS[index]
        from_x, to_x = span_of(dx, 4, 1)
        from_y, to_y = span_of(dy, 4, 1)
        src, dst = data_ref.at[from_x, from_y], ext_ref.at[to_x, to_y, 1 - dz]
        remote(src, dst, send.at[0], recv.at[0 if rank < 2 else 1], DIRECTIONS[index])
    for copy in pieces[2:]:
        copy.start()
    moments(data_ref, up_rows, leaf_ref, mid_ref, top_ref, high_ref, low_ref)
    pltpu.make_async_copy(data_ref, ext_ref.at[pl.ds(1, 4), pl.ds(1, 4), 1], recv.at[0]).start()
    pltpu.make_async_copy(top_ref, tops_ref.at[ix, iy, iz], recv.at[2]).start()
    pltpu.make_async_copy(leaf_ref, wide_ref.at[pl.ds(1, 2), pl.ds(1, 2), pl.ds(1, 2)], recv.at[4]).start()
    pltpu.make_async_copy(mid_ref, mids_ref.at[13], recv.at[4]).start()
    for step in plane:
        remote(top_ref, tops_ref.at[ix, iy, iz], send.at[1], recv.at[2], step)
    for step in DIRECTIONS:
        spans = [span_of(d, 2, 1) for d in step]
        src = leaf_ref.at[spans[0][0], spans[1][0], spans[2][0]]
        dst = wide_ref.at[spans[0][1], spans[1][1], spans[2][1]]
        remote(src, dst, send.at[0], recv.at[4], step)
        slot = ((1 - step[0]) * 3 + (1 - step[1])) * 3 + (1 - step[2])
        remote(mid_ref, mids_ref.at[slot], send.at[0], recv.at[4], step)

    def drain(view, semaphore):
        pltpu.make_async_copy(view, view, semaphore).wait()

    clear_rows(rows_ref)
    done = 0
    inside = [(x, y) for x in range(1, 5) for y in range(1, 5)]
    fill_cells(inside, (1,), lambda x, y, ez: data_ref.at[x - 1, y - 1], table_ref)
    for k in range(PIECES - 1):
        pieces[k].wait()
        ready = ((k + 1) * (25600 // PIECES) - 256) // (3 * TERMS)
        align_operators(done, ready, whole_ref, aligned_ref)
        done = ready
    drain(ext_ref.at[pl.ds(0, 4), pl.ds(0, 4), pl.ds(0, 3)], recv.at[0])
    turn_cells(inside, ext_ref, turned_ref)
    turned = lambda x, y, ez: turned_ref.at[x, y, ez]
    fill_cells(inside, (0, 2), turned, table_ref)
    near_inside((0, 1, 2, 3), data_ref, table_ref, sums_ref)
    drain(tops_ref.at[ix], recv.at[2])
    for step in line:
        remote(tops_ref.at[ix], tops_ref.at[ix], send.at[0], recv.at[3], step)
    pieces[-1].wait()
    align_operators(done, TRIPLES, whole_ref, aligned_ref)
    for copy in loads[4:]:
        copy.wait()
    octant_operators(down_ref, down_rows)
    down_operators(octant_own, down_rows, downs_ref)
    drain(ext_ref.at[pl.ds(0, 5), pl.ds(0, 4)], recv.at[1])
    outside = [(x, y) for x in range(6) for y in range(6) if (x, y) not in inside]
    turn_cells(outside, ext_ref, turned_ref)
    fill_cells(outside, (0, 1, 2), turned, table_ref)
    near_outside(data_ref, table_ref, sums_ref)
    near_rows(sums_ref, data_ref, near_ref)
    drain(pool_ref.at[pl.ds(0, 728)], recv.at[4])
    gather_boxes(wide_ref, mids_ref, rows_ref)
    drain(tops_ref.at[pl.ds(0, 7)], recv.at[3])
    tops = (ix // 2, iy // 2, iz // 2)
    gather_upper(tops, tops_ref, rows_ref)
    operators = [octant_operator(up_rows, octant) for octant in range(8)]
    lattice_term = gather_top(tops, tops_ref, upper_ref, operators, lattice_ref, coarse_ref, rows_ref)
    convert_tiles(rows_ref, tiles_ref)
    extra = far_products(tiles_ref, aligned_ref, acc_ref)
    locals_down(octant_own, acc_ref, lattice_term + extra, downs_ref, local_ref)
    evaluate(local_ref, slope_ref, high_ref, low_ref, near_ref, live_ref, out_ref)
    drain(pool_ref, send.at[0])
    drain(line_ref, send.at[1])


VMEM = pl.BlockSpec(memory_space=pltpu.VMEM)


def shape(*dims):
    return jax.ShapeDtypeStruct(dims, F32)


def whole_call(sizes, *operands):
    dma = pltpu.SemaphoreType.DMA
    return pl.pallas_call(
        functools.partial(whole_kernel, *sizes),
        out_shape=shape(4, 4, 4, LANES),
        in_specs=[pl.BlockSpec(memory_space=pltpu.HBM)] * 8,
        out_specs=VMEM,
        scratch_shapes=[
            pltpu.VMEM((3, 4, 4, LANES), F32),
            pltpu.VMEM((4, 4, LANES), F32),
            pltpu.VMEM((4, 4, 4), jnp.int32),
            pltpu.VMEM((TERMS, 8, TERMS), BF16),
            pltpu.VMEM((TERMS, 8, TERMS), BF16),
            pltpu.VMEM((TERMS, 3 * LANES), BF16),
            pltpu.VMEM((TERMS, TERMS), BF16),
            pltpu.VMEM((4, 4, 4, LANES), F32),
            pltpu.VMEM((4, 4, LANES), F32),
            pltpu.VMEM((6, 6, 3, 4, LANES), F32),
            pltpu.VMEM((4, 4, 4, 8, LANES), F32),
            pltpu.VMEM((27, 8, LANES), F32),
            pltpu.VMEM((*sizes, 1, LANES), F32),
            pltpu.VMEM((2, 2, 2, 8, LANES), F32),
            pltpu.VMEM((8, LANES), F32),
            pltpu.VMEM((1, LANES), F32),
            pltpu.VMEM((TERMS * 8, LANES), F32),
            pltpu.VMEM((TERMS * 8, LANES), F32),
            pltpu.VMEM((9, KPAD, LANES), BF16),
            pltpu.VMEM((KPAD, 2048), BF16),
            pltpu.VMEM((KPAD, 2048), BF16),
            pltpu.VMEM((6, 6, 3, 4, LANES), F32),
            pltpu.VMEM((6, 6, 3, 4, SLOTS, LANES), F32),
            pltpu.VMEM((4, 4, 4, 8, LANES), F32),
            pltpu.VMEM((4, 4, 4, LANES), F32),
            pltpu.VMEM((TERMS, 25600), BF16),
            pltpu.VMEM((KPAD, TRIPLES * 256), BF16),
            pltpu.VMEM((218 * 16, LANES), F32),
            pltpu.VMEM((4, 218, 16, LANES), BF16),
            pltpu.VMEM((8, 32, LANES), F32),
            pltpu.VMEM((32, LANES), F32),
            pltpu.VMEM((LANES, LANES), F32),
            pltpu.VMEM((64, LANES), F32),
            pltpu.VMEM((1248, LANES), F32),
            pltpu.VMEM((31, 1, LANES), F32),
            dma((2,)),
            dma((5,)),
            dma((7 + PIECES,)),
        ],
        compiler_params=pltpu.CompilerParams(collective_id=0, has_side_effects=True),
        name="whole",
    )(*operands)


def part_kernel(both_ref, pot_ref, field_ref):
    pot_ref[...] = both_ref[0]
    field_ref[...] = both_ref[1:4]


def part_call(both):
    return pl.pallas_call(
        part_kernel,
        out_shape=(shape(4, 4, LANES), shape(3, 4, 4, LANES)),
        in_specs=[VMEM],
        out_specs=(VMEM,) * 2,
        name="part",
    )(both)


def solution(mesh):
    sizes = tuple(mesh.shape[axis] for axis in ("gx", "gy", "gz"))

    def per_device(
        positions, charges, counts, moment_shift, far_operators, local_shift, lattice_operator
    ):
        slope = jnp.asarray(slope_matrix()).astype(BF16)
        native_up = jnp.transpose(moment_shift, (1, 0, 2))
        native_down = jnp.transpose(local_shift, (1, 0, 2))
        both = whole_call(
            sizes,
            positions,
            charges,
            counts,
            native_up,
            native_down,
            slope,
            lattice_operator,
            far_operators,
        )
        return part_call(both)

    placed = (
        P(None, "gx", "gy", "gz"),
        P("gx", "gy", "gz"),
        P("gx", "gy", "gz"),
        P(),
        P(),
        P(),
        P(),
    )
    return jax.shard_map(
        per_device,
        mesh=mesh,
        in_specs=placed,
        out_specs=(P("gx", "gy", "gz"), P(None, "gx", "gy", "gz")),
        check_vma=False,
    )
```
